32 devices in a mesh: dp: 4 (over y, z), tp: 8 (over x, core).
Axes of the slice: x: 4, y: 2, z: 2, core: 2. Of those that a mesh axis runs over, the one named last changes fastest.
The devices are a block of a 4x4x8 slice.
Arguments:
- tokens: int32 [4, 128], P('dp'), parts along dimension 0
- positions: int32 [4, 128], P('dp'), parts along dimension 0
- embedding: bfloat16 [16384, 2048], P('tp')
- gain_attn: float32 [2048], replicated
- gain_mlp: float32 [2048], replicated
- w_query: bfloat16 [2048, 16, 128], P(None, 'tp')
- w_key: bfloat16 [2048, 8, 128], P(None, 'tp')
- w_value: bfloat16 [2048, 8, 128], P(None, 'tp')
- w_out: bfloat16 [16, 128, 2048], P('tp')
- w_gate: bfloat16 [2048, 6144], P(None, 'tp')
- w_up: bfloat16 [2048, 6144], P(None, 'tp')
- w_down: bfloat16 [6144, 2048], P('tp')
- grad_hidden: bfloat16 [4, 128, 2048], P('dp', 'tp'), parts along dimension 0
Outputs:
- output 1: bfloat16 [4, 128, 2048], P('dp', 'tp'), parts along dimension 0
- output 2: float32 [65536, 2048], P(('dp', 'tp')), parts along dimension 0
- output 3: float32 [8192, 16, 128], P('dp', 'tp'), parts along dimension 0
- output 4: float32 [8192, 8, 128], P('dp', 'tp'), parts along dimension 0
- output 5: float32 [8192, 8, 128], P('dp', 'tp'), parts along dimension 0
- output 6: float32 [64, 128, 2048], P(('dp', 'tp')), parts along dimension 0
- output 7: float32 [8192, 6144], P('dp', 'tp'), parts along dimension 0
- output 8: float32 [8192, 6144], P('dp', 'tp'), parts along dimension 0
- output 9: float32 [24576, 2048], P(('dp', 'tp')), parts along dimension 0
- output 10: float32 [8192], P('dp'), parts along dimension 0
- output 11: float32 [8192], P('dp'), parts along dimension 0
There are 4 independent parts. The reference program is written for one: setup_inputs(seed, part) draws one part's arguments, and reference() takes and returns one part's arrays. A program takes and returns all parts, laid end to end along the dimension named above; an argument that names none is the same for every part.
All inputs are finite; a program needn't handle non-finite values.
Results may differ from the reference program's by a relative error of at most 0.02.
Values are sent between devices in bfloat16 or wider.
A program may use at most 768 MiB of HBM per device.

```python
import jax
import jax.numpy as jnp
from jax import lax

BATCH_SIZE = 1
SEQ_LEN = 128
VOCAB_SIZE = 16384
MODEL_DIM = 2048
NUM_HEADS = 16
KV_HEADS = 8
HEAD_DIM = 128
FFN_DIM = 6144
HOT_COUNT = 16
ROPE_THETA = 1000000.0
RMS_EPS = 1e-5


def draw_tokens(rng_key):
    sub_keys = jax.random.split(rng_key, 7)
    tok_shape = (BATCH_SIZE, SEQ_LEN)
    first_draw = jax.random.randint(sub_keys[0], tok_shape, 0, VOCAB_SIZE)
    second_draw = jax.random.randint(sub_keys[1], tok_shape, 0, VOCAB_SIZE)
    base_ids = jnp.minimum(first_draw, second_draw)
    hot_ids = jax.random.randint(sub_keys[2], (HOT_COUNT,), 0, VOCAB_SIZE)
    hot_pick = jax.random.randint(sub_keys[3], tok_shape, 0, HOT_COUNT)
    use_hot = jax.random.randint(sub_keys[4], tok_shape, 0, 4) == 0
    token_ids = jnp.where(use_hot, hot_ids[hot_pick], base_ids)
    top_place = jax.random.randint(sub_keys[5], (), 0, SEQ_LEN // 2)
    low_place = jax.random.randint(sub_keys[6], (), SEQ_LEN // 2, SEQ_LEN)
    token_ids = token_ids.at[0, top_place].set(VOCAB_SIZE - 1)
    token_ids = token_ids.at[0, low_place].set(0)
    return token_ids.astype(jnp.int32)


def draw_positions(rng_key):
    pos_steps = jax.random.randint(rng_key, (BATCH_SIZE, SEQ_LEN), 1, 4)
    return jnp.cumsum(pos_steps, axis=1).astype(jnp.int32)


def scaled_normal(rng_key, dim_shape, factor):
    return (jax.random.normal(rng_key, dim_shape, jnp.float32) * factor).astype(jnp.bfloat16)


def setup_inputs(seed: int = 0, part: int = 0) -> dict:
    shared = jax.random.split(jax.random.key(seed), 10)
    part_keys = jax.random.split(jax.random.fold_in(jax.random.key(seed + 1), part), 3)
    in_scale = MODEL_DIM ** -0.5
    return {
        'tokens': draw_tokens(part_keys[0]),
        'positions': draw_positions(part_keys[1]),
        'embedding': scaled_normal(shared[0], (VOCAB_SIZE, MODEL_DIM), 1.0),
        'gain_attn': 1.0 + 0.25 * jax.random.normal(shared[1], (MODEL_DIM,), jnp.float32),
        'gain_mlp': 1.0 + 0.25 * jax.random.normal(shared[2], (MODEL_DIM,), jnp.float32),
        'w_query': scaled_normal(shared[3], (MODEL_DIM, NUM_HEADS, HEAD_DIM), in_scale),
        'w_key': scaled_normal(shared[4], (MODEL_DIM, KV_HEADS, HEAD_DIM), in_scale),
        'w_value': scaled_normal(shared[5], (MODEL_DIM, KV_HEADS, HEAD_DIM), in_scale),
        'w_out': scaled_normal(shared[6], (NUM_HEADS, HEAD_DIM, MODEL_DIM), (NUM_HEADS * HEAD_DIM) ** -0.5),
        'w_gate': scaled_normal(shared[7], (MODEL_DIM, FFN_DIM), in_scale),
        'w_up': scaled_normal(shared[8], (MODEL_DIM, FFN_DIM), in_scale),
        'w_down': scaled_normal(shared[9], (FFN_DIM, MODEL_DIM), FFN_DIM ** -0.5),
        'grad_hidden': scaled_normal(part_keys[2], (BATCH_SIZE, SEQ_LEN, MODEL_DIM), 1.0),
    }


def rope_tables(positions, head_dim):
    half_dim = head_dim // 2
    inv_freq = ROPE_THETA ** (-jnp.arange(half_dim, dtype=jnp.float32) * (2.0 / head_dim))
    angles = positions.astype(jnp.float32)[:, :, None] * inv_freq
    return jnp.cos(angles)[:, :, None, :], jnp.sin(angles)[:, :, None, :]


def rotate(values, cos_tab, sin_tab):
    half_dim = values.shape[-1] // 2
    first_half = values[..., :half_dim]
    second_half = values[..., half_dim:]
    return jnp.concatenate([first_half * cos_tab - second_half * sin_tab, second_half * cos_tab + first_half * sin_tab], axis=-1)


def rms_norm(hidden, gain_vec):
    hidden_f = hidden.astype(jnp.float32)
    inv_rms = lax.rsqrt(jnp.mean(hidden_f * hidden_f, axis=-1, keepdims=True) + RMS_EPS)
    return (hidden_f * inv_rms * gain_vec).astype(jnp.bfloat16)


def layer(first_x, gain_pair, weight_mats, positions):
    w_query, w_key, w_value, w_out, w_gate, w_up, w_down = weight_mats
    batch_size, seq_len = positions.shape
    num_heads, head_dim = w_query.shape[1], w_query.shape[2]
    kv_heads = w_key.shape[1]
    group_size = num_heads // kv_heads
    cos_tab, sin_tab = rope_tables(positions, head_dim)
    normed1 = rms_norm(first_x, gain_pair[0]).astype(jnp.float32)
    queries = rotate(jnp.einsum('bsd,dhe->bshe', normed1, w_query), cos_tab, sin_tab)
    queries = queries.astype(jnp.bfloat16).astype(jnp.float32).reshape(batch_size, seq_len, kv_heads, group_size, head_dim)
    keys_rot = rotate(jnp.einsum('bsd,dhe->bshe', normed1, w_key), cos_tab, sin_tab).astype(jnp.bfloat16).astype(jnp.float32)
    values = jnp.einsum('bsd,dhe->bshe', normed1, w_value).astype(jnp.bfloat16).astype(jnp.float32)
    causal = jnp.arange(seq_len)[:, None] >= jnp.arange(seq_len)[None, :]
    scores = jnp.einsum('bqkgd,bskd->bkgqs', queries, keys_rot) * head_dim ** -0.5
    probs_f = jax.nn.softmax(jnp.where(causal, scores, -1e30), axis=-1)
    probs_r = probs_f.astype(jnp.bfloat16).astype(jnp.float32)
    attn_heads = jnp.einsum('bkgqs,bskd->bqkgd', probs_r, values).astype(jnp.bfloat16).astype(jnp.float32)
    attn_heads = attn_heads.reshape(batch_size, seq_len, num_heads, head_dim)
    attn_out = jnp.einsum('bshe,hed->bsd', attn_heads, w_out)
    hidden1 = (first_x.astype(jnp.float32) + attn_out).astype(jnp.bfloat16)
    normed2 = rms_norm(hidden1, gain_pair[1]).astype(jnp.float32)
    gate_pre = jnp.einsum('bsd,df->bsf', normed2, w_gate)
    up_pre = jnp.einsum('bsd,df->bsf', normed2, w_up)
    act_r = (jax.nn.silu(gate_pre) * up_pre).astype(jnp.bfloat16).astype(jnp.float32)
    mlp_out = jnp.einsum('bsf,fd->bsd', act_r, w_down)
    return (hidden1.astype(jnp.float32) + mlp_out).astype(jnp.bfloat16)


def reference(tokens, positions, embedding, gain_attn, gain_mlp, w_query, w_key, w_value, w_out, w_gate, w_up, w_down, grad_hidden):
    first_x = jnp.take(embedding, tokens, axis=0)
    weight_mats = tuple(weight.astype(jnp.float32) for weight in (w_query, w_key, w_value, w_out, w_gate, w_up, w_down))
    hidden_out, back_fn = jax.vjp(lambda x_in, gain_pair, mats_in: layer(x_in, gain_pair, mats_in, positions), first_x, (gain_attn, gain_mlp), weight_mats)
    grad_x, grad_gains, grad_mats = back_fn(grad_hidden)
    grad_embedding = jax.ops.segment_sum(grad_x.reshape(-1, MODEL_DIM).astype(jnp.float32), tokens.reshape(-1), num_segments=VOCAB_SIZE)
    return (hidden_out, grad_embedding, grad_mats[0], grad_mats[1], grad_mats[2], grad_mats[3], grad_mats[4], grad_mats[5], grad_mats[6], grad_gains[0], grad_gains[1])
```

```python
import functools

import jax
import jax.numpy as jnp
import numpy as np
from jax import lax
from jax.experimental import pallas as pl
from jax.experimental.pallas import tpu as pltpu
from jax.sharding import PartitionSpec as P

ROPE_THETA = 1000000.0
RMS_EPS = 1e-5
MESH = pl.DeviceIdType.MESH
BF = jnp.bfloat16
F32 = jnp.float32
NT = (((1,), (1,)), ((), ()))
TN = (((0,), (0,)), ((), ()))

N1, GH, N2, GH1, GF, GAIN = range(6)
R_EMB, R_ATT, R_GN2, R_MLP, R_GN1 = range(5)
RS_CHUNKS = {R_EMB: 4, R_ATT: 2, R_GN2: 4, R_MLP: 2, R_GN1: 2}


def dot(a, b, dims=(((1,), (0,)), ((), ()))):
    return lax.dot_general(a, b, dims, preferred_element_type=F32)


def layer_kernel(n_tp, local_heads,
                 tok, pos, invf, ga, gm, gh_in, emb, wq4, wk, wv, wo, wg, wu, wd,
                 o_n1, o_n2, o_gh, o_gh1, o_gf, o_act, o_gcat, o_heads, o_gqkv, o_gain, o_hid,
                 embv, onehot, wqr, wqf, wqkv, wov, wguv, wdv, ag, pb, rd, sb, rr,
                 act, gcat, heads, gqkv, gbuf, hid, x0f, nrm1, nrm2, h1f, gh1f, inv, gact, qkvb, tabs, probs,
                 ag_s, ag_r, rs_s, rs_r, loc):
    chips = n_tp // 2
    seq = tok.shape[1]
    rows, dim = emb.shape
    ffn = wd.shape[0]
    blk = gh_in.shape[0]
    hd = wk.shape[1]
    scale = hd ** -0.5
    qw = local_heads * hd

    me = lax.axis_index('tp')
    chip = me // 2
    core = lax.rem(me, 2)
    sib = 2 * chip + 1 - core

    def peer_chip(d):
        return lax.rem(chip + d, chips)

    def peer(d):
        return 2 * peer_chip(d) + core

    order = sorted(range(1, chips), key=lambda d: -min(d, chips - d))

    barrier = pltpu.get_barrier_semaphore()
    for dev in [sib] + [peer(d) for d in range(1, chips)]:
        pl.semaphore_signal(barrier, inc=1, device_id={'tp': dev}, device_id_type=MESH)

    pending = []
    nloc = [0]

    def local(src, dst):
        cp = pltpu.make_async_copy(src, dst, loc.at[nloc[0]])
        nloc[0] += 1
        cp.start()
        return cp

    n_emb = RS_CHUNKS[R_EMB]
    ew = dim // n_emb
    emb_cp = [local(emb.at[:, pl.ds(j * ew, ew)], embv.at[:, pl.ds(j * ew, ew)]) for j in range(n_emb)]

    tok_t = jnp.transpose(jnp.broadcast_to(tok[...].astype(F32), (seq, seq)))
    tok_t = tok_t - (me * rows).astype(F32)
    lane = lax.broadcasted_iota(jnp.int32, (seq, seq), 1).astype(F32)
    for b in range(rows // seq):
        onehot[:, b * seq:(b + 1) * seq] = jnp.where(tok_t == lane + float(b * seq), 1.0, 0.0).astype(BF)

    def remote(src, dst, s, r, dev):
        return pltpu.make_async_remote_copy(src_ref=src, dst_ref=dst, send_sem=s, recv_sem=r,
                                            device_id={'tp': dev}, device_id_type=MESH)

    def send(*args):
        cp = remote(*args)
        cp.start()
        pending.append(cp)

    def ag_ref(p, t):
        return gbuf.at[t] if p == GAIN else ag.at[p, t]

    def ag_start(p):
        mine = ag_ref(p, me)
        for d in order:
            send(mine, mine, ag_s.at[p, d], ag_r.at[p, d], peer(d))
        send(mine, mine, ag_s.at[p, 0], ag_r.at[p, 0], sib)

    def ag_finish(p):
        for d in sorted(range(1, chips), key=lambda d: min(d, chips - d)):
            src = lax.rem(chip + chips - d, chips)
            got = ag_ref(p, 2 * src + core)
            remote(got, got, ag_s.at[p, d], ag_r.at[p, d], sib).wait_recv()
            send(got, got, ag_s.at[p, chips - 1 + d], ag_r.at[p, chips - 1 + d], sib)
        got = ag_ref(p, sib)
        remote(got, got, ag_s.at[p, 0], ag_r.at[p, 0], sib).wait_recv()
        for d in sorted(range(1, chips), key=lambda d: min(d, chips - d)):
            src = lax.rem(chip + chips - d, chips)
            got = ag_ref(p, 2 * src + 1 - core)
            remote(got, got, ag_s.at[p, chips - 1 + d], ag_r.at[p, chips - 1 + d], sib).wait_recv()

    def gathered(p):
        return ag[p].reshape(seq, dim)

    def rs_cols(p, j):
        w = dim // RS_CHUNKS[p]
        return slice(j * w, (j + 1) * w)

    def rs_local(p, j, val):
        c = rs_cols(p, j)
        w = c.stop - c.start
        pb[p, :, :, :, c] = val.astype(BF).reshape(chips, 2, blk, w)
        send(pb.at[p, :, 1 - core, :, c], rd.at[p, :, :, c], rs_s.at[p, j, 0], rs_r.at[p, j, 0], sib)

    def rs_cross(p, j):
        c = rs_cols(p, j)
        remote(rd.at[p, :, :, c], rd.at[p, :, :, c], rs_s.at[p, j, 0], rs_r.at[p, j, 0], sib).wait_recv()
        for d in order:
            to = peer_chip(d)
            both = pb[p, to, core, :, c].astype(F32) + rd[p, to, :, c].astype(F32)
            sb[p, to, :, c] = both.astype(BF)
            send(sb.at[p, to, :, c], rr.at[p, d - 1, :, c], rs_s.at[p, j, d], rs_r.at[p, j, d], peer(d))

    def rs_finish(p):
        parts = []
        for j in range(RS_CHUNKS[p]):
            c = rs_cols(p, j)
            total = pb[p, chip, core, :, c].astype(F32) + rd[p, chip, :, c].astype(F32)
            for d in order[::-1]:
                remote(rr.at[p, d - 1, :, c], rr.at[p, d - 1, :, c], rs_s.at[p, j, d], rs_r.at[p, j, d], sib).wait_recv()
                total = total + rr[p, d - 1, :, c].astype(F32)
            parts.append(total)
        return jnp.concatenate(parts, axis=1)

    def rs_start(p, chunk):
        for j in range(RS_CHUNKS[p] + 1):
            if j < RS_CHUNKS[p]:
                rs_local(p, j, chunk(rs_cols(p, j)))
            if j > 0:
                rs_cross(p, j - 1)

    def norm_fwd(x, gain):
        r = lax.rsqrt(jnp.mean(x * x, axis=-1, keepdims=True) + RMS_EPS)
        n = x * r
        return (n * gain).astype(BF), n, r

    def norm_bwd(g, n, r, gain):
        part = jnp.sum(g * n, axis=0, keepdims=True)
        scaled = g * gain
        return r * (scaled - n * jnp.mean(scaled * n, axis=-1, keepdims=True)), part

    pl.semaphore_wait(barrier, chips)

    w_cp = {}

    def emb_chunk(c):
        j = c.start // ew
        emb_cp[j].wait()
        if j == n_emb - 2:
            w_cp['k'] = local(wk, wqkv.at[:, pl.ds(qw, hd)])
            w_cp['v'] = local(wv, wqkv.at[:, pl.ds(qw + hd, hd)])
            w_cp['q'] = local(wq4, wqr)
            w_cp['o'] = local(wo, wov)
        if j == n_emb - 1:
            w_cp['d'] = local(wd, wdv)
            w_cp['g'] = local(wg, wguv.at[:, pl.ds(0, ffn)])
            w_cp['u'] = local(wu, wguv.at[:, pl.ds(ffn, ffn)])
        return dot(onehot[...], embv[:, c])

    rs_start(R_EMB, emb_chunk)

    pos_t = jnp.transpose(jnp.broadcast_to(pos[...].astype(F32), (seq, seq)))
    angle = pos_t * invf[...]
    half = lax.broadcasted_iota(jnp.int32, (seq, hd), 1) < hd // 2
    tabs[0] = jnp.cos(angle)
    sin = jnp.sin(angle)
    tabs[1] = jnp.where(half, -sin, sin)
    w_cp['q'].wait()
    wqf[...] = wqr[...].astype(F32)
    for h in range(local_heads):
        wqkv[:, h * hd:(h + 1) * hd] = wqf[pl.ds(h, dim, stride=local_heads), :].astype(BF)

    x0 = rs_finish(R_EMB)
    x0f[...] = x0
    n1b, n1, r1 = norm_fwd(x0, ga[...])
    ag[N1, me] = n1b
    nrm1[...] = n1
    inv[0] = jnp.broadcast_to(r1, (blk, hd))
    ag_start(N1)
    ag[GH, me] = gh_in[...]
    ag_start(GH)
    w_cp['k'].wait()
    w_cp['v'].wait()
    ag_finish(N1)
    outs = [local(ag.at[N1], o_n1)]

    def rotate(v, sign):
        return v * tabs[0] + sign * (pltpu.roll(v, hd // 2, 1) * tabs[1])

    qkv = dot(gathered(N1), wqkv[...])
    for h in range(local_heads + 1):
        qkvb[:, h * hd:(h + 1) * hd] = rotate(qkv[:, h * hd:(h + 1) * hd], 1.0).astype(BF)
    qkvb[:, qw + hd:] = qkv[:, qw + hd:].astype(BF)
    kb = qkvb[:, qw:qw + hd]
    vb = qkvb[:, qw + hd:]
    causal = lax.broadcasted_iota(jnp.int32, (seq, seq), 0) >= lax.broadcasted_iota(jnp.int32, (seq, seq), 1)
    for h in range(local_heads):
        s = dot(qkvb[:, h * hd:(h + 1) * hd], kb, NT) * scale
        s = jnp.where(causal, s, -1e30)
        e = jnp.exp(s - jnp.max(s, axis=-1, keepdims=True))
        pr = e / jnp.sum(e, axis=-1, keepdims=True)
        probs[h] = pr
        heads[:, h * hd:(h + 1) * hd] = dot(pr.astype(BF), vb).astype(BF)
    w_cp['o'].wait()
    rs_start(R_ATT, lambda c: dot(heads[...], wov[:, c]))
    outs.append(local(heads, o_heads))

    ag_finish(GH)
    outs.append(local(ag.at[GH], o_gh))
    w_cp['d'].wait()
    gact[...] = dot(gathered(GH), wdv[...], NT).astype(BF).astype(F32)

    h1 = (x0f[...] + rs_finish(R_ATT).astype(BF).astype(F32)).astype(BF).astype(F32)
    h1f[...] = h1
    n2b, n2, r2 = norm_fwd(h1, gm[...])
    ag[N2, me] = n2b
    nrm2[...] = n2
    inv[1] = jnp.broadcast_to(r2, (blk, hd))
    ag_start(N2)
    w_cp['g'].wait()
    w_cp['u'].wait()
    ag_finish(N2)
    outs.append(local(ag.at[N2], o_n2))

    fw = 256
    for j in range(ffn // fw):
        c = slice(j * fw, (j + 1) * fw)
        cu = slice(ffn + j * fw, ffn + (j + 1) * fw)
        gate = dot(gathered(N2), wguv[:, c])
        up = dot(gathered(N2), wguv[:, cu])
        sig = jax.nn.sigmoid(gate)
        ga_act = gate * sig
        act[:, c] = (ga_act * up).astype(BF)
        g = gact[:, c]
        gcat[:, cu] = (g * ga_act).astype(BF)
        gcat[:, c] = (g * up * sig * (1.0 + gate * (1.0 - sig))).astype(BF)
    rs_start(R_GN2, lambda c: dot(gcat[...], wguv[c, :], NT))
    outs.append(local(gcat, o_gcat))
    outs.append(local(act, o_act))
    for j in range(RS_CHUNKS[R_MLP]):
        rs_local(R_MLP, j, dot(act[...], wdv[:, rs_cols(R_MLP, j)]))

    gn2 = rs_finish(R_GN2).astype(BF).astype(F32)
    g_in, gain_part = norm_bwd(gn2, nrm2[...], inv[1][:, :1], gm[...])
    gbuf[me, 1:2, :] = gain_part
    gh1 = (gh_in[...].astype(F32) + g_in).astype(BF)
    gh1f[...] = gh1.astype(F32)
    ag[GH1, me] = gh1
    ag_start(GH1)
    for j in range(RS_CHUNKS[R_MLP]):
        rs_cross(R_MLP, j)
    ag_finish(GH1)
    outs.append(local(ag.at[GH1], o_gh1))

    ghd = dot(gathered(GH1), wov[...], NT).astype(BF)
    gv = jnp.zeros((seq, hd), F32)
    gk = jnp.zeros((seq, hd), F32)
    for h in range(local_heads):
        g = ghd[:, h * hd:(h + 1) * hd]
        pr = probs[h]
        gp = dot(g, vb, NT).astype(BF).astype(F32)
        gv = gv + dot(pr.astype(BF), g, TN)
        gs = (pr * (gp - jnp.sum(gp * pr, axis=-1, keepdims=True)) * scale).astype(BF)
        gq = dot(gs, kb).astype(BF).astype(F32)
        gk = gk + dot(gs, qkvb[:, h * hd:(h + 1) * hd], TN)
        gqkv[:, h * hd:(h + 1) * hd] = rotate(gq, -1.0).astype(BF)
    gqkv[:, qw:qw + hd] = rotate(gk.astype(BF).astype(F32), -1.0).astype(BF)
    gqkv[:, qw + hd:] = gv.astype(BF)
    rs_start(R_GN1, lambda c: dot(gqkv[...], wqkv[c, :], NT))
    outs.append(local(gqkv, o_gqkv))
    hid[...] = (h1f[...] + rs_finish(R_MLP).astype(BF).astype(F32)).astype(BF)
    outs.append(local(hid, o_hid))

    gn1 = rs_finish(R_GN1).astype(BF).astype(F32)
    g_in, gain_part = norm_bwd(gn1, nrm1[...], inv[0][:, :1], ga[...])
    gbuf[me, 0:1, :] = gain_part
    ag[GF, me] = (gh1f[...] + g_in).astype(BF)
    ag_start(GF)
    ag_start(GAIN)
    ag_finish(GF)
    outs.append(local(ag.at[GF], o_gf))
    ag_finish(GAIN)
    outs.append(local(gbuf, o_gain))
    for cp in pending:
        cp.wait_send()
    for cp in outs:
        cp.wait()


def grads_kernel(n_tp, local_heads,
                 tok, n1, n2, gh, gh1, gf, act, gcat, heads, gqkv, gain, hid,
                 o_hid, o_emb, o_wq, o_wk, o_wv, o_wo, o_wg, o_wu, o_wd, o_ga, o_gm,
                 wide, tall, qbuf, kvbuf, s_wide, s_tall, s_qkv):
    seq, dim = n1.shape
    rows = o_emb.shape[0]
    ffn = act.shape[1]
    hd = gqkv.shape[1] // (local_heads + 2)
    me = lax.axis_index('tp')
    n_wide, wr = wide.shape[0], wide.shape[1]
    n_tall, tr = tall.shape[0], tall.shape[1]
    busy = {}

    def put(key, src, dst, sem):
        cp = pltpu.make_async_copy(src, dst, sem)
        cp.start()
        busy[key] = cp

    def free(key):
        if key in busy:
            busy.pop(key).wait()

    tok_l = tok[...] - me * rows
    row = lax.broadcasted_iota(jnp.int32, (wr, seq), 0)
    wide_units = []
    for u in range(act.shape[1] // wr):
        wide_units.append((lambda u=u: dot(act[:, u * wr:(u + 1) * wr], gh[...], TN), o_wd.at[pl.ds(u * wr, wr)]))
    for u in range(heads.shape[1] // wr):
        wide_units.append((lambda u=u: dot(heads[:, u * wr:(u + 1) * wr], gh1[...], TN), o_wo.at[pl.ds(u * wr, wr)]))
    for u in range(rows // wr):
        wide_units.append((lambda u=u: dot(jnp.where(row + u * wr == tok_l, 1.0, 0.0).astype(BF), gf[...]), o_emb.at[pl.ds(u * wr, wr)]))
    tall_units = []
    for half, out in ((0, o_wg), (1, o_wu)):
        for u in range(dim // tr):
            tall_units.append((lambda u=u, half=half: dot(n2[:, u * tr:(u + 1) * tr], gcat[:, half * ffn:(half + 1) * ffn], TN),
                               out.at[pl.ds(u * tr, tr)]))
    iw = it = 0
    while iw < len(wide_units) or it < len(tall_units):
        if it < len(tall_units):
            slot = it % n_tall
            free(('t', slot))
            tall[slot] = tall_units[it][0]()
            put(('t', slot), tall.at[slot], tall_units[it][1], s_tall.at[slot])
            it += 1
        if iw < len(wide_units):
            slot = iw % n_wide
            free(('w', slot))
            wide[slot] = wide_units[iw][0]()
            put(('w', slot), wide.at[slot], wide_units[iw][1], s_wide.at[slot])
            iw += 1
    qw = local_heads * hd
    for i, out in enumerate((o_wk, o_wv)):
        kvbuf[i] = dot(n1[...], gqkv[:, qw + i * hd:qw + (i + 1) * hd], TN)
        put(('k', i), kvbuf.at[i], out, s_qkv.at[i])
    for h in range(local_heads):
        qbuf[pl.ds(h, dim, stride=local_heads), :] = dot(n1[...], gqkv[:, h * hd:(h + 1) * hd], TN)
    put(('q', 0), qbuf, o_wq, s_qkv.at[2])

    o_hid[...] = hid[...]
    total = gain[0]
    for t in range(1, n_tp):
        total = total + gain[t]
    o_ga[...] = total[0:1]
    o_gm[...] = total[1:2]
    for key in list(busy):
        free(key)


def solution(mesh):
    n_tp = mesh.shape['tp']
    chips = n_tp // 2
    in_specs = (P('dp', None), P('dp', None), P('tp', None), P(None), P(None),
                P(None, 'tp', None), P(None, 'tp', None), P(None, 'tp', None), P('tp', None, None),
                P(None, 'tp'), P(None, 'tp'), P('tp', None), P('dp', 'tp', None))
    out_specs = (P('dp', 'tp', None), P(('dp', 'tp'), None),
                 P('dp', 'tp', None), P('dp', 'tp', None), P('dp', 'tp', None), P(('dp', 'tp'), None, None),
                 P('dp', 'tp'), P('dp', 'tp'), P(('dp', 'tp'), None), P('dp'), P('dp'))

    def device_fn(tokens, positions, emb, gain_attn, gain_mlp, w_query, w_key, w_value, w_out, w_gate, w_up, w_down, grad_hidden):
        seq = tokens.shape[1]
        rows, dim = emb.shape
        lh, hd = w_query.shape[1], w_query.shape[2]
        ffn = w_down.shape[0]
        blk = grad_hidden.shape[1]
        qkvw = (lh + 2) * hd
        inv_freq = (np.float32(ROPE_THETA) ** (-np.arange(hd // 2, dtype=np.float32) * np.float32(2.0 / hd))).astype(np.float32)
        invf = jnp.asarray(np.concatenate([inv_freq, inv_freq])[None, :])

        def sds(shape, dt=BF):
            return jax.ShapeDtypeStruct(shape, dt)

        vm = pl.BlockSpec(memory_space=pltpu.VMEM)
        hb = pl.BlockSpec(memory_space=pl.ANY)
        maxc = max(RS_CHUNKS.values())
        mid = pl.pallas_call(
            functools.partial(layer_kernel, n_tp, lh),
            name='layer',
            out_shape=[sds((n_tp, blk, dim))] * 5 + [sds((seq, ffn)), sds((seq, 2 * ffn)), sds((seq, lh * hd)), sds((seq, qkvw)),
                                                    sds((n_tp, 2, dim), F32), sds((blk, dim))],
            in_specs=[vm] * 6 + [hb] * 8,
            out_specs=[hb] * 11,
            scratch_shapes=[
                pltpu.VMEM((rows, dim), BF), pltpu.VMEM((seq, rows), BF), pltpu.VMEM((dim * lh, hd), BF), pltpu.VMEM((dim * lh, hd), F32),
                pltpu.VMEM((dim, qkvw), BF), pltpu.VMEM((lh * hd, dim), BF), pltpu.VMEM((dim, 2 * ffn), BF), pltpu.VMEM((ffn, dim), BF),
                pltpu.VMEM((5, n_tp, blk, dim), BF), pltpu.VMEM((5, chips, 2, blk, dim), BF), pltpu.VMEM((5, chips, blk, dim), BF),
                pltpu.VMEM((5, chips, blk, dim), BF), pltpu.VMEM((5, chips - 1, blk, dim), BF),
                pltpu.VMEM((seq, ffn), BF), pltpu.VMEM((seq, 2 * ffn), BF), pltpu.VMEM((seq, lh * hd), BF), pltpu.VMEM((seq, qkvw), BF),
                pltpu.VMEM((n_tp, 2, dim), F32), pltpu.VMEM((blk, dim), BF),
                pltpu.VMEM((blk, dim), F32), pltpu.VMEM((blk, dim), F32), pltpu.VMEM((blk, dim), F32), pltpu.VMEM((blk, dim), F32),
                pltpu.VMEM((blk, dim), F32), pltpu.VMEM((2, blk, hd), F32), pltpu.VMEM((seq, ffn), F32), pltpu.VMEM((seq, qkvw), BF),
                pltpu.VMEM((2, seq, hd), F32), pltpu.VMEM((lh, seq, seq), F32),
                pltpu.SemaphoreType.DMA((6, 2 * chips - 1)), pltpu.SemaphoreType.DMA((6, 2 * chips - 1)),
                pltpu.SemaphoreType.DMA((5, maxc, chips)), pltpu.SemaphoreType.DMA((5, maxc, chips)),
                pltpu.SemaphoreType.DMA((32,)),
            ],
            compiler_params=pltpu.CompilerParams(collective_id=0, has_side_effects=True, vmem_limit_bytes=64 * 1024 * 1024 - 65536),
        )(tokens, positions, invf, gain_attn.reshape(1, dim), gain_mlp.reshape(1, dim), grad_hidden.reshape(blk, dim),
          emb, w_query.reshape(dim * lh, hd), w_key.reshape(dim, hd), w_value.reshape(dim, hd), w_out.reshape(lh * hd, dim),
          w_gate, w_up, w_down)
        n1, n2, gh, gh1, gf, act, gcat, heads, gqkv, gain, hid = mid
        n1, n2, gh, gh1, gf = (a.reshape(seq, dim) for a in (n1, n2, gh, gh1, gf))
        wide_rows, tall_rows = 256, 512
        res = pl.pallas_call(
            functools.partial(grads_kernel, n_tp, lh),
            name='grads',
            out_shape=[sds((blk, dim)), sds((rows, dim), F32), sds((dim * lh, hd), F32), sds((dim, hd), F32), sds((dim, hd), F32),
                       sds((lh * hd, dim), F32), sds((dim, ffn), F32), sds((dim, ffn), F32), sds((ffn, dim), F32),
                       sds((1, dim), F32), sds((1, dim), F32)],
            in_specs=[vm] * 12,
            out_specs=[vm] + [hb] * 8 + [vm] * 2,
            scratch_shapes=[
                pltpu.VMEM((3, wide_rows, dim), F32), pltpu.VMEM((3, tall_rows, ffn), F32), pltpu.VMEM((dim * lh, hd), F32),
                pltpu.VMEM((2, dim, hd), F32),
                pltpu.SemaphoreType.DMA((3,)), pltpu.SemaphoreType.DMA((3,)), pltpu.SemaphoreType.DMA((3,)),
            ],
            compiler_params=pltpu.CompilerParams(vmem_limit_bytes=60 * 1024 * 1024),
        )(tokens, n1, n2, gh, gh1, gf, act, gcat, heads, gqkv, gain, hid)
        o_hid, o_emb, o_wq, o_wk, o_wv, o_wo, o_wg, o_wu, o_wd, o_ga, o_gm = res
        return (o_hid.reshape(1, blk, dim), o_emb, o_wq.reshape(dim, lh, hd), o_wk.reshape(dim, 1, hd), o_wv.reshape(dim, 1, hd),
                o_wo.reshape(lh, hd, dim), o_wg, o_wu, o_wd, o_ga.reshape(dim), o_gm.reshape(dim))

    return jax.shard_map(device_fn, mesh=mesh, in_specs=in_specs, out_specs=out_specs, check_vma=False)
```

```python
import functools

import jax
import jax.numpy as jnp
import numpy as np
from jax import lax
from jax.experimental import pallas as pl
from jax.experimental.pallas import tpu as pltpu
from jax.sharding import PartitionSpec as P

ROPE_THETA = 1000000.0
RMS_EPS = 1e-5
MESH = pl.DeviceIdType.MESH
BF = jnp.bfloat16
F32 = jnp.float32
NT = (((1,), (1,)), ((), ()))
TN = (((0,), (0,)), ((), ()))

N1, GH, N2, GH1, GF, GAIN = range(6)
R_EMB, R_ATT, R_GN2, R_MLP, R_GN1 = range(5)
RS_CHUNKS = {R_EMB: 4, R_ATT: 2, R_GN2: 4, R_MLP: 2, R_GN1: 2}


def dot(a, b, dims=(((1,), (0,)), ((), ()))):
    return lax.dot_general(a, b, dims, preferred_element_type=F32)


def scoped(name):
    def wrap(fn):
        def run(p, *rest):
            with jax.named_scope(f'{name}_{p}'):
                return fn(p, *rest)
        return run
    return wrap


def layer_kernel(n_tp, local_heads,
                 h_tok, h_pos, h_invf, h_ga, h_gm, h_gh, emb, wq4, wk, wv, wo, wg, wu, wd,
                 o_n1, o_n2, o_gh, o_gh1, o_gf, o_act, o_gcat, o_heads, o_gqkv, o_gain, o_hid,
                 tok, pos, invf, ga, gm, gh_in, embv, onehot, wqr, wqf, wqkv, wov, wguv, wdv, ag, pb, rd, sb, rr,
                 act, gcat, heads, gqkv, gbuf, hid, x0f, nrm1, nrm2, h1f, gh1f, inv, gact, qkvb, tabs, probs,
                 ag_s, ag_r, rs_s, rs_r, loc):
    chips = n_tp // 2
    seq = h_tok.shape[1]
    rows, dim = emb.shape
    ffn = wd.shape[0]
    blk = gh_in.shape[0]
    hd = wk.shape[1]
    scale = hd ** -0.5
    qw = local_heads * hd

    me = lax.axis_index('tp')
    chip = me // 2
    core = lax.rem(me, 2)
    sib = 2 * chip + 1 - core

    def peer_chip(d):
        return lax.rem(chip + d, chips)

    def peer(d):
        return 2 * peer_chip(d) + core

    order = sorted(range(1, chips), key=lambda d: -min(d, chips - d))

    barrier = pltpu.get_barrier_semaphore()
    for dev in [sib] + [peer(d) for d in range(1, chips)]:
        pl.semaphore_signal(barrier, inc=1, device_id={'tp': dev}, device_id_type=MESH)

    nloc = [1]

    def local(src, dst, slot=None):
        if slot is None:
            slot = nloc[0]
            nloc[0] += 1
        cp = pltpu.make_async_copy(src, dst, loc.at[slot])
        cp.start()
        return cp

    n_emb = RS_CHUNKS[R_EMB]
    ew = dim // n_emb

    def emb_load(j):
        return local(emb.at[:, pl.ds(j * ew, ew)], embv.at[:, pl.ds(j * ew, ew)])

    in_cp = [local(h_tok, tok)]
    emb_cp = [emb_load(0), emb_load(1)]
    in_cp += [local(a, b) for a, b in ((h_pos, pos), (h_invf, invf), (h_ga, ga), (h_gm, gm), (h_gh, gh_in))]
    in_cp[0].wait()

    tok_t = jnp.transpose(jnp.broadcast_to(tok[...].astype(F32), (seq, seq)))
    tok_t = tok_t - (me * rows).astype(F32)
    lane = lax.broadcasted_iota(jnp.int32, (seq, seq), 1).astype(F32)
    for b in range(rows // seq):
        onehot[:, b * seq:(b + 1) * seq] = jnp.where(tok_t == lane + float(b * seq), 1.0, 0.0).astype(BF)

    def remote(src, dst, s, r, dev):
        return pltpu.make_async_remote_copy(src_ref=src, dst_ref=dst, send_sem=s, recv_sem=r,
                                            device_id={'tp': dev}, device_id_type=MESH)

    def send(*args):
        remote(*args).start()

    near = sorted(range(1, chips), key=lambda d: min(d, chips - d))
    incoming = [(d, c) for d in near for c in (1, 0)]

    ag_set = {N1: 0, N2: 0, GH1: 0, GF: 0, GH: 1, GAIN: 1}

    def ag_ref(p, t):
        return gbuf.at[t] if p == GAIN else ag.at[p, t]

    def ag_block(p, d, c):
        return ag_ref(p, 2 * lax.rem(chip + chips - d, chips) + c)

    def ag_wait_sends(p):
        own = gbuf.at[pl.ds(0, chips)] if p == GAIN else ag.at[p, pl.ds(0, chips)]
        passed = gbuf.at[pl.ds(0, n_tp - 2)] if p == GAIN else ag.at[p, pl.ds(0, n_tp - 2)]
        remote(own, own, ag_s.at[ag_set[p], 0], ag_r.at[ag_set[p], 0], sib).wait_send()

        @pl.when(core == 1)
        def _():
            remote(passed, passed, ag_s.at[ag_set[p], 1], ag_r.at[ag_set[p], 0], sib).wait_send()

    @scoped('ag_start')
    def ag_start(p):
        mine = ag_ref(p, me)
        q = ag_set[p]
        for d in order:
            send(mine, mine, ag_s.at[q, 0], ag_r.at[q, 2 * d - core], 2 * peer_chip(d) + 1)
        send(mine, mine, ag_s.at[q, 0], ag_r.at[q, 0], sib)

    @scoped('ag_finish')
    def ag_finish(*ps):
        @pl.when(core == 1)
        def _():
            for d, c in incoming:
                for p in ps:
                    got = ag_block(p, d, c)
                    q = ag_set[p]
                    remote(got, got, ag_s.at[q, 1], ag_r.at[q, 2 * d - c], sib).wait_recv()
                    send(got, got, ag_s.at[q, 1], ag_r.at[q, 2 * d - c], sib)

        for p in ps:
            got = ag_ref(p, sib)
            remote(got, got, ag_s.at[ag_set[p], 0], ag_r.at[ag_set[p], 0], sib).wait_recv()

        @pl.when(core == 0)
        def _():
            for d, c in incoming:
                for p in ps:
                    got = ag_block(p, d, c)
                    remote(got, got, ag_s.at[ag_set[p], 1], ag_r.at[ag_set[p], 2 * d - c], sib).wait_recv()

    def gathered(p):
        return ag[p].reshape(seq, dim)

    rs_set = {R_EMB: 0, R_ATT: 0, R_GN2: 0, R_GN1: 0, R_MLP: 1}

    def rs_wait_sends(p):
        q = rs_set[p]
        remote(rd.at[p], rd.at[p], rs_s.at[q, 0], rs_r.at[q, 0, 0], sib).wait_send()
        remote(rr.at[p], rr.at[p], rs_s.at[q, 1], rs_r.at[q, 0, 0], sib).wait_send()

    def rs_cols(p, j):
        w = dim // RS_CHUNKS[p]
        return slice(j * w, (j + 1) * w)

    @scoped('rs_local')
    def rs_local(p, j, val):
        c = rs_cols(p, j)
        w = c.stop - c.start
        pb[p, :, :, :, c] = val.astype(BF).reshape(chips, 2, blk, w)
        send(pb.at[p, :, 1 - core, :, c], rd.at[p, :, :, c], rs_s.at[rs_set[p], 0], rs_r.at[rs_set[p], j, 0], sib)

    @scoped('rs_cross')
    def rs_cross(p, j):
        c = rs_cols(p, j)
        remote(rd.at[p, :, :, c], rd.at[p, :, :, c], rs_s.at[rs_set[p], 0], rs_r.at[rs_set[p], j, 0], sib).wait_recv()
        for d in order:
            to = peer_chip(d)
            both = pb[p, to, core, :, c].astype(F32) + rd[p, to, :, c].astype(F32)
            sb[p, to, :, c] = both.astype(BF)
            send(sb.at[p, to, :, c], rr.at[p, d - 1, :, c], rs_s.at[rs_set[p], 1], rs_r.at[rs_set[p], j, d], peer(d))

    @scoped('rs_finish')
    def rs_finish(p):
        parts = []
        for j in range(RS_CHUNKS[p]):
            c = rs_cols(p, j)
            total = pb[p, chip, core, :, c].astype(F32) + rd[p, chip, :, c].astype(F32)
            for d in order[::-1]:
                remote(rr.at[p, d - 1, :, c], rr.at[p, d - 1, :, c], rs_s.at[rs_set[p], 1], rs_r.at[rs_set[p], j, d], sib).wait_recv()
                total = total + rr[p, d - 1, :, c].astype(F32)
            parts.append(total)
        return jnp.concatenate(parts, axis=1)

    def rs_start(p, chunk):
        n = RS_CHUNKS[p]
        lag = 2 if n > 2 else 1
        for j in range(n + lag):
            if j < n:
                val = chunk(rs_cols(p, j))
                if p == R_EMB and j == 0:
                    with jax.named_scope('barrier'):
                        pl.semaphore_wait(barrier, chips)
                rs_local(p, j, val)
            if j >= lag:
                rs_cross(p, j - lag)

    def norm_fwd(x, gain):
        r = lax.rsqrt(jnp.mean(x * x, axis=-1, keepdims=True) + RMS_EPS)
        n = x * r
        return (n * gain).astype(BF), n, r

    def norm_bwd(g, n, r, gain):
        part = jnp.sum(g * n, axis=0, keepdims=True)
        scaled = g * gain
        return r * (scaled - n * jnp.mean(scaled * n, axis=-1, keepdims=True)), part

    w_cp = {}

    def emb_chunk(c):
        j = c.start // ew
        emb_cp[j].wait()
        if j + 2 < n_emb:
            emb_cp.append(emb_load(j + 2))
        if j == n_emb - 2:
            w_cp['k'] = local(wk, wqkv.at[:, pl.ds(qw, hd)])
            w_cp['v'] = local(wv, wqkv.at[:, pl.ds(qw + hd, hd)])
            w_cp['q'] = local(wq4, wqr)
            w_cp['o'] = local(wo, wov)
        if j == n_emb - 1:
            w_cp['d'] = local(wd, wdv)
            w_cp['g'] = local(wg, wguv.at[:, pl.ds(0, ffn)])
            w_cp['u'] = local(wu, wguv.at[:, pl.ds(ffn, ffn)])
        return dot(onehot[...], embv[:, c])

    rs_start(R_EMB, emb_chunk)

    in_cp[1].wait()
    in_cp[2].wait()
    pos_t = jnp.transpose(jnp.broadcast_to(pos[...].astype(F32), (seq, seq)))
    angle = pos_t * invf[...]
    half = lax.broadcasted_iota(jnp.int32, (seq, hd), 1) < hd // 2
    tabs[0] = jnp.cos(angle)
    sin = jnp.sin(angle)
    tabs[1] = jnp.where(half, -sin, sin)
    w_cp['q'].wait()
    wqf[...] = wqr[...].astype(F32)
    for h in range(local_heads):
        wqkv[:, h * hd:(h + 1) * hd] = wqf[pl.ds(h, dim, stride=local_heads), :].astype(BF)

    for cp in in_cp[3:]:
        cp.wait()
    x0 = rs_finish(R_EMB)
    x0f[...] = x0
    n1b, n1, r1 = norm_fwd(x0, ga[...])
    ag[N1, me] = n1b
    nrm1[...] = n1
    inv[0] = jnp.broadcast_to(r1, (blk, hd))
    ag_start(N1)
    ag[GH, me] = gh_in[...]
    w_cp['k'].wait()
    w_cp['v'].wait()
    ag_finish(N1)
    ag_start(GH)
    outs = []
    local(ag.at[N1], o_n1, 0)

    def rotate(v, sign):
        return v * tabs[0] + sign * (pltpu.roll(v, hd // 2, 1) * tabs[1])

    qkv = dot(gathered(N1), wqkv[...])
    for h in range(local_heads + 1):
        qkvb[:, h * hd:(h + 1) * hd] = rotate(qkv[:, h * hd:(h + 1) * hd], 1.0).astype(BF)
    qkvb[:, qw + hd:] = qkv[:, qw + hd:].astype(BF)
    kb = qkvb[:, qw:qw + hd]
    vb = qkvb[:, qw + hd:]
    causal = lax.broadcasted_iota(jnp.int32, (seq, seq), 0) >= lax.broadcasted_iota(jnp.int32, (seq, seq), 1)
    for h in range(local_heads):
        s = dot(qkvb[:, h * hd:(h + 1) * hd], kb, NT) * scale
        s = jnp.where(causal, s, -1e30)
        e = jnp.exp(s - jnp.max(s, axis=-1, keepdims=True))
        pr = e / jnp.sum(e, axis=-1, keepdims=True)
        probs[h] = pr
        heads[:, h * hd:(h + 1) * hd] = dot(pr.astype(BF), vb).astype(BF)
    w_cp['o'].wait()
    rs_wait_sends(R_EMB)
    rs_start(R_ATT, lambda c: dot(heads[...], wov[:, c]))
    outs.append(local(heads, o_heads))

    ag_finish(GH)
    local(ag.at[GH], o_gh, 0)
    w_cp['d'].wait()

    h1 = (x0f[...] + rs_finish(R_ATT).astype(BF).astype(F32)).astype(BF).astype(F32)
    h1f[...] = h1
    n2b, n2, r2 = norm_fwd(h1, gm[...])
    ag[N2, me] = n2b
    nrm2[...] = n2
    inv[1] = jnp.broadcast_to(r2, (blk, hd))
    ag_wait_sends(N1)
    ag_start(N2)
    with jax.named_scope('gact'):
        gact[...] = dot(gathered(GH), wdv[...], NT).astype(BF).astype(F32)
    w_cp['g'].wait()
    w_cp['u'].wait()
    ag_finish(N2)
    local(ag.at[N2], o_n2, 0)

    fw = 256
    for j in range(ffn // fw):
        c = slice(j * fw, (j + 1) * fw)
        cu = slice(ffn + j * fw, ffn + (j + 1) * fw)
        gate = dot(gathered(N2), wguv[:, c])
        up = dot(gathered(N2), wguv[:, cu])
        sig = jax.nn.sigmoid(gate)
        ga_act = gate * sig
        act[:, c] = (ga_act * up).astype(BF)
        g = gact[:, c]
        gcat[:, cu] = (g * ga_act).astype(BF)
        gcat[:, c] = (g * up * sig * (1.0 + gate * (1.0 - sig))).astype(BF)
    rs_wait_sends(R_ATT)
    rs_start(R_GN2, lambda c: dot(gcat[...], wguv[c, :], NT))
    outs.append(local(gcat, o_gcat))
    outs.append(local(act, o_act))
    for j in range(RS_CHUNKS[R_MLP]):
        rs_local(R_MLP, j, dot(act[...], wdv[:, rs_cols(R_MLP, j)]))

    gn2 = rs_finish(R_GN2).astype(BF).astype(F32)
    g_in, gain_part = norm_bwd(gn2, nrm2[...], inv[1][:, :1], gm[...])
    gbuf[me, 1:2, :] = gain_part
    gh1 = (gh_in[...].astype(F32) + g_in).astype(BF)
    gh1f[...] = gh1.astype(F32)
    ag[GH1, me] = gh1
    ag_wait_sends(N2)
    ag_start(GH1)
    ag_finish(GH1)
    for j in range(RS_CHUNKS[R_MLP]):
        rs_cross(R_MLP, j)
    local(ag.at[GH1], o_gh1, 0)

    ghd = dot(gathered(GH1), wov[...], NT).astype(BF)
    gv = jnp.zeros((seq, hd), F32)
    gk = jnp.zeros((seq, hd), F32)
    for h in range(local_heads):
        g = ghd[:, h * hd:(h + 1) * hd]
        pr = probs[h]
        gp = dot(g, vb, NT).astype(BF).astype(F32)
        gv = gv + dot(pr.astype(BF), g, TN)
        gs = (pr * (gp - jnp.sum(gp * pr, axis=-1, keepdims=True)) * scale).astype(BF)
        gq = dot(gs, kb).astype(BF).astype(F32)
        gk = gk + dot(gs, qkvb[:, h * hd:(h + 1) * hd], TN)
        gqkv[:, h * hd:(h + 1) * hd] = rotate(gq, -1.0).astype(BF)
    gqkv[:, qw:qw + hd] = rotate(gk.astype(BF).astype(F32), -1.0).astype(BF)
    gqkv[:, qw + hd:] = gv.astype(BF)
    rs_wait_sends(R_GN2)
    rs_start(R_GN1, lambda c: dot(gqkv[...], wqkv[c, :], NT))
    outs.append(local(gqkv, o_gqkv))
    hid[...] = (h1f[...] + rs_finish(R_MLP).astype(BF).astype(F32)).astype(BF)
    outs.append(local(hid, o_hid))

    gn1 = rs_finish(R_GN1).astype(BF).astype(F32)
    g_in, gain_part = norm_bwd(gn1, nrm1[...], inv[0][:, :1], ga[...])
    gbuf[me, 0:1, :] = gain_part
    ag[GF, me] = (gh1f[...] + g_in).astype(BF)
    ag_wait_sends(GH)
    ag_wait_sends(GH1)
    ag_start(GAIN)
    ag_start(GF)
    ag_finish(GAIN, GF)
    local(ag.at[GF], o_gf, 0)
    outs.append(local(gbuf, o_gain))
    with jax.named_scope('tail_send'):
        rs_wait_sends(R_GN1)
        rs_wait_sends(R_MLP)
        ag_wait_sends(GAIN)
        ag_wait_sends(GF)

    with jax.named_scope('tail_out'):
        for cp in outs:
            cp.wait()
        pltpu.make_async_copy(ag, ag, loc.at[0]).wait()


def grads_kernel(n_tp, local_heads,
                 h_tok, h_gain, h_hid, h_gh, h_act, h_n2, h_gcat, h_gh1, h_heads, h_n1, h_gqkv, h_gf,
                 o_hid, o_emb, o_wq, o_wk, o_wv, o_wo, o_wg, o_wu, o_wd, o_ga, o_gm,
                 tok, gain, hid, gains, gh, act, n2, gcat, gh1, heads, n1, gqkv, gf, wide, tall, qbuf, kvbuf, s_in, s_wide, s_tall, s_qkv, s_out):
    seq, dim = n1.shape
    rows = o_emb.shape[0]
    ffn = act.shape[1]
    hd = gqkv.shape[1] // (local_heads + 2)
    me = lax.axis_index('tp')
    n_wide, wr = wide.shape[0], wide.shape[1]
    n_tall, tr = tall.shape[0], tall.shape[1]
    busy = {}

    def put(key, src, dst, sem):
        cp = pltpu.make_async_copy(src, dst, sem)
        cp.start()
        busy[key] = cp

    def free(key):
        if key in busy:
            busy.pop(key).wait()

    fetch = ('act', 'gh', 'n2', 'gcat', 'tok', 'gh1', 'heads', 'gf', 'n1', 'gqkv', 'gain', 'hid')
    pairs = ((h_act, act), (h_gh, gh), (h_n2, n2), (h_gcat, gcat), (h_tok, tok), (h_gh1, gh1), (h_heads, heads), (h_gf, gf), (h_n1, n1), (h_gqkv, gqkv),
             (h_gain, gain), (h_hid, hid))
    loaded = [0]

    def load_to(name):
        while loaded[0] <= fetch.index(name):
            i = loaded[0]
            put(('in', fetch[i]), pairs[i][0], pairs[i][1], s_in.at[i])
            loaded[0] += 1

    def use(*wanted):
        for n in wanted:
            load_to(n)
        for n in wanted:
            free(('in', n))

    load_to('gcat')
    row = lax.broadcasted_iota(jnp.int32, (wr, seq), 0)
    wide_units = []
    for u in range(ffn // wr):
        wide_units.append((('gh', 'act'), lambda u=u: dot(act[:, u * wr:(u + 1) * wr], gh[...], TN), o_wd.at[pl.ds(u * wr, wr)]))
    for u in range(heads.shape[1] // wr):
        wide_units.append((('gh1', 'heads'), lambda u=u: dot(heads[:, u * wr:(u + 1) * wr], gh1[...], TN), o_wo.at[pl.ds(u * wr, wr)]))
    for u in range(rows // wr):
        wide_units.append((('gf', 'tok'), lambda u=u: dot(jnp.where(row + u * wr == tok[...] - me * rows, 1.0, 0.0).astype(BF), gf[...]),
                           o_emb.at[pl.ds(u * wr, wr)]))
    tall_units = []
    for half, out in ((0, o_wg), (1, o_wu)):
        for u in range(dim // tr):
            tall_units.append((('n2', 'gcat'), lambda u=u, half=half: dot(n2[:, u * tr:(u + 1) * tr], gcat[:, half * ffn:(half + 1) * ffn], TN),
                               out.at[pl.ds(u * tr, tr)]))
    iw = it = 0
    while iw < len(wide_units) or it < len(tall_units):
        if iw < len(wide_units):
            slot = iw % n_wide
            names, fn, dst = wide_units[iw]
            use(*names)
            free(('w', slot))
            with jax.named_scope(f'wide_{iw}'):
                wide[slot] = fn()
                put(('w', slot), wide.at[slot], dst, s_wide.at[slot])
            iw += 1
            if iw == 1:
                load_to('hid')
        if it < len(tall_units):
            slot = it % n_tall
            names, fn, dst = tall_units[it]
            use(*names)
            free(('t', slot))
            with jax.named_scope(f'tall_{it}'):
                tall[slot] = fn()
                put(('t', slot), tall.at[slot], dst, s_tall.at[slot])
            it += 1
    use('gain', 'hid')
    total = gain[0]
    for t in range(1, n_tp):
        total = total + gain[t]
    gains[...] = total
    put(('out', 0), hid, o_hid, s_out.at[0])
    put(('out', 1), gains.at[pl.ds(0, 1)], o_ga, s_out.at[1])
    put(('out', 2), gains.at[pl.ds(1, 1)], o_gm, s_out.at[2])
    qw = local_heads * hd
    use('n1', 'gqkv')
    with jax.named_scope('qkv'):
        for h in range(local_heads):
            qbuf[pl.ds(h, dim, stride=local_heads), :] = dot(n1[...], gqkv[:, h * hd:(h + 1) * hd], TN)
        put(('q', 0), qbuf, o_wq, s_qkv.at[2])
        for i, out in enumerate((o_wk, o_wv)):
            kvbuf[i] = dot(n1[...], gqkv[:, qw + i * hd:qw + (i + 1) * hd], TN)
            put(('k', i), kvbuf.at[i], out, s_qkv.at[i])

    with jax.named_scope('drain'):
        for key in list(busy):
            free(key)


def solution(mesh):
    n_tp = mesh.shape['tp']
    chips = n_tp // 2
    in_specs = (P('dp', None), P('dp', None), P('tp', None), P(None), P(None),
                P(None, 'tp', None), P(None, 'tp', None), P(None, 'tp', None), P('tp', None, None),
                P(None, 'tp'), P(None, 'tp'), P('tp', None), P('dp', 'tp', None))
    out_specs = (P('dp', 'tp', None), P(('dp', 'tp'), None),
                 P('dp', 'tp', None), P('dp', 'tp', None), P('dp', 'tp', None), P(('dp', 'tp'), None, None),
                 P('dp', 'tp'), P('dp', 'tp'), P(('dp', 'tp'), None), P('dp'), P('dp'))

    def device_fn(tokens, positions, emb, gain_attn, gain_mlp, w_query, w_key, w_value, w_out, w_gate, w_up, w_down, grad_hidden):
        seq = tokens.shape[1]
        rows, dim = emb.shape
        lh, hd = w_query.shape[1], w_query.shape[2]
        ffn = w_down.shape[0]
        blk = grad_hidden.shape[1]
        qkvw = (lh + 2) * hd
        inv_freq = (np.float32(ROPE_THETA) ** (-np.arange(hd // 2, dtype=np.float32) * np.float32(2.0 / hd))).astype(np.float32)
        invf = jnp.asarray(np.concatenate([inv_freq, inv_freq])[None, :])

        def sds(shape, dt=BF):
            return jax.ShapeDtypeStruct(shape, dt)

        hb = pl.BlockSpec(memory_space=pl.ANY)
        maxc = max(RS_CHUNKS.values())
        mid = pl.pallas_call(
            functools.partial(layer_kernel, n_tp, lh),
            name='layer',
            out_shape=[sds((n_tp, blk, dim))] * 5 + [sds((seq, ffn)), sds((seq, 2 * ffn)), sds((seq, lh * hd)), sds((seq, qkvw)),
                                                    sds((n_tp, 2, dim), F32), sds((blk, dim))],
            in_specs=[hb] * 14,
            out_specs=[hb] * 11,
            scratch_shapes=[
                pltpu.VMEM((1, seq), jnp.int32), pltpu.VMEM((1, seq), jnp.int32), pltpu.VMEM((1, hd), F32),
                pltpu.VMEM((1, dim), F32), pltpu.VMEM((1, dim), F32), pltpu.VMEM((blk, dim), BF),
                pltpu.VMEM((rows, dim), BF), pltpu.VMEM((seq, rows), BF), pltpu.VMEM((dim * lh, hd), BF), pltpu.VMEM((dim * lh, hd), F32),
                pltpu.VMEM((dim, qkvw), BF), pltpu.VMEM((lh * hd, dim), BF), pltpu.VMEM((dim, 2 * ffn), BF), pltpu.VMEM((ffn, dim), BF),
                pltpu.VMEM((5, n_tp, blk, dim), BF), pltpu.VMEM((5, chips, 2, blk, dim), BF), pltpu.VMEM((5, chips, blk, dim), BF),
                pltpu.VMEM((5, chips, blk, dim), BF), pltpu.VMEM((5, chips - 1, blk, dim), BF),
                pltpu.VMEM((seq, ffn), BF), pltpu.VMEM((seq, 2 * ffn), BF), pltpu.VMEM((seq, lh * hd), BF), pltpu.VMEM((seq, qkvw), BF),
                pltpu.VMEM((n_tp, 2, dim), F32), pltpu.VMEM((blk, dim), BF),
                pltpu.VMEM((blk, dim), F32), pltpu.VMEM((blk, dim), F32), pltpu.VMEM((blk, dim), F32), pltpu.VMEM((blk, dim), F32),
                pltpu.VMEM((blk, dim), F32), pltpu.VMEM((2, blk, hd), F32), pltpu.VMEM((seq, ffn), F32), pltpu.VMEM((seq, qkvw), BF),
                pltpu.VMEM((2, seq, hd), F32), pltpu.VMEM((lh, seq, seq), F32),
                pltpu.SemaphoreType.DMA((2, 2)), pltpu.SemaphoreType.DMA((2, 2 * chips - 1)),
                pltpu.SemaphoreType.DMA((2, 2)), pltpu.SemaphoreType.DMA((2, maxc, chips)),
                pltpu.SemaphoreType.DMA((24,)),
            ],
            compiler_params=pltpu.CompilerParams(collective_id=0, has_side_effects=True, vmem_limit_bytes=64 * 1024 * 1024 - 65536),
        )(tokens, positions, invf, gain_attn.reshape(1, dim), gain_mlp.reshape(1, dim), grad_hidden.reshape(blk, dim),
          emb, w_query.reshape(dim * lh, hd), w_key.reshape(dim, hd), w_value.reshape(dim, hd), w_out.reshape(lh * hd, dim),
          w_gate, w_up, w_down)
        n1, n2, gh, gh1, gf, act, gcat, heads, gqkv, gain, hid = mid
        n1, n2, gh, gh1, gf = (a.reshape(seq, dim) for a in (n1, n2, gh, gh1, gf))
        wide_rows, tall_rows = 256, 512
        res = pl.pallas_call(
            functools.partial(grads_kernel, n_tp, lh),
            name='grads',
            out_shape=[sds((blk, dim)), sds((rows, dim), F32), sds((dim * lh, hd), F32), sds((dim, hd), F32), sds((dim, hd), F32),
                       sds((lh * hd, dim), F32), sds((dim, ffn), F32), sds((dim, ffn), F32), sds((ffn, dim), F32),
                       sds((1, dim), F32), sds((1, dim), F32)],
            in_specs=[hb] * 12,
            out_specs=[hb] * 11,
            scratch_shapes=[
                pltpu.VMEM((1, seq), jnp.int32), pltpu.VMEM((n_tp, 2, dim), F32), pltpu.VMEM((blk, dim), BF), pltpu.VMEM((2, dim), F32),
                pltpu.VMEM((seq, dim), BF), pltpu.VMEM((seq, ffn), BF), pltpu.VMEM((seq, dim), BF), pltpu.VMEM((seq, 2 * ffn), BF),
                pltpu.VMEM((seq, dim), BF), pltpu.VMEM((seq, lh * hd), BF), pltpu.VMEM((seq, dim), BF), pltpu.VMEM((seq, qkvw), BF),
                pltpu.VMEM((seq, dim), BF),
                pltpu.VMEM((3, wide_rows, dim), F32), pltpu.VMEM((3, tall_rows, ffn), F32), pltpu.VMEM((dim * lh, hd), F32),
                pltpu.VMEM((2, dim, hd), F32),
                pltpu.SemaphoreType.DMA((12,)), pltpu.SemaphoreType.DMA((3,)), pltpu.SemaphoreType.DMA((3,)), pltpu.SemaphoreType.DMA((3,)),
                pltpu.SemaphoreType.DMA((3,)),
            ],
            compiler_params=pltpu.CompilerParams(vmem_limit_bytes=60 * 1024 * 1024),
        )(tokens, gain, hid, gh, act, n2, gcat, gh1, heads, n1, gqkv, gf)
        o_hid, o_emb, o_wq, o_wk, o_wv, o_wo, o_wg, o_wu, o_wd, o_ga, o_gm = res
        return (o_hid.reshape(1, blk, dim), o_emb, o_wq.reshape(dim, lh, hd), o_wk.reshape(dim, 1, hd), o_wv.reshape(dim, 1, hd),
                o_wo.reshape(lh, hd, dim), o_wg, o_wu, o_wd, o_ga.reshape(dim), o_gm.reshape(dim))

    return jax.shard_map(device_fn, mesh=mesh, in_specs=in_specs, out_specs=out_specs, check_vma=False)
```

```python
import functools

import jax
import jax.numpy as jnp
import numpy as np
from jax import lax
from jax.experimental import pallas as pl
from jax.experimental.pallas import tpu as pltpu
from jax.sharding import PartitionSpec as P

ROPE_THETA = 1000000.0
RMS_EPS = 1e-5
MESH = pl.DeviceIdType.MESH
BF = jnp.bfloat16
F32 = jnp.float32
NT = (((1,), (1,)), ((), ()))
TN = (((0,), (0,)), ((), ()))

N1, GH, N2, GH1, GF, GAIN_M, GAIN_A = range(7)
R_EMB, R_ATT, R_GN2, R_MLP, R_GN1 = range(5)
RS_CHUNKS = {R_EMB: 4, R_ATT: 2, R_GN2: 4, R_MLP: 2, R_GN1: 2}
AG_CHUNKS = {N1: 2, GH: 1, N2: 1, GH1: 2, GF: 1, GAIN_M: 1, GAIN_A: 1}


def dot(a, b, dims=(((1,), (0,)), ((), ()))):
    return lax.dot_general(a, b, dims, preferred_element_type=F32)


def scoped(name):
    def wrap(fn):
        def run(p, *rest, **kw):
            with jax.named_scope(f'{name}_{p}'):
                return fn(p, *rest, **kw)
        return run
    return wrap


def layer_kernel(n_tp, local_heads,
                 h_tok, h_pos, h_invf, h_ga, h_gm, h_gh, emb, wq4, wk, wv, wo, wg, wu, wd,
                 o_n1, o_n2, o_gh, o_gh1, o_gf, act, gcat, heads, gqkv, gain_m, gain_a, hid,
                 tok, pos, invf, ga, gm, gh_in, embv, onehot, wqr, wqf, wqkv, wov, wguv, wdv, pb, rd, sb, rr,
                 wgut, wqkvt, x0f, nrm1, nrm2, h1f, gh1f, inv, gact, qkvb, tabs, probs,
                 ag_s, ag_r, rs_s, rs_r, loc):
    chips = n_tp // 2
    seq = h_tok.shape[1]
    rows, dim = emb.shape
    ffn = wd.shape[0]
    blk = gh_in.shape[0]
    hd = wk.shape[1]
    scale = hd ** -0.5
    qw = local_heads * hd

    me = lax.axis_index('tp')
    chip = me // 2
    core = lax.rem(me, 2)
    sib = 2 * chip + 1 - core

    def peer_chip(d):
        return lax.rem(chip + d, chips)

    def peer(d):
        return 2 * peer_chip(d) + core

    order = sorted(range(1, chips), key=lambda d: -min(d, chips - d))

    barrier = pltpu.get_barrier_semaphore()
    for dev in [sib] + [peer(d) for d in range(1, chips)]:
        pl.semaphore_signal(barrier, inc=1, device_id={'tp': dev}, device_id_type=MESH)

    nloc = [1]

    def local(src, dst, slot=None):
        if slot is None:
            slot = nloc[0]
            nloc[0] += 1
        cp = pltpu.make_async_copy(src, dst, loc.at[slot])
        cp.start()
        return cp

    n_emb = RS_CHUNKS[R_EMB]
    ew = dim // n_emb

    def emb_load(j):
        return local(emb.at[:, pl.ds(j * ew, ew)], embv.at[:, pl.ds(j * ew, ew)])

    in_cp = [local(h_tok, tok)]
    emb_cp = [emb_load(0), emb_load(1)]
    in_cp += [local(a, b) for a, b in ((h_pos, pos), (h_invf, invf), (h_ga, ga), (h_gm, gm), (h_gh, gh_in))]
    in_cp[0].wait()

    tok_t = jnp.transpose(jnp.broadcast_to(tok[...].astype(F32), (seq, seq)))
    tok_t = tok_t - (me * rows).astype(F32)
    lane = lax.broadcasted_iota(jnp.int32, (seq, seq), 1).astype(F32)
    for b in range(rows // seq):
        onehot[:, b * seq:(b + 1) * seq] = jnp.where(tok_t == lane + float(b * seq), 1.0, 0.0).astype(BF)

    def remote(src, dst, s, r, dev):
        return pltpu.make_async_remote_copy(src_ref=src, dst_ref=dst, send_sem=s, recv_sem=r,
                                            device_id={'tp': dev}, device_id_type=MESH)

    def send(*args):
        remote(*args).start()

    near = sorted(range(1, chips), key=lambda d: min(d, chips - d))
    incoming = [(d, c) for d in near for c in (1, 0)]

    ag_set = {N1: 0, N2: 0, GH1: 0, GF: 0, GH: 1, GAIN_M: 1, GAIN_A: 1}
    ag = {N1: o_n1, GH: o_gh, N2: o_n2, GH1: o_gh1, GF: o_gf, GAIN_M: gain_m, GAIN_A: gain_a}
    per = 2 * chips - 1

    def ag_view(p, t, j):
        w = dim // AG_CHUNKS[p]
        return ag[p].at[t, :, pl.ds(j * w, w)]

    def ag_block(p, d, c, j):
        return ag_view(p, 2 * lax.rem(chip + chips - d, chips) + c, j)

    def ag_recv(p, j, i):
        return ag_r.at[(per * j if ag_set[p] == 0 else ag_r.shape[0] - per) + i]

    def ag_wait_sends(p):
        own, passed = ag[p].at[pl.ds(0, chips)], ag[p].at[pl.ds(0, n_tp - 2)]
        remote(own, own, ag_s.at[ag_set[p], 0], ag_recv(p, 0, 0), sib).wait_send()

        @pl.when(core == 1)
        def _():
            remote(passed, passed, ag_s.at[ag_set[p], 1], ag_recv(p, 0, 0), sib).wait_send()

    @scoped('ag_start')
    def ag_start(p):
        q = ag_set[p]
        for j in range(AG_CHUNKS[p]):
            mine = ag_view(p, me, j)
            for d in order:
                send(mine, mine, ag_s.at[q, 0], ag_recv(p, j, 2 * d - core), 2 * peer_chip(d) + 1)
            send(mine, mine, ag_s.at[q, 0], ag_recv(p, j, 0), sib)

    @scoped('ag_finish')
    def ag_finish(j, *ps, early=None, forward=True, collect=True):
        if j == 0 and forward:
            @pl.when(core == 1)
            def _():
                for k in range(AG_CHUNKS[ps[0]]):
                    for d, c in incoming:
                        for p in ps:
                            got = ag_block(p, d, c, k)
                            q = ag_set[p]
                            remote(got, got, ag_s.at[q, 1], ag_recv(p, k, 2 * d - c), sib).wait_recv()
                            send(got, got, ag_s.at[q, 1], ag_recv(p, k, 2 * d - c), sib)

        if not collect:
            return
        for p in ps:
            got = ag_view(p, sib, j)
            remote(got, got, ag_s.at[ag_set[p], 0], ag_recv(p, j, 0), sib).wait_recv()

        @pl.when(core == 0)
        def _():
            for i, (d, c) in enumerate(incoming):
                if i == 2 and early is not None:
                    early()
                for p in ps:
                    got = ag_block(p, d, c, j)
                    remote(got, got, ag_s.at[ag_set[p], 1], ag_recv(p, j, 2 * d - c), sib).wait_recv()

    def gathered(p, j=None):
        if j is None:
            return ag[p][...].reshape(seq, dim)
        w = dim // AG_CHUNKS[p]
        return ag[p][:, :, j * w:(j + 1) * w].reshape(seq, w)

    def gathered_dot(p, weight, early):
        w = dim // AG_CHUNKS[p]
        total = None
        for j in range(AG_CHUNKS[p]):
            ag_finish(j, p, early=early if j == 0 else None)
            part = weight(gathered(p, j), slice(j * w, (j + 1) * w))
            total = part if total is None else total + part
        return total

    rs_set = {R_EMB: 0, R_ATT: 0, R_GN2: 0, R_GN1: 0, R_MLP: 1}

    def rs_wait_sends(p):
        q = rs_set[p]
        remote(rd.at[p], rd.at[p], rs_s.at[q, 0], rs_r.at[q, 0, 0], sib).wait_send()
        remote(rr.at[p], rr.at[p], rs_s.at[q, 1], rs_r.at[q, 0, 0], sib).wait_send()

    def rs_cols(p, j):
        w = dim // RS_CHUNKS[p]
        return slice(j * w, (j + 1) * w)

    @scoped('rs_local')
    def rs_local(p, j, val):
        c = rs_cols(p, j)
        w = c.stop - c.start
        pb[p, :, :, :, c] = val.astype(BF).reshape(chips, 2, blk, w)
        send(pb.at[p, :, 1 - core, :, c], rd.at[p, :, :, c], rs_s.at[rs_set[p], 0], rs_r.at[rs_set[p], j, 0], sib)

    @scoped('rs_cross')
    def rs_cross(p, j):
        c = rs_cols(p, j)
        remote(rd.at[p, :, :, c], rd.at[p, :, :, c], rs_s.at[rs_set[p], 0], rs_r.at[rs_set[p], j, 0], sib).wait_recv()
        for d in order:
            to = peer_chip(d)
            both = pb[p, to, core, :, c].astype(F32) + rd[p, to, :, c].astype(F32)
            sb[p, to, :, c] = both.astype(BF)
            send(sb.at[p, to, :, c], rr.at[p, d - 1, :, c], rs_s.at[rs_set[p], 1], rs_r.at[rs_set[p], j, d], peer(d))

    @scoped('rs_finish')
    def rs_finish(p):
        parts = []
        for j in range(RS_CHUNKS[p]):
            c = rs_cols(p, j)
            total = pb[p, chip, core, :, c].astype(F32) + rd[p, chip, :, c].astype(F32)
            for d in order[::-1]:
                remote(rr.at[p, d - 1, :, c], rr.at[p, d - 1, :, c], rs_s.at[rs_set[p], 1], rs_r.at[rs_set[p], j, d], sib).wait_recv()
                total = total + rr[p, d - 1, :, c].astype(F32)
            parts.append(total)
        return jnp.concatenate(parts, axis=1)

    def rs_start(p, chunk):
        n = RS_CHUNKS[p]
        for j in range(n):
            val = chunk(rs_cols(p, j))
            if p == R_EMB and j == 0:
                with jax.named_scope('barrier'):
                    pl.semaphore_wait(barrier, chips)
            rs_local(p, j, val)
            if j > 0:
                @pl.when(core == 0)
                def _():
                    rs_cross(p, j - 1)

        @pl.when(core == 0)
        def _():
            rs_cross(p, n - 1)

        @pl.when(core == 1)
        def _():
            for j in range(n):
                rs_cross(p, j)

    def on_core(k, fn):
        @pl.when(core == k)
        def _():
            fn()

    def norm_fwd(x, gain):
        r = lax.rsqrt(jnp.mean(x * x, axis=-1, keepdims=True) + RMS_EPS)
        n = x * r
        return (n * gain).astype(BF), n, r

    def norm_bwd(g, n, r, gain):
        part = jnp.sum(g * n, axis=0, keepdims=True)
        scaled = g * gain
        return r * (scaled - n * jnp.mean(scaled * n, axis=-1, keepdims=True)), part

    w_cp = {}

    def emb_chunk(c):
        j = c.start // ew
        emb_cp[j].wait()
        if j + 2 < n_emb:
            emb_cp.append(emb_load(j + 2))
        if j == n_emb - 2:
            w_cp['g'] = local(wg, wguv.at[:, pl.ds(0, ffn)])
            w_cp['u'] = local(wu, wguv.at[:, pl.ds(ffn, ffn)])
        if j == n_emb - 1:
            w_cp['k'] = local(wk, wqkv.at[:, pl.ds(qw, hd)])
            w_cp['v'] = local(wv, wqkv.at[:, pl.ds(qw + hd, hd)])
            w_cp['q'] = local(wq4, wqr)
            w_cp['o'] = local(wo, wov)
            w_cp['d'] = local(wd, wdv)
        return dot(onehot[...], embv[:, c])

    rs_start(R_EMB, emb_chunk)

    tw = 256
    eye = (lax.broadcasted_iota(jnp.int32, (tw, tw), 0) == lax.broadcasted_iota(jnp.int32, (tw, tw), 1)).astype(F32).astype(BF)
    w_cp['g'].wait()
    w_cp['u'].wait()
    with jax.named_scope('wgut'):
        for b in range(2 * ffn // tw):
            wgut[b * tw:(b + 1) * tw, :] = dot(eye, wguv[:, b * tw:(b + 1) * tw], NT).astype(BF)

    for cp in in_cp[3:]:
        cp.wait()
    x0 = rs_finish(R_EMB)
    x0f[...] = x0
    n1b, n1, r1 = norm_fwd(x0, ga[...])
    o_n1[me] = n1b
    nrm1[...] = n1
    inv[0] = jnp.broadcast_to(r1, (blk, hd))
    ag_start(N1)
    o_gh[me] = gh_in[...]
    w_cp['k'].wait()
    w_cp['v'].wait()
    in_cp[1].wait()
    in_cp[2].wait()
    pos_t = jnp.transpose(jnp.broadcast_to(pos[...].astype(F32), (seq, seq)))
    angle = pos_t * invf[...]
    half = lax.broadcasted_iota(jnp.int32, (seq, hd), 1) < hd // 2
    tabs[0] = jnp.cos(angle)
    sin = jnp.sin(angle)
    tabs[1] = jnp.where(half, -sin, sin)
    w_cp['q'].wait()
    wqf[...] = wqr[...].astype(F32)
    for h in range(local_heads):
        wqkv[:, h * hd:(h + 1) * hd] = wqf[pl.ds(h, dim, stride=local_heads), :].astype(BF)


    with jax.named_scope('wqkvt'):
        for b in range((qw + 2 * hd) // tw):
            wqkvt[b * tw:(b + 1) * tw, :] = dot(eye, wqkv[:, b * tw:(b + 1) * tw], NT).astype(BF)

    def rotate(v, sign):
        return v * tabs[0] + sign * (pltpu.roll(v, hd // 2, 1) * tabs[1])

    qkv = gathered_dot(N1, lambda a, k: dot(a, wqkv[k, :]), lambda: ag_start(GH))
    on_core(1, lambda: ag_start(GH))
    for h in range(local_heads + 1):
        qkvb[:, h * hd:(h + 1) * hd] = rotate(qkv[:, h * hd:(h + 1) * hd], 1.0).astype(BF)
    qkvb[:, qw + hd:] = qkv[:, qw + hd:].astype(BF)
    kb = qkvb[:, qw:qw + hd]
    vb = qkvb[:, qw + hd:]
    causal = lax.broadcasted_iota(jnp.int32, (seq, seq), 0) >= lax.broadcasted_iota(jnp.int32, (seq, seq), 1)
    for h in range(local_heads):
        s = dot(qkvb[:, h * hd:(h + 1) * hd], kb, NT) * scale
        s = jnp.where(causal, s, -1e30)
        e = jnp.exp(s - jnp.max(s, axis=-1, keepdims=True))
        pr = e / jnp.sum(e, axis=-1, keepdims=True)
        probs[h] = pr
        heads[:, h * hd:(h + 1) * hd] = dot(pr.astype(BF), vb).astype(BF)
    w_cp['o'].wait()
    rs_wait_sends(R_EMB)
    rs_start(R_ATT, lambda c: dot(heads[...], wov[:, c]))

    ag_finish(0, GH)
    w_cp['d'].wait()

    h1 = (x0f[...] + rs_finish(R_ATT).astype(BF).astype(F32)).astype(BF).astype(F32)
    h1f[...] = h1
    n2b, n2, r2 = norm_fwd(h1, gm[...])
    o_n2[me] = n2b
    nrm2[...] = n2
    inv[1] = jnp.broadcast_to(r2, (blk, hd))
    ag_wait_sends(N1)
    ag_start(N2)
    with jax.named_scope('gact'):
        gact[...] = dot(gathered(GH), wdv[...], NT).astype(BF).astype(F32)

    ag_finish(0, N2)
    fw = 256
    for j in range(ffn // fw):
        c = slice(j * fw, (j + 1) * fw)
        cu = slice(ffn + j * fw, ffn + (j + 1) * fw)
        gate = dot(gathered(N2), wguv[:, c])
        up = dot(gathered(N2), wguv[:, cu])
        sig = jax.nn.sigmoid(gate)
        ga_act = gate * sig
        act[:, c] = (ga_act * up).astype(BF)
        g = gact[:, c]
        gcat[:, cu] = (g * ga_act).astype(BF)
        gcat[:, c] = (g * up * sig * (1.0 + gate * (1.0 - sig))).astype(BF)
    rs_wait_sends(R_ATT)
    rs_start(R_GN2, lambda c: dot(gcat[...], wgut[:, c]))
    for j in range(RS_CHUNKS[R_MLP]):
        rs_local(R_MLP, j, dot(act[...], wdv[:, rs_cols(R_MLP, j)]))

    gn2 = rs_finish(R_GN2).astype(BF).astype(F32)
    g_in, gain_part = norm_bwd(gn2, nrm2[...], inv[1][:, :1], gm[...])
    gain_m[me] = gain_part
    gh1 = (gh_in[...].astype(F32) + g_in).astype(BF)
    gh1f[...] = gh1.astype(F32)
    o_gh1[me] = gh1
    ag_wait_sends(N2)
    ag_start(GH1)
    ag_wait_sends(GH)
    ag_start(GAIN_M)
    def mlp_cross():
        for j in range(RS_CHUNKS[R_MLP]):
            rs_cross(R_MLP, j)

    ghd = gathered_dot(GH1, lambda a, k: dot(a, wov[:, k], NT), mlp_cross).astype(BF)
    on_core(1, mlp_cross)
    ag_finish(0, GAIN_M, collect=False)

    gv = jnp.zeros((seq, hd), F32)
    gk = jnp.zeros((seq, hd), F32)
    for h in range(local_heads):
        g = ghd[:, h * hd:(h + 1) * hd]
        pr = probs[h]
        gp = dot(g, vb, NT).astype(BF).astype(F32)
        gv = gv + dot(pr.astype(BF), g, TN)
        gs = (pr * (gp - jnp.sum(gp * pr, axis=-1, keepdims=True)) * scale).astype(BF)
        gq = dot(gs, kb).astype(BF).astype(F32)
        gk = gk + dot(gs, qkvb[:, h * hd:(h + 1) * hd], TN)
        gqkv[:, h * hd:(h + 1) * hd] = rotate(gq, -1.0).astype(BF)
    gqkv[:, qw:qw + hd] = rotate(gk.astype(BF).astype(F32), -1.0).astype(BF)
    gqkv[:, qw + hd:] = gv.astype(BF)
    ag_finish(0, GAIN_M, forward=False)
    rs_wait_sends(R_GN2)
    rs_start(R_GN1, lambda c: dot(gqkv[...], wqkvt[:, c]))
    hid[...] = (h1f[...] + rs_finish(R_MLP).astype(BF).astype(F32)).astype(BF)

    gn1 = rs_finish(R_GN1).astype(BF).astype(F32)
    g_in, gain_part = norm_bwd(gn1, nrm1[...], inv[0][:, :1], ga[...])
    gain_a[me] = gain_part
    o_gf[me] = (gh1f[...] + g_in).astype(BF)
    ag_wait_sends(GAIN_M)
    ag_wait_sends(GH1)
    ag_start(GAIN_A)
    ag_start(GF)
    ag_finish(0, GAIN_A, GF)
    with jax.named_scope('tail_send'):
        rs_wait_sends(R_GN1)
        rs_wait_sends(R_MLP)
        ag_wait_sends(GAIN_A)
        ag_wait_sends(GF)


def grads_kernel(n_tp, local_heads,
                 tok, gain_m, gain_a, hid, gh, act, n2, gcat, gh1, heads, n1, gqkv, gf,
                 o_hid, o_emb, o_wq, o_wk, o_wv, o_wo, o_wg, o_wu, o_wd, o_ga, o_gm,
                 gains, wide, tall, qbuf, kvbuf, s_wide, s_tall, s_qkv, s_out):
    seq, dim = n1.shape
    rows = o_emb.shape[0]
    ffn = act.shape[1]
    hd = gqkv.shape[1] // (local_heads + 2)
    me = lax.axis_index('tp')
    n_wide, wr = wide.shape[0], wide.shape[1]
    n_tall, tr = tall.shape[0], tall.shape[1]
    busy = {}

    def put(key, src, dst, sem):
        cp = pltpu.make_async_copy(src, dst, sem)
        cp.start()
        busy[key] = cp

    def free(key):
        if key in busy:
            busy.pop(key).wait()

    row = lax.broadcasted_iota(jnp.int32, (wr, seq), 0)
    wide_units = []
    for u in range(ffn // wr):
        wide_units.append((lambda u=u: dot(act[:, u * wr:(u + 1) * wr], gh[...], TN), o_wd.at[pl.ds(u * wr, wr)]))
    for u in range(heads.shape[1] // wr):
        wide_units.append((lambda u=u: dot(heads[:, u * wr:(u + 1) * wr], gh1[...], TN), o_wo.at[pl.ds(u * wr, wr)]))
    for u in range(rows // wr):
        wide_units.append((lambda u=u: dot(jnp.where(row + u * wr == tok[...] - me * rows, 1.0, 0.0).astype(BF), gf[...]),
                           o_emb.at[pl.ds(u * wr, wr)]))
    tall_units = []
    for half, out in ((0, o_wg), (1, o_wu)):
        for u in range(dim // tr):
            tall_units.append((lambda u=u, half=half: dot(n2[:, u * tr:(u + 1) * tr], gcat[:, half * ffn:(half + 1) * ffn], TN),
                               out.at[pl.ds(u * tr, tr)]))
    iw = it = 0
    while iw < len(wide_units) or it < len(tall_units):
        if iw < len(wide_units):
            slot = iw % n_wide
            fn, dst = wide_units[iw]
            free(('w', slot))
            with jax.named_scope(f'wide_{iw}'):
                wide[slot] = fn()
                put(('w', slot), wide.at[slot], dst, s_wide.at[slot])
            iw += 1
        if it < len(tall_units):
            slot = it % n_tall
            fn, dst = tall_units[it]
            free(('t', slot))
            with jax.named_scope(f'tall_{it}'):
                tall[slot] = fn()
                put(('t', slot), tall.at[slot], dst, s_tall.at[slot])
            it += 1
    for i, part in enumerate((gain_a, gain_m)):
        total = part[0]
        for t in range(1, n_tp):
            total = total + part[t]
        gains[i:i + 1, :] = total
    put(('out', 0), hid, o_hid, s_out.at[0])
    put(('out', 1), gains.at[pl.ds(0, 1)], o_ga, s_out.at[1])
    put(('out', 2), gains.at[pl.ds(1, 1)], o_gm, s_out.at[2])
    qw = local_heads * hd
    with jax.named_scope('qkv'):
        for h in range(local_heads):
            qbuf[pl.ds(h, dim, stride=local_heads), :] = dot(n1[...], gqkv[:, h * hd:(h + 1) * hd], TN)
        put(('q', 0), qbuf, o_wq, s_qkv.at[2])
        for i, out in enumerate((o_wk, o_wv)):
            kvbuf[i] = dot(n1[...], gqkv[:, qw + i * hd:qw + (i + 1) * hd], TN)
            put(('k', i), kvbuf.at[i], out, s_qkv.at[i])

    with jax.named_scope('drain'):
        for key in list(busy):
            free(key)


def solution(mesh):
    n_tp = mesh.shape['tp']
    chips = n_tp // 2
    in_specs = (P('dp', None), P('dp', None), P('tp', None), P(None), P(None),
                P(None, 'tp', None), P(None, 'tp', None), P(None, 'tp', None), P('tp', None, None),
                P(None, 'tp'), P(None, 'tp'), P('tp', None), P('dp', 'tp', None))
    out_specs = (P('dp', 'tp', None), P(('dp', 'tp'), None),
                 P('dp', 'tp', None), P('dp', 'tp', None), P('dp', 'tp', None), P(('dp', 'tp'), None, None),
                 P('dp', 'tp'), P('dp', 'tp'), P(('dp', 'tp'), None), P('dp'), P('dp'))

    def device_fn(tokens, positions, emb, gain_attn, gain_mlp, w_query, w_key, w_value, w_out, w_gate, w_up, w_down, grad_hidden):
        seq = tokens.shape[1]
        rows, dim = emb.shape
        lh, hd = w_query.shape[1], w_query.shape[2]
        ffn = w_down.shape[0]
        blk = grad_hidden.shape[1]
        qkvw = (lh + 2) * hd
        inv_freq = (np.float32(ROPE_THETA) ** (-np.arange(hd // 2, dtype=np.float32) * np.float32(2.0 / hd))).astype(np.float32)
        invf = jnp.asarray(np.concatenate([inv_freq, inv_freq])[None, :])

        def sds(shape, dt=BF):
            return jax.ShapeDtypeStruct(shape, dt)

        hb = pl.BlockSpec(memory_space=pltpu.HBM)
        vm = pl.BlockSpec(memory_space=pltpu.VMEM)
        maxc = max(RS_CHUNKS.values())
        mid = pl.pallas_call(
            functools.partial(layer_kernel, n_tp, lh),
            name='layer',
            out_shape=[sds((n_tp, blk, dim))] * 5 + [sds((seq, ffn)), sds((seq, 2 * ffn)), sds((seq, lh * hd)), sds((seq, qkvw)),
                                                    sds((n_tp, 1, dim), F32), sds((n_tp, 1, dim), F32), sds((blk, dim))],
            in_specs=[hb] * 14,
            out_specs=[vm] * 12,
            scratch_shapes=[
                pltpu.VMEM((1, seq), jnp.int32), pltpu.VMEM((1, seq), jnp.int32), pltpu.VMEM((1, hd), F32),
                pltpu.VMEM((1, dim), F32), pltpu.VMEM((1, dim), F32), pltpu.VMEM((blk, dim), BF),
                pltpu.VMEM((rows, dim), BF), pltpu.VMEM((seq, rows), BF), pltpu.VMEM((dim * lh, hd), BF), pltpu.VMEM((dim * lh, hd), F32),
                pltpu.VMEM((dim, qkvw), BF), pltpu.VMEM((lh * hd, dim), BF), pltpu.VMEM((dim, 2 * ffn), BF), pltpu.VMEM((ffn, dim), BF),
                pltpu.VMEM((5, chips, 2, blk, dim), BF), pltpu.VMEM((5, chips, blk, dim), BF),
                pltpu.VMEM((5, chips, blk, dim), BF), pltpu.VMEM((5, chips - 1, blk, dim), BF),
                pltpu.VMEM((2 * ffn, dim), BF), pltpu.VMEM((qkvw, dim), BF), pltpu.VMEM((blk, dim), F32), pltpu.VMEM((blk, dim), F32), pltpu.VMEM((blk, dim), F32), pltpu.VMEM((blk, dim), F32),
                pltpu.VMEM((blk, dim), F32), pltpu.VMEM((2, blk, hd), F32), pltpu.VMEM((seq, ffn), F32), pltpu.VMEM((seq, qkvw), BF),
                pltpu.VMEM((2, seq, hd), F32), pltpu.VMEM((lh, seq, seq), F32),
                pltpu.SemaphoreType.DMA((2, 2)), pltpu.SemaphoreType.DMA(((max(AG_CHUNKS.values()) + 1) * (2 * chips - 1),)),
                pltpu.SemaphoreType.DMA((2, 2)), pltpu.SemaphoreType.DMA((2, maxc, chips)),
                pltpu.SemaphoreType.DMA((18,)),
            ],
            compiler_params=pltpu.CompilerParams(collective_id=0, has_side_effects=True, vmem_limit_bytes=44 * 1024 * 1024),
        )(*(pltpu.with_memory_space_constraint(a, pltpu.HBM) for a in (
            tokens, positions, invf, gain_attn.reshape(1, dim), gain_mlp.reshape(1, dim), grad_hidden.reshape(blk, dim),
            emb, w_query.reshape(dim * lh, hd), w_key.reshape(dim, hd), w_value.reshape(dim, hd), w_out.reshape(lh * hd, dim),
            w_gate, w_up, w_down)))
        n1, n2, gh, gh1, gf, act, gcat, heads, gqkv, gain_m, gain_a, hid = mid
        n1, n2, gh, gh1, gf = (a.reshape(seq, dim) for a in (n1, n2, gh, gh1, gf))
        wide_rows, tall_rows = 256, 512
        res = pl.pallas_call(
            functools.partial(grads_kernel, n_tp, lh),
            name='grads',
            out_shape=[sds((blk, dim)), sds((rows, dim), F32), sds((dim * lh, hd), F32), sds((dim, hd), F32), sds((dim, hd), F32),
                       sds((lh * hd, dim), F32), sds((dim, ffn), F32), sds((dim, ffn), F32), sds((ffn, dim), F32),
                       sds((1, dim), F32), sds((1, dim), F32)],
            in_specs=[vm] * 13,
            out_specs=[hb] * 11,
            scratch_shapes=[
                pltpu.VMEM((2, dim), F32),
                pltpu.VMEM((3, wide_rows, dim), F32), pltpu.VMEM((3, tall_rows, ffn), F32), pltpu.VMEM((dim * lh, hd), F32),
                pltpu.VMEM((2, dim, hd), F32),
                pltpu.SemaphoreType.DMA((3,)), pltpu.SemaphoreType.DMA((3,)), pltpu.SemaphoreType.DMA((3,)),
                pltpu.SemaphoreType.DMA((3,)),
            ],
            compiler_params=pltpu.CompilerParams(vmem_limit_bytes=24 * 1024 * 1024),
        )(tokens, gain_m, gain_a, hid, gh, act, n2, gcat, gh1, heads, n1, gqkv, gf)
        o_hid, o_emb, o_wq, o_wk, o_wv, o_wo, o_wg, o_wu, o_wd, o_ga, o_gm = res
        return (o_hid.reshape(1, blk, dim), o_emb, o_wq.reshape(dim, lh, hd), o_wk.reshape(dim, 1, hd), o_wv.reshape(dim, 1, hd),
                o_wo.reshape(lh, hd, dim), o_wg, o_wu, o_wd, o_ga.reshape(dim), o_gm.reshape(dim))

    return jax.shard_map(device_fn, mesh=mesh, in_specs=in_specs, out_specs=out_specs, check_vma=False)
```

```python
import functools

import jax
import jax.numpy as jnp
import numpy as np
from jax import lax
from jax.experimental import pallas as pl
from jax.experimental.pallas import tpu as pltpu
from jax.sharding import PartitionSpec as P

ROPE_THETA = 1000000.0
RMS_EPS = 1e-5
MESH = pl.DeviceIdType.MESH
BF = jnp.bfloat16
F32 = jnp.float32
NT = (((1,), (1,)), ((), ()))
TN = (((0,), (0,)), ((), ()))

N1, GH, N2, GH1, GF, GAIN_M, GAIN_A = range(7)
R_EMB, R_ATT, R_GN2, R_MLP, R_GN1 = range(5)
RS_CHUNKS = {R_EMB: 4, R_ATT: 2, R_GN2: 4, R_MLP: 2, R_GN1: 2}
AG_CHUNKS = {N1: 4, GH: 1, N2: 1, GH1: 2, GF: 1, GAIN_M: 1, GAIN_A: 1}


def dot(a, b, dims=(((1,), (0,)), ((), ()))):
    return lax.dot_general(a, b, dims, preferred_element_type=F32)


def scoped(name):
    def wrap(fn):
        def run(p, *rest, **kw):
            with jax.named_scope(f'{name}_{p}'):
                return fn(p, *rest, **kw)
        return run
    return wrap


def layer_kernel(n_tp, local_heads,
                 h_tok, h_pos, h_invf, h_ga, h_gm, h_gh, emb, wq4, wk, wv, wo, wg, wu, wd,
                 o_n1, o_n2, o_gh, o_gh1, o_gf, act, gcat, heads, gqkv, gain_m, gain_a, hid,
                 tok, pos, invf, ga, gm, gh_in, embv, onehot, wqr, wqf, wqkv, wov, wguv, wdv, pb, rd, sb, rr,
                 x0g, wgut, wqkvt, x0f, nrm1, nrm2, h1f, gh1f, inv, gact, qkvb, tabs, probs,
                 ag_s, ag_r, rs_s, rs_r, loc):
    chips = n_tp // 2
    seq = h_tok.shape[1]
    rows, dim = emb.shape
    ffn = wd.shape[0]
    blk = gh_in.shape[0]
    hd = wk.shape[1]
    scale = hd ** -0.5
    qw = local_heads * hd

    me = lax.axis_index('tp')
    chip = me // 2
    core = lax.rem(me, 2)
    sib = 2 * chip + 1 - core

    def peer_chip(d):
        return lax.rem(chip + d, chips)

    def peer(d):
        return 2 * peer_chip(d) + core

    order = sorted(range(1, chips), key=lambda d: -min(d, chips - d))

    barrier = pltpu.get_barrier_semaphore()
    for dev in [sib] + [peer(d) for d in range(1, chips)]:
        pl.semaphore_signal(barrier, inc=1, device_id={'tp': dev}, device_id_type=MESH)

    nloc = [1]

    def local(src, dst, slot=None):
        if slot is None:
            slot = nloc[0]
            nloc[0] += 1
        cp = pltpu.make_async_copy(src, dst, loc.at[slot])
        cp.start()
        return cp

    n_emb = RS_CHUNKS[R_EMB]
    ew = dim // n_emb

    def emb_load(j):
        return local(emb.at[:, pl.ds(j * ew, ew)], embv.at[:, pl.ds(j * ew, ew)])

    in_cp = [local(h_tok, tok)]
    emb_cp = [emb_load(j) for j in range(3)]
    in_cp += [local(a, b) for a, b in ((h_pos, pos), (h_invf, invf), (h_ga, ga), (h_gm, gm), (h_gh, gh_in))]
    in_cp[0].wait()

    tok_t = jnp.transpose(jnp.broadcast_to(tok[...].astype(F32), (seq, seq)))
    tok_t = tok_t - (me * rows).astype(F32)
    lane = lax.broadcasted_iota(jnp.int32, (seq, seq), 1).astype(F32)
    for b in range(rows // seq):
        onehot[:, b * seq:(b + 1) * seq] = jnp.where(tok_t == lane + float(b * seq), 1.0, 0.0).astype(BF)

    def remote(src, dst, s, r, dev):
        return pltpu.make_async_remote_copy(src_ref=src, dst_ref=dst, send_sem=s, recv_sem=r,
                                            device_id={'tp': dev}, device_id_type=MESH)

    def send(*args):
        remote(*args).start()

    near = sorted(range(1, chips), key=lambda d: min(d, chips - d))
    incoming = [(d, c) for d in near for c in (1, 0)]

    ag_set = {N1: 0, N2: 0, GH1: 0, GF: 0, GH: 1, GAIN_M: 1, GAIN_A: 1}
    ag = {N1: x0g, GH: o_gh, N2: o_n2, GH1: o_gh1, GF: o_gf, GAIN_M: gain_m, GAIN_A: gain_a}
    per = 2 * chips - 1

    def ag_view(p, t, j):
        w = dim // AG_CHUNKS[p]
        return ag[p].at[t, :, pl.ds(j * w, w)]

    def ag_block(p, d, c, j):
        return ag_view(p, 2 * lax.rem(chip + chips - d, chips) + c, j)

    def ag_recv(p, j, i):
        return ag_r.at[(per * j if ag_set[p] == 0 else ag_r.shape[0] - per) + i]

    def ag_wait_sends(p):
        own, passed = ag[p].at[pl.ds(0, chips)], ag[p].at[pl.ds(0, n_tp - 2)]
        remote(own, own, ag_s.at[ag_set[p], 0], ag_recv(p, 0, 0), sib).wait_send()

        @pl.when(core == 1)
        def _():
            remote(passed, passed, ag_s.at[ag_set[p], 1], ag_recv(p, 0, 0), sib).wait_send()

    @scoped('ag_start')
    def ag_start(p, only=None):
        q = ag_set[p]
        for j in range(AG_CHUNKS[p]) if only is None else (only,):
            mine = ag_view(p, me, j)
            for d in order:
                send(mine, mine, ag_s.at[q, 0], ag_recv(p, j, 2 * d - core), 2 * peer_chip(d) + 1)
            send(mine, mine, ag_s.at[q, 0], ag_recv(p, j, 0), sib)

    @scoped('ag_finish')
    def ag_finish(j, *ps, early=None, forward=True, collect=True):
        if j == 0 and forward:
            @pl.when(core == 1)
            def _():
                for k in range(AG_CHUNKS[ps[0]]):
                    for d, c in incoming:
                        for p in ps:
                            got = ag_block(p, d, c, k)
                            q = ag_set[p]
                            remote(got, got, ag_s.at[q, 1], ag_recv(p, k, 2 * d - c), sib).wait_recv()
                            send(got, got, ag_s.at[q, 1], ag_recv(p, k, 2 * d - c), sib)

        if not collect:
            return
        for p in ps:
            got = ag_view(p, sib, j)
            remote(got, got, ag_s.at[ag_set[p], 0], ag_recv(p, j, 0), sib).wait_recv()

        @pl.when(core == 0)
        def _():
            for i, (d, c) in enumerate(incoming):
                if i == 2 and early is not None:
                    early()
                for p in ps:
                    got = ag_block(p, d, c, j)
                    remote(got, got, ag_s.at[ag_set[p], 1], ag_recv(p, j, 2 * d - c), sib).wait_recv()

    def gathered(p, j=None):
        if j is None:
            return ag[p][...].reshape(seq, dim)
        w = dim // AG_CHUNKS[p]
        return ag[p][:, :, j * w:(j + 1) * w].reshape(seq, w)

    def gathered_dot(p, weight, early):
        w = dim // AG_CHUNKS[p]
        total = None
        for j in range(AG_CHUNKS[p]):
            ag_finish(j, p, early=early if j == 0 else None)
            part = weight(gathered(p, j), slice(j * w, (j + 1) * w))
            total = part if total is None else total + part
        return total

    rs_set = {R_EMB: 0, R_ATT: 0, R_GN2: 0, R_GN1: 0, R_MLP: 1}

    def rs_wait_sends(p):
        q = rs_set[p]
        remote(rd.at[p], rd.at[p], rs_s.at[q, 0], rs_r.at[q, 0, 0], sib).wait_send()
        remote(rr.at[p], rr.at[p], rs_s.at[q, 1], rs_r.at[q, 0, 0], sib).wait_send()

    def rs_cols(p, j):
        w = dim // RS_CHUNKS[p]
        return slice(j * w, (j + 1) * w)

    @scoped('rs_local')
    def rs_local(p, j, val):
        c = rs_cols(p, j)
        w = c.stop - c.start
        pb[p, :, :, :, c] = val.astype(BF).reshape(chips, 2, blk, w)
        send(pb.at[p, :, 1 - core, :, c], rd.at[p, :, :, c], rs_s.at[rs_set[p], 0], rs_r.at[rs_set[p], j, 0], sib)

    @scoped('rs_cross')
    def rs_cross(p, j):
        c = rs_cols(p, j)
        remote(rd.at[p, :, :, c], rd.at[p, :, :, c], rs_s.at[rs_set[p], 0], rs_r.at[rs_set[p], j, 0], sib).wait_recv()
        for d in order:
            to = peer_chip(d)
            both = pb[p, to, core, :, c].astype(F32) + rd[p, to, :, c].astype(F32)
            sb[p, to, :, c] = both.astype(BF)
            send(sb.at[p, to, :, c], rr.at[p, d - 1, :, c], rs_s.at[rs_set[p], 1], rs_r.at[rs_set[p], j, d], peer(d))

    @scoped('rs_finish')
    def rs_finish(p, only=None):
        parts = []
        for j in range(RS_CHUNKS[p]) if only is None else (only,):
            c = rs_cols(p, j)
            total = pb[p, chip, core, :, c].astype(F32) + rd[p, chip, :, c].astype(F32)
            for d in order[::-1]:
                remote(rr.at[p, d - 1, :, c], rr.at[p, d - 1, :, c], rs_s.at[rs_set[p], 1], rs_r.at[rs_set[p], j, d], sib).wait_recv()
                total = total + rr[p, d - 1, :, c].astype(F32)
            parts.append(total)
        return jnp.concatenate(parts, axis=1)

    def rs_start(p, chunk):
        n = RS_CHUNKS[p]
        for j in range(n):
            val = chunk(rs_cols(p, j))
            if p == R_EMB and j == 0:
                with jax.named_scope('barrier'):
                    pl.semaphore_wait(barrier, chips)
            rs_local(p, j, val)
            if j > 0:
                @pl.when(core == 0)
                def _():
                    rs_cross(p, j - 1)

        @pl.when(core == 0)
        def _():
            rs_cross(p, n - 1)

        @pl.when(core == 1)
        def _():
            for j in range(n):
                rs_cross(p, j)

    def on_core(k, fn):
        @pl.when(core == k)
        def _():
            fn()

    def norm_fwd(x, gain):
        r = lax.rsqrt(jnp.mean(x * x, axis=-1, keepdims=True) + RMS_EPS)
        n = x * r
        return (n * gain).astype(BF), n, r

    def norm_bwd(g, n, r, gain):
        part = jnp.sum(g * n, axis=0, keepdims=True)
        scaled = g * gain
        return r * (scaled - n * jnp.mean(scaled * n, axis=-1, keepdims=True)), part

    w_cp = {}

    def emb_chunk(c):
        j = c.start // ew
        emb_cp[j].wait()
        if j + 3 < n_emb:
            emb_cp.append(emb_load(j + 3))
        if j == n_emb - 2:
            w_cp['k'] = local(wk, wqkv.at[:, pl.ds(qw, hd)])
            w_cp['v'] = local(wv, wqkv.at[:, pl.ds(qw + hd, hd)])
            w_cp['q'] = local(wq4, wqr)
        if j == n_emb - 1:
            w_cp['o'] = local(wo, wov)
            w_cp['g'] = local(wg, wguv.at[:, pl.ds(0, ffn)])
            w_cp['u'] = local(wu, wguv.at[:, pl.ds(ffn, ffn)])
            w_cp['d'] = local(wd, wdv)
        return dot(onehot[...], embv[:, c])

    rs_start(R_EMB, emb_chunk)

    in_cp[1].wait()
    in_cp[2].wait()
    pos_t = jnp.transpose(jnp.broadcast_to(pos[...].astype(F32), (seq, seq)))
    angle = pos_t * invf[...]
    half = lax.broadcasted_iota(jnp.int32, (seq, hd), 1) < hd // 2
    tabs[0] = jnp.cos(angle)
    sin = jnp.sin(angle)
    tabs[1] = jnp.where(half, -sin, sin)
    for cp in in_cp[3:]:
        cp.wait()
    for j in range(RS_CHUNKS[R_EMB]):
        part = rs_finish(R_EMB, j)
        x0f[:, rs_cols(R_EMB, j)] = part
        x0g[me, :, rs_cols(R_EMB, j)] = part.astype(BF)
        ag_start(N1, j)
    x0 = x0f[...]
    n1b, n1, r1 = norm_fwd(x0, ga[...])
    nrm1[...] = n1
    inv[0] = jnp.broadcast_to(r1, (blk, hd))
    o_gh[me] = gh_in[...]
    w_cp['k'].wait()
    w_cp['v'].wait()
    w_cp['q'].wait()
    wqf[...] = wqr[...].astype(F32)
    for h in range(local_heads):
        wqkv[:, h * hd:(h + 1) * hd] = wqf[pl.ds(h, dim, stride=local_heads), :].astype(BF)


    tw = 256
    eye = (lax.broadcasted_iota(jnp.int32, (tw, tw), 0) == lax.broadcasted_iota(jnp.int32, (tw, tw), 1)).astype(F32).astype(BF)
    with jax.named_scope('wqkvt'):
        for b in range((qw + 2 * hd) // tw):
            wqkvt[b * tw:(b + 1) * tw, :] = dot(eye, wqkv[:, b * tw:(b + 1) * tw], NT).astype(BF)

    def rotate(v, sign):
        return v * tabs[0] + sign * (pltpu.roll(v, hd // 2, 1) * tabs[1])

    square = None
    for j in range(AG_CHUNKS[N1]):
        ag_finish(j, N1, early=(lambda: ag_start(GH)) if j == 0 else None)
        part = gathered(N1, j).astype(F32)
        part = jnp.sum(part * part, axis=-1, keepdims=True)
        square = part if square is None else square + part
    rms = lax.rsqrt(square * (1.0 / dim) + RMS_EPS)
    cw = dim // AG_CHUNKS[N1]
    for j in range(AG_CHUNKS[N1]):
        c = slice(j * cw, (j + 1) * cw)
        o_n1[:, :, c] = (gathered(N1, j).astype(F32) * rms * ga[:, c]).astype(BF).reshape(n_tp, blk, cw)
    qkv = dot(o_n1[...].reshape(seq, dim), wqkv[...])
    on_core(1, lambda: ag_start(GH))
    for h in range(local_heads + 1):
        qkvb[:, h * hd:(h + 1) * hd] = rotate(qkv[:, h * hd:(h + 1) * hd], 1.0).astype(BF)
    qkvb[:, qw + hd:] = qkv[:, qw + hd:].astype(BF)
    kb = qkvb[:, qw:qw + hd]
    vb = qkvb[:, qw + hd:]
    causal = lax.broadcasted_iota(jnp.int32, (seq, seq), 0) >= lax.broadcasted_iota(jnp.int32, (seq, seq), 1)
    for h in range(local_heads):
        s = dot(qkvb[:, h * hd:(h + 1) * hd], kb, NT) * scale
        s = jnp.where(causal, s, -1e30)
        e = jnp.exp(s - jnp.max(s, axis=-1, keepdims=True))
        pr = e / jnp.sum(e, axis=-1, keepdims=True)
        probs[h] = pr
        heads[:, h * hd:(h + 1) * hd] = dot(pr.astype(BF), vb).astype(BF)
    w_cp['o'].wait()
    rs_wait_sends(R_EMB)
    rs_start(R_ATT, lambda c: dot(heads[...], wov[:, c]))

    w_cp['g'].wait()
    w_cp['u'].wait()
    with jax.named_scope('wgut'):
        for b in range(2 * ffn // tw):
            wgut[b * tw:(b + 1) * tw, :] = dot(eye, wguv[:, b * tw:(b + 1) * tw], NT).astype(BF)
    ag_finish(0, GH)
    w_cp['d'].wait()

    h1 = (x0f[...] + rs_finish(R_ATT).astype(BF).astype(F32)).astype(BF).astype(F32)
    h1f[...] = h1
    n2b, n2, r2 = norm_fwd(h1, gm[...])
    o_n2[me] = n2b
    nrm2[...] = n2
    inv[1] = jnp.broadcast_to(r2, (blk, hd))
    ag_wait_sends(N1)
    ag_start(N2)
    with jax.named_scope('gact'):
        gact[...] = dot(gathered(GH), wdv[...], NT).astype(BF).astype(F32)

    ag_finish(0, N2)
    fw = 256
    for j in range(ffn // fw):
        c = slice(j * fw, (j + 1) * fw)
        cu = slice(ffn + j * fw, ffn + (j + 1) * fw)
        gate = dot(gathered(N2), wguv[:, c])
        up = dot(gathered(N2), wguv[:, cu])
        sig = jax.nn.sigmoid(gate)
        ga_act = gate * sig
        act[:, c] = (ga_act * up).astype(BF)
        g = gact[:, c]
        gcat[:, cu] = (g * ga_act).astype(BF)
        gcat[:, c] = (g * up * sig * (1.0 + gate * (1.0 - sig))).astype(BF)
    rs_wait_sends(R_ATT)
    rs_start(R_GN2, lambda c: dot(gcat[...], wgut[:, c]))
    for j in range(RS_CHUNKS[R_MLP]):
        rs_local(R_MLP, j, dot(act[...], wdv[:, rs_cols(R_MLP, j)]))

    gn2 = rs_finish(R_GN2).astype(BF).astype(F32)
    g_in, gain_part = norm_bwd(gn2, nrm2[...], inv[1][:, :1], gm[...])
    gain_m[me] = gain_part
    gh1 = (gh_in[...].astype(F32) + g_in).astype(BF)
    gh1f[...] = gh1.astype(F32)
    o_gh1[me] = gh1
    ag_wait_sends(N2)
    ag_start(GH1)
    ag_wait_sends(GH)
    ag_start(GAIN_M)
    def mlp_cross():
        for j in range(RS_CHUNKS[R_MLP]):
            rs_cross(R_MLP, j)

    ghd = gathered_dot(GH1, lambda a, k: dot(a, wov[:, k], NT), mlp_cross).astype(BF)
    on_core(1, mlp_cross)
    ag_finish(0, GAIN_M, collect=False)

    gv = jnp.zeros((seq, hd), F32)
    gk = jnp.zeros((seq, hd), F32)
    for h in range(local_heads):
        g = ghd[:, h * hd:(h + 1) * hd]
        pr = probs[h]
        gp = dot(g, vb, NT).astype(BF).astype(F32)
        gv = gv + dot(pr.astype(BF), g, TN)
        gs = (pr * (gp - jnp.sum(gp * pr, axis=-1, keepdims=True)) * scale).astype(BF)
        gq = dot(gs, kb).astype(BF).astype(F32)
        gk = gk + dot(gs, qkvb[:, h * hd:(h + 1) * hd], TN)
        gqkv[:, h * hd:(h + 1) * hd] = rotate(gq, -1.0).astype(BF)
    gqkv[:, qw:qw + hd] = rotate(gk.astype(BF).astype(F32), -1.0).astype(BF)
    gqkv[:, qw + hd:] = gv.astype(BF)
    ag_finish(0, GAIN_M, forward=False)
    rs_wait_sends(R_GN2)
    rs_start(R_GN1, lambda c: dot(gqkv[...], wqkvt[:, c]))
    hid[...] = (h1f[...] + rs_finish(R_MLP).astype(BF).astype(F32)).astype(BF)

    gn1 = rs_finish(R_GN1).astype(BF).astype(F32)
    g_in, gain_part = norm_bwd(gn1, nrm1[...], inv[0][:, :1], ga[...])
    gain_a[me] = gain_part
    o_gf[me] = (gh1f[...] + g_in).astype(BF)
    ag_wait_sends(GAIN_M)
    ag_wait_sends(GH1)
    ag_start(GAIN_A)
    ag_start(GF)
    ag_finish(0, GAIN_A, GF)
    with jax.named_scope('tail_send'):
        rs_wait_sends(R_GN1)
        rs_wait_sends(R_MLP)
        ag_wait_sends(GAIN_A)
        ag_wait_sends(GF)


def grads_kernel(n_tp, local_heads,
                 tok, gain_m, gain_a, hid, gh, act, n2, gcat, gh1, heads, n1, gqkv, gf,
                 o_hid, o_emb, o_wq, o_wk, o_wv, o_wo, o_wg, o_wu, o_wd, o_ga, o_gm,
                 gains, wide, tall, qbuf, kvbuf, s_wide, s_tall, s_qkv, s_out):
    seq, dim = n1.shape
    rows = o_emb.shape[0]
    ffn = act.shape[1]
    hd = gqkv.shape[1] // (local_heads + 2)
    me = lax.axis_index('tp')
    n_wide, wr = wide.shape[0], wide.shape[1]
    n_tall, tr = tall.shape[0], tall.shape[1]
    busy = {}

    def put(key, src, dst, sem):
        cp = pltpu.make_async_copy(src, dst, sem)
        cp.start()
        busy[key] = cp

    def free(key):
        if key in busy:
            busy.pop(key).wait()

    row = lax.broadcasted_iota(jnp.int32, (wr, seq), 0)
    wide_units = []
    for u in range(ffn // wr):
        wide_units.append((lambda u=u: dot(act[:, u * wr:(u + 1) * wr], gh[...], TN), o_wd.at[pl.ds(u * wr, wr)]))
    for u in range(heads.shape[1] // wr):
        wide_units.append((lambda u=u: dot(heads[:, u * wr:(u + 1) * wr], gh1[...], TN), o_wo.at[pl.ds(u * wr, wr)]))
    for u in range(rows // wr):
        wide_units.append((lambda u=u: dot(jnp.where(row + u * wr == tok[...] - me * rows, 1.0, 0.0).astype(BF), gf[...]),
                           o_emb.at[pl.ds(u * wr, wr)]))
    tall_units = []
    for half, out in ((0, o_wg), (1, o_wu)):
        for u in range(dim // tr):
            tall_units.append((lambda u=u, half=half: dot(n2[:, u * tr:(u + 1) * tr], gcat[:, half * ffn:(half + 1) * ffn], TN),
                               out.at[pl.ds(u * tr, tr)]))
    iw = it = 0
    while iw < len(wide_units) or it < len(tall_units):
        if iw < len(wide_units):
            slot = iw % n_wide
            fn, dst = wide_units[iw]
            free(('w', slot))
            with jax.named_scope(f'wide_{iw}'):
                wide[slot] = fn()
                put(('w', slot), wide.at[slot], dst, s_wide.at[slot])
            iw += 1
        if it < len(tall_units):
            slot = it % n_tall
            fn, dst = tall_units[it]
            free(('t', slot))
            with jax.named_scope(f'tall_{it}'):
                tall[slot] = fn()
                put(('t', slot), tall.at[slot], dst, s_tall.at[slot])
            it += 1
    for i, part in enumerate((gain_a, gain_m)):
        total = part[0]
        for t in range(1, n_tp):
            total = total + part[t]
        gains[i:i + 1, :] = total
    put(('out', 0), hid, o_hid, s_out.at[0])
    put(('out', 1), gains.at[pl.ds(0, 1)], o_ga, s_out.at[1])
    put(('out', 2), gains.at[pl.ds(1, 1)], o_gm, s_out.at[2])
    qw = local_heads * hd
    with jax.named_scope('qkv'):
        for h in range(local_heads):
            qbuf[pl.ds(h, dim, stride=local_heads), :] = dot(n1[...], gqkv[:, h * hd:(h + 1) * hd], TN)
        put(('q', 0), qbuf, o_wq, s_qkv.at[2])
        for i, out in enumerate((o_wk, o_wv)):
            kvbuf[i] = dot(n1[...], gqkv[:, qw + i * hd:qw + (i + 1) * hd], TN)
            put(('k', i), kvbuf.at[i], out, s_qkv.at[i])

    with jax.named_scope('drain'):
        for key in list(busy):
            free(key)


def solution(mesh):
    n_tp = mesh.shape['tp']
    chips = n_tp // 2
    in_specs = (P('dp', None), P('dp', None), P('tp', None), P(None), P(None),
                P(None, 'tp', None), P(None, 'tp', None), P(None, 'tp', None), P('tp', None, None),
                P(None, 'tp'), P(None, 'tp'), P('tp', None), P('dp', 'tp', None))
    out_specs = (P('dp', 'tp', None), P(('dp', 'tp'), None),
                 P('dp', 'tp', None), P('dp', 'tp', None), P('dp', 'tp', None), P(('dp', 'tp'), None, None),
                 P('dp', 'tp'), P('dp', 'tp'), P(('dp', 'tp'), None), P('dp'), P('dp'))

    def device_fn(tokens, positions, emb, gain_attn, gain_mlp, w_query, w_key, w_value, w_out, w_gate, w_up, w_down, grad_hidden):
        seq = tokens.shape[1]
        rows, dim = emb.shape
        lh, hd = w_query.shape[1], w_query.shape[2]
        ffn = w_down.shape[0]
        blk = grad_hidden.shape[1]
        qkvw = (lh + 2) * hd
        inv_freq = (np.float32(ROPE_THETA) ** (-np.arange(hd // 2, dtype=np.float32) * np.float32(2.0 / hd))).astype(np.float32)
        invf = jnp.asarray(np.concatenate([inv_freq, inv_freq])[None, :])

        def sds(shape, dt=BF):
            return jax.ShapeDtypeStruct(shape, dt)

        hb = pl.BlockSpec(memory_space=pltpu.HBM)
        vm = pl.BlockSpec(memory_space=pltpu.VMEM)
        maxc = max(RS_CHUNKS.values())
        mid = pl.pallas_call(
            functools.partial(layer_kernel, n_tp, lh),
            name='layer',
            out_shape=[sds((n_tp, blk, dim))] * 5 + [sds((seq, ffn)), sds((seq, 2 * ffn)), sds((seq, lh * hd)), sds((seq, qkvw)),
                                                    sds((n_tp, 1, dim), F32), sds((n_tp, 1, dim), F32), sds((blk, dim))],
            in_specs=[hb] * 14,
            out_specs=[vm] * 12,
            scratch_shapes=[
                pltpu.VMEM((1, seq), jnp.int32), pltpu.VMEM((1, seq), jnp.int32), pltpu.VMEM((1, hd), F32),
                pltpu.VMEM((1, dim), F32), pltpu.VMEM((1, dim), F32), pltpu.VMEM((blk, dim), BF),
                pltpu.VMEM((rows, dim), BF), pltpu.VMEM((seq, rows), BF), pltpu.VMEM((dim * lh, hd), BF), pltpu.VMEM((dim * lh, hd), F32),
                pltpu.VMEM((dim, qkvw), BF), pltpu.VMEM((lh * hd, dim), BF), pltpu.VMEM((dim, 2 * ffn), BF), pltpu.VMEM((ffn, dim), BF),
                pltpu.VMEM((5, chips, 2, blk, dim), BF), pltpu.VMEM((5, chips, blk, dim), BF),
                pltpu.VMEM((5, chips, blk, dim), BF), pltpu.VMEM((5, chips - 1, blk, dim), BF),
                pltpu.VMEM((n_tp, blk, dim), BF), pltpu.VMEM((2 * ffn, dim), BF), pltpu.VMEM((qkvw, dim), BF), pltpu.VMEM((blk, dim), F32), pltpu.VMEM((blk, dim), F32), pltpu.VMEM((blk, dim), F32), pltpu.VMEM((blk, dim), F32),
                pltpu.VMEM((blk, dim), F32), pltpu.VMEM((2, blk, hd), F32), pltpu.VMEM((seq, ffn), F32), pltpu.VMEM((seq, qkvw), BF),
                pltpu.VMEM((2, seq, hd), F32), pltpu.VMEM((lh, seq, seq), F32),
                pltpu.SemaphoreType.DMA((2, 2)), pltpu.SemaphoreType.DMA(((max(AG_CHUNKS.values()) + 1) * (2 * chips - 1),)),
                pltpu.SemaphoreType.DMA((2, 2)), pltpu.SemaphoreType.DMA((2, maxc, chips)),
                pltpu.SemaphoreType.DMA((18,)),
            ],
            compiler_params=pltpu.CompilerParams(collective_id=0, has_side_effects=True, vmem_limit_bytes=44 * 1024 * 1024),
        )(*(pltpu.with_memory_space_constraint(a, pltpu.HBM) for a in (
            tokens, positions, invf, gain_attn.reshape(1, dim), gain_mlp.reshape(1, dim), grad_hidden.reshape(blk, dim),
            emb, w_query.reshape(dim * lh, hd), w_key.reshape(dim, hd), w_value.reshape(dim, hd), w_out.reshape(lh * hd, dim),
            w_gate, w_up, w_down)))
        n1, n2, gh, gh1, gf, act, gcat, heads, gqkv, gain_m, gain_a, hid = mid
        n1, n2, gh, gh1, gf = (a.reshape(seq, dim) for a in (n1, n2, gh, gh1, gf))
        wide_rows, tall_rows = 256, 512
        res = pl.pallas_call(
            functools.partial(grads_kernel, n_tp, lh),
            name='grads',
            out_shape=[sds((blk, dim)), sds((rows, dim), F32), sds((dim * lh, hd), F32), sds((dim, hd), F32), sds((dim, hd), F32),
                       sds((lh * hd, dim), F32), sds((dim, ffn), F32), sds((dim, ffn), F32), sds((ffn, dim), F32),
                       sds((1, dim), F32), sds((1, dim), F32)],
            in_specs=[vm] * 13,
            out_specs=[hb] * 11,
            scratch_shapes=[
                pltpu.VMEM((2, dim), F32),
                pltpu.VMEM((3, wide_rows, dim), F32), pltpu.VMEM((3, tall_rows, ffn), F32), pltpu.VMEM((dim * lh, hd), F32),
                pltpu.VMEM((2, dim, hd), F32),
                pltpu.SemaphoreType.DMA((3,)), pltpu.SemaphoreType.DMA((3,)), pltpu.SemaphoreType.DMA((3,)),
                pltpu.SemaphoreType.DMA((3,)),
            ],
            compiler_params=pltpu.CompilerParams(vmem_limit_bytes=24 * 1024 * 1024),
        )(tokens, gain_m, gain_a, hid, gh, act, n2, gcat, gh1, heads, n1, gqkv, gf)
        o_hid, o_emb, o_wq, o_wk, o_wv, o_wo, o_wg, o_wu, o_wd, o_ga, o_gm = res
        return (o_hid.reshape(1, blk, dim), o_emb, o_wq.reshape(dim, lh, hd), o_wk.reshape(dim, 1, hd), o_wv.reshape(dim, 1, hd),
                o_wo.reshape(lh, hd, dim), o_wg, o_wu, o_wd, o_ga.reshape(dim), o_gm.reshape(dim))

    return jax.shard_map(device_fn, mesh=mesh, in_specs=in_specs, out_specs=out_specs, check_vma=False)
```

```python
import functools

import jax
import jax.numpy as jnp
import numpy as np
from jax import lax
from jax.experimental import pallas as pl
from jax.experimental.pallas import tpu as pltpu
from jax.sharding import PartitionSpec as P

ROPE_THETA = 1000000.0
RMS_EPS = 1e-5
MESH = pl.DeviceIdType.MESH
BF = jnp.bfloat16
F32 = jnp.float32
NT = (((1,), (1,)), ((), ()))
TN = (((0,), (0,)), ((), ()))

N1, GH, N2, GH1, GF = range(5)
R_EMB, R_ATT, R_GN2, R_MLP, R_GN1 = range(5)
RS_CHUNKS = {R_EMB: 4, R_ATT: 4, R_GN2: 4, R_MLP: 2, R_GN1: 4}
AG_CHUNKS = {N1: 4, GH: 1, N2: 4, GH1: 4, GF: 4}


def dot(a, b, dims=(((1,), (0,)), ((), ()))):
    return lax.dot_general(a, b, dims, preferred_element_type=F32)


def scoped(name):
    def wrap(fn):
        def run(p, *rest, **kw):
            with jax.named_scope(f'{name}_{p}'):
                return fn(p, *rest, **kw)
        return run
    return wrap


def layer_kernel(n_tp, local_heads,
                 h_tok, h_pos, h_invf, h_ga, h_gm, h_gh, emb, wq4, wk, wv, wo, wg, wu, wd,
                 o_n1, o_n2, o_gh, o_gh1, o_gf, act, gcat, heads, gqkv, gain_m, gain_a, hid,
                 tok, pos, invf, ga, gm, gh_in, embv, onehot, wqr, wqf, wqkv, wov, wguv, wdv, pb, rd, sb, rr,
                 x0g, h1g, gn2g, gn1g, wgut, wqkvt, x0f, h1f, inv, gact, qkvb, tabs, probs,
                 ag_s, ag_r, rs_s, rs_r, loc):
    chips = n_tp // 2
    seq = h_tok.shape[1]
    rows, dim = emb.shape
    ffn = wd.shape[0]
    blk = gh_in.shape[0]
    hd = wk.shape[1]
    scale = hd ** -0.5
    qw = local_heads * hd

    me = lax.axis_index('tp')
    chip = me // 2
    core = lax.rem(me, 2)
    sib = 2 * chip + 1 - core

    def peer_chip(d):
        return lax.rem(chip + d, chips)

    def peer(d):
        return 2 * peer_chip(d) + core

    order = sorted(range(1, chips), key=lambda d: -min(d, chips - d))

    barrier = pltpu.get_barrier_semaphore()
    for dev in [sib] + [peer(d) for d in range(1, chips)]:
        pl.semaphore_signal(barrier, inc=1, device_id={'tp': dev}, device_id_type=MESH)

    nloc = [1]

    def local(src, dst, slot=None):
        if slot is None:
            slot = nloc[0]
            nloc[0] += 1
        cp = pltpu.make_async_copy(src, dst, loc.at[slot])
        cp.start()
        return cp

    n_emb = RS_CHUNKS[R_EMB]
    ew = dim // n_emb

    def emb_load(j):
        return local(emb.at[:, pl.ds(j * ew, ew)], embv.at[:, pl.ds(j * ew, ew)])

    in_cp = [local(h_tok, tok)]
    emb_cp = [emb_load(j) for j in range(3)]
    in_cp += [local(a, b) for a, b in ((h_pos, pos), (h_invf, invf), (h_ga, ga), (h_gm, gm), (h_gh, gh_in))]
    in_cp[0].wait()

    tok_t = jnp.transpose(jnp.broadcast_to(tok[...].astype(F32), (seq, seq)))
    tok_t = tok_t - (me * rows).astype(F32)
    lane = lax.broadcasted_iota(jnp.int32, (seq, seq), 1).astype(F32)
    for b in range(rows // seq):
        onehot[:, b * seq:(b + 1) * seq] = jnp.where(tok_t == lane + float(b * seq), 1.0, 0.0).astype(BF)

    def remote(src, dst, s, r, dev):
        return pltpu.make_async_remote_copy(src_ref=src, dst_ref=dst, send_sem=s, recv_sem=r,
                                            device_id={'tp': dev}, device_id_type=MESH)

    def send(*args):
        remote(*args).start()

    near = sorted(range(1, chips), key=lambda d: min(d, chips - d))
    incoming = [(d, c) for d in near for c in (1, 0)]

    ag_set = {N1: 0, N2: 0, GH1: 0, GF: 0, GH: 1}
    ag = {N1: x0g, GH: o_gh, N2: h1g, GH1: gn2g, GF: gn1g}
    per = 2 * chips - 1

    def ag_view(p, t, j):
        w = dim // AG_CHUNKS[p]
        return ag[p].at[t, :, pl.ds(j * w, w)]

    def ag_block(p, d, c, j):
        return ag_view(p, 2 * lax.rem(chip + chips - d, chips) + c, j)

    def ag_recv(p, j, i):
        return ag_r.at[(per * j if ag_set[p] == 0 else ag_r.shape[0] - per) + i]

    def ag_wait_sends(p):
        own, passed = ag[p].at[pl.ds(0, chips)], ag[p].at[pl.ds(0, n_tp - 2)]
        remote(own, own, ag_s.at[ag_set[p], 0], ag_recv(p, 0, 0), sib).wait_send()

        @pl.when(core == 1)
        def _():
            remote(passed, passed, ag_s.at[ag_set[p], 1], ag_recv(p, 0, 0), sib).wait_send()

    @scoped('ag_start')
    def ag_start(p, only=None):
        q = ag_set[p]
        for j in range(AG_CHUNKS[p]) if only is None else (only,):
            mine = ag_view(p, me, j)
            for d in order:
                send(mine, mine, ag_s.at[q, 0], ag_recv(p, j, 2 * d - core), 2 * peer_chip(d) + 1)
            send(mine, mine, ag_s.at[q, 0], ag_recv(p, j, 0), sib)

    @scoped('ag_finish')
    def ag_finish(j, *ps, early=None, forward=True, collect=True):
        if j == 0 and forward:
            @pl.when(core == 1)
            def _():
                for k in range(AG_CHUNKS[ps[0]]):
                    for d, c in incoming:
                        for p in ps:
                            got = ag_block(p, d, c, k)
                            q = ag_set[p]
                            remote(got, got, ag_s.at[q, 1], ag_recv(p, k, 2 * d - c), sib).wait_recv()
                            send(got, got, ag_s.at[q, 1], ag_recv(p, k, 2 * d - c), sib)

        if not collect:
            return
        for p in ps:
            got = ag_view(p, sib, j)
            remote(got, got, ag_s.at[ag_set[p], 0], ag_recv(p, j, 0), sib).wait_recv()

        @pl.when(core == 0)
        def _():
            for i, (d, c) in enumerate(incoming):
                if i == 2 and early is not None:
                    early()
                for p in ps:
                    got = ag_block(p, d, c, j)
                    remote(got, got, ag_s.at[ag_set[p], 1], ag_recv(p, j, 2 * d - c), sib).wait_recv()

    def gathered(p, j=None):
        if j is None:
            return ag[p][...].reshape(seq, dim)
        w = dim // AG_CHUNKS[p]
        return ag[p][:, :, j * w:(j + 1) * w].reshape(seq, w)

    def gathered_dot(p, weight, early):
        w = dim // AG_CHUNKS[p]
        total = None
        for j in range(AG_CHUNKS[p]):
            ag_finish(j, p, early=early if j == 0 else None)
            part = weight(gathered(p, j), slice(j * w, (j + 1) * w))
            total = part if total is None else total + part
        return total

    rs_set = {R_EMB: 0, R_ATT: 0, R_GN2: 0, R_GN1: 0, R_MLP: 1}

    def rs_wait_sends(p):
        q = rs_set[p]
        remote(rd.at[p], rd.at[p], rs_s.at[q, 0], rs_r.at[q, 0, 0], sib).wait_send()
        remote(rr.at[p], rr.at[p], rs_s.at[q, 1], rs_r.at[q, 0, 0], sib).wait_send()

    def rs_cols(p, j):
        w = dim // RS_CHUNKS[p]
        return slice(j * w, (j + 1) * w)

    @scoped('rs_local')
    def rs_local(p, j, val):
        c = rs_cols(p, j)
        w = c.stop - c.start
        pb[p, :, :, :, c] = val.astype(BF).reshape(chips, 2, blk, w)
        send(pb.at[p, :, 1 - core, :, c], rd.at[p, :, :, c], rs_s.at[rs_set[p], 0], rs_r.at[rs_set[p], j, 0], sib)

    @scoped('rs_cross')
    def rs_cross(p, j):
        c = rs_cols(p, j)
        remote(rd.at[p, :, :, c], rd.at[p, :, :, c], rs_s.at[rs_set[p], 0], rs_r.at[rs_set[p], j, 0], sib).wait_recv()
        for d in order:
            to = peer_chip(d)
            both = pb[p, to, core, :, c].astype(F32) + rd[p, to, :, c].astype(F32)
            sb[p, to, :, c] = both.astype(BF)
            send(sb.at[p, to, :, c], rr.at[p, d - 1, :, c], rs_s.at[rs_set[p], 1], rs_r.at[rs_set[p], j, d], peer(d))

    @scoped('rs_finish')
    def rs_finish(p, only=None):
        parts = []
        for j in range(RS_CHUNKS[p]) if only is None else (only,):
            c = rs_cols(p, j)
            total = pb[p, chip, core, :, c].astype(F32) + rd[p, chip, :, c].astype(F32)
            for d in order[::-1]:
                remote(rr.at[p, d - 1, :, c], rr.at[p, d - 1, :, c], rs_s.at[rs_set[p], 1], rs_r.at[rs_set[p], j, d], sib).wait_recv()
                total = total + rr[p, d - 1, :, c].astype(F32)
            parts.append(total)
        return jnp.concatenate(parts, axis=1)

    def rs_start(p, chunk):
        n = RS_CHUNKS[p]
        for j in range(n):
            val = chunk(rs_cols(p, j))
            if p == R_EMB and j == 0:
                with jax.named_scope('barrier'):
                    pl.semaphore_wait(barrier, chips)
            rs_local(p, j, val)
            if j > 0:
                @pl.when(core == 0)
                def _():
                    rs_cross(p, j - 1)

        @pl.when(core == 0)
        def _():
            rs_cross(p, n - 1)

        @pl.when(core == 1)
        def _():
            for j in range(n):
                rs_cross(p, j)

    def on_core(k, fn):
        @pl.when(core == k)
        def _():
            fn()

    def spread(v):
        return jnp.broadcast_to(v, (seq, hd))

    def norm_fwd(p, slot, gain, out, early=None):
        square = None
        for j in range(AG_CHUNKS[p]):
            ag_finish(j, p, early=early if j == 0 else None)
            part = gathered(p, j).astype(F32)
            part = jnp.sum(part * part, axis=-1, keepdims=True)
            square = part if square is None else square + part
        r = lax.rsqrt(square * (1.0 / dim) + RMS_EPS)
        inv[slot] = spread(r)
        w = dim // AG_CHUNKS[p]
        for j in range(AG_CHUNKS[p]):
            c = slice(j * w, (j + 1) * w)
            out[:, :, c] = (gathered(p, j).astype(F32) * r * gain[:, c]).astype(BF).reshape(n_tp, blk, w)

    def norm_bwd(p, p_in, slot, gain, around, out, gain_out, early=None, use=None):
        w = dim // AG_CHUNKS[p]
        r = inv[slot][:, :1]
        both = None
        for j in range(AG_CHUNKS[p]):
            c = slice(j * w, (j + 1) * w)
            ag_finish(j, p, early=early if j == 0 else None)
            if j == 0 and early is not None:
                on_core(1, early)
            g = gathered(p, j).astype(F32)
            n = gathered(p_in, j).astype(F32) * r
            gn = g * n
            gain_out[:, c] = jnp.sum(gn, axis=0, keepdims=True)
            part = jnp.sum(gn * gain[:, c], axis=-1, keepdims=True)
            both = part if both is None else both + part
        mean = both * (1.0 / dim)
        for j in range(AG_CHUNKS[p]):
            c = slice(j * w, (j + 1) * w)
            n = gathered(p_in, j).astype(F32) * r
            g_in = r * (gathered(p, j).astype(F32) * gain[:, c] - n * mean)
            total = (around[:, :, c].reshape(seq, w).astype(F32) + g_in).astype(BF)
            out[:, :, c] = total.reshape(n_tp, blk, w)
            if use is not None:
                use(total, c)

    w_cp = {}

    def emb_chunk(c):
        j = c.start // ew
        emb_cp[j].wait()
        if j + 3 < n_emb:
            emb_cp.append(emb_load(j + 3))
        if j == n_emb - 2:
            w_cp['k'] = local(wk, wqkv.at[:, pl.ds(qw, hd)])
            w_cp['v'] = local(wv, wqkv.at[:, pl.ds(qw + hd, hd)])
            w_cp['q'] = local(wq4, wqr)
        if j == n_emb - 1:
            w_cp['o'] = local(wo, wov)
            w_cp['g'] = local(wg, wguv.at[:, pl.ds(0, ffn)])
            w_cp['u'] = local(wu, wguv.at[:, pl.ds(ffn, ffn)])
            w_cp['d'] = local(wd, wdv)
        return dot(onehot[...], embv[:, c])

    rs_start(R_EMB, emb_chunk)

    in_cp[1].wait()
    in_cp[2].wait()
    pos_t = jnp.transpose(jnp.broadcast_to(pos[...].astype(F32), (seq, seq)))
    angle = pos_t * invf[...]
    half = lax.broadcasted_iota(jnp.int32, (seq, hd), 1) < hd // 2
    tabs[0] = jnp.cos(angle)
    sin = jnp.sin(angle)
    tabs[1] = jnp.where(half, -sin, sin)
    for cp in in_cp[3:]:
        cp.wait()
    for j in range(RS_CHUNKS[R_EMB]):
        part = rs_finish(R_EMB, j)
        x0f[:, rs_cols(R_EMB, j)] = part
        x0g[me, :, rs_cols(R_EMB, j)] = part.astype(BF)
        ag_start(N1, j)
    o_gh[me] = gh_in[...]
    w_cp['k'].wait()
    w_cp['v'].wait()
    w_cp['q'].wait()
    wqf[...] = wqr[...].astype(F32)
    for h in range(local_heads):
        wqkv[:, h * hd:(h + 1) * hd] = wqf[pl.ds(h, dim, stride=local_heads), :].astype(BF)


    tw = 256
    eye = (lax.broadcasted_iota(jnp.int32, (tw, tw), 0) == lax.broadcasted_iota(jnp.int32, (tw, tw), 1)).astype(F32).astype(BF)
    with jax.named_scope('wqkvt'):
        for b in range((qw + 2 * hd) // tw):
            wqkvt[b * tw:(b + 1) * tw, :] = dot(eye, wqkv[:, b * tw:(b + 1) * tw], NT).astype(BF)

    def rotate(v, sign):
        return v * tabs[0] + sign * (pltpu.roll(v, hd // 2, 1) * tabs[1])

    norm_fwd(N1, 0, ga, o_n1, early=lambda: ag_start(GH))
    qkv = dot(o_n1[...].reshape(seq, dim), wqkv[...])
    on_core(1, lambda: ag_start(GH))
    for h in range(local_heads + 1):
        qkvb[:, h * hd:(h + 1) * hd] = rotate(qkv[:, h * hd:(h + 1) * hd], 1.0).astype(BF)
    qkvb[:, qw + hd:] = qkv[:, qw + hd:].astype(BF)
    kb = qkvb[:, qw:qw + hd]
    vb = qkvb[:, qw + hd:]
    causal = lax.broadcasted_iota(jnp.int32, (seq, seq), 0) >= lax.broadcasted_iota(jnp.int32, (seq, seq), 1)
    for h in range(local_heads):
        s = dot(qkvb[:, h * hd:(h + 1) * hd], kb, NT) * scale
        s = jnp.where(causal, s, -1e30)
        e = jnp.exp(s - jnp.max(s, axis=-1, keepdims=True))
        pr = e / jnp.sum(e, axis=-1, keepdims=True)
        probs[h] = pr
        heads[:, h * hd:(h + 1) * hd] = dot(pr.astype(BF), vb).astype(BF)
    w_cp['o'].wait()
    rs_wait_sends(R_EMB)
    rs_start(R_ATT, lambda c: dot(heads[...], wov[:, c]))

    w_cp['g'].wait()
    w_cp['u'].wait()
    with jax.named_scope('wgut'):
        for b in range(2 * ffn // tw):
            wgut[b * tw:(b + 1) * tw, :] = dot(eye, wguv[:, b * tw:(b + 1) * tw], NT).astype(BF)
    ag_finish(0, GH)
    w_cp['d'].wait()

    ag_wait_sends(N1)
    aw = 256
    for j in range(RS_CHUNKS[R_ATT]):
        c = rs_cols(R_ATT, j)
        h1 = (x0f[:, c] + rs_finish(R_ATT, j).astype(BF).astype(F32)).astype(BF)
        h1f[:, c] = h1.astype(F32)
        h1g[me, :, c] = h1
        ag_start(N2, j)
        if j * aw < ffn:
            with jax.named_scope('gact'):
                k = slice(j * aw, (j + 1) * aw)
                gact[:, k] = dot(gathered(GH), wdv[k, :], NT).astype(BF).astype(F32)
    norm_fwd(N2, 1, gm, o_n2)

    n2 = o_n2[...].reshape(seq, dim)
    fw = 256
    for j in range(ffn // fw):
        c = slice(j * fw, (j + 1) * fw)
        cu = slice(ffn + j * fw, ffn + (j + 1) * fw)
        gate = dot(n2, wguv[:, c])
        up = dot(n2, wguv[:, cu])
        sig = jax.nn.sigmoid(gate)
        ga_act = gate * sig
        act[:, c] = (ga_act * up).astype(BF)
        g = gact[:, c]
        gcat[:, cu] = (g * ga_act).astype(BF)
        gcat[:, c] = (g * up * sig * (1.0 + gate * (1.0 - sig))).astype(BF)
    rs_wait_sends(R_ATT)
    rs_start(R_GN2, lambda c: dot(gcat[...], wgut[:, c]))
    for j in range(RS_CHUNKS[R_MLP]):
        rs_local(R_MLP, j, dot(act[...], wdv[:, rs_cols(R_MLP, j)]))

    ag_wait_sends(N2)
    for j in range(RS_CHUNKS[R_GN2]):
        gn2g[me, :, rs_cols(R_GN2, j)] = rs_finish(R_GN2, j).astype(BF)
        ag_start(GH1, j)

    def mlp_cross():
        for j in range(RS_CHUNKS[R_MLP]):
            rs_cross(R_MLP, j)

    ghd_parts = []
    norm_bwd(GH1, N2, 1, gm, o_gh, o_gh1, gain_m, early=mlp_cross, use=lambda a, c: ghd_parts.append(dot(a, wov[:, c], NT)))
    ghd = sum(ghd_parts[1:], ghd_parts[0]).astype(BF)

    gv = jnp.zeros((seq, hd), F32)
    gk = jnp.zeros((seq, hd), F32)
    for h in range(local_heads):
        g = ghd[:, h * hd:(h + 1) * hd]
        pr = probs[h]
        gp = dot(g, vb, NT).astype(BF).astype(F32)
        gv = gv + dot(pr.astype(BF), g, TN)
        gs = (pr * (gp - jnp.sum(gp * pr, axis=-1, keepdims=True)) * scale).astype(BF)
        gq = dot(gs, kb).astype(BF).astype(F32)
        gk = gk + dot(gs, qkvb[:, h * hd:(h + 1) * hd], TN)
        gqkv[:, h * hd:(h + 1) * hd] = rotate(gq, -1.0).astype(BF)
    gqkv[:, qw:qw + hd] = rotate(gk.astype(BF).astype(F32), -1.0).astype(BF)
    gqkv[:, qw + hd:] = gv.astype(BF)
    rs_wait_sends(R_GN2)
    rs_start(R_GN1, lambda c: dot(gqkv[...], wqkvt[:, c]))

    ag_wait_sends(GH1)
    for j in range(RS_CHUNKS[R_GN1]):
        gn1g[me, :, rs_cols(R_GN1, j)] = rs_finish(R_GN1, j).astype(BF)
        ag_start(GF, j)
    hid[...] = (h1f[...] + rs_finish(R_MLP).astype(BF).astype(F32)).astype(BF)
    norm_bwd(GF, N1, 0, ga, o_gh1, o_gf, gain_a)
    with jax.named_scope('tail_send'):
        rs_wait_sends(R_GN1)
        rs_wait_sends(R_MLP)
        ag_wait_sends(GH)
        ag_wait_sends(GF)


def grads_kernel(n_tp, local_heads,
                 tok, gain_m, gain_a, hid, gh, act, n2, gcat, gh1, heads, n1, gqkv, gf,
                 o_hid, o_emb, o_wq, o_wk, o_wv, o_wo, o_wg, o_wu, o_wd, o_ga, o_gm,
                 wide, tall, qbuf, kvbuf, s_wide, s_tall, s_qkv, s_out):
    seq, dim = n1.shape
    rows = o_emb.shape[0]
    ffn = act.shape[1]
    hd = gqkv.shape[1] // (local_heads + 2)
    me = lax.axis_index('tp')
    n_wide, wr = wide.shape[0], wide.shape[1]
    n_tall, tr = tall.shape[0], tall.shape[1]
    busy = {}

    def put(key, src, dst, sem):
        cp = pltpu.make_async_copy(src, dst, sem)
        cp.start()
        busy[key] = cp

    def free(key):
        if key in busy:
            busy.pop(key).wait()

    row = lax.broadcasted_iota(jnp.int32, (wr, seq), 0)
    wide_units = []
    for u in range(ffn // wr):
        wide_units.append((lambda u=u: dot(act[:, u * wr:(u + 1) * wr], gh[...], TN), o_wd.at[pl.ds(u * wr, wr)]))
    for u in range(heads.shape[1] // wr):
        wide_units.append((lambda u=u: dot(heads[:, u * wr:(u + 1) * wr], gh1[...], TN), o_wo.at[pl.ds(u * wr, wr)]))
    for u in range(rows // wr):
        wide_units.append((lambda u=u: dot(jnp.where(row + u * wr == tok[...] - me * rows, 1.0, 0.0).astype(BF), gf[...]),
                           o_emb.at[pl.ds(u * wr, wr)]))
    tall_units = []
    for half, out in ((0, o_wg), (1, o_wu)):
        for u in range(dim // tr):
            tall_units.append((lambda u=u, half=half: dot(n2[:, u * tr:(u + 1) * tr], gcat[:, half * ffn:(half + 1) * ffn], TN),
                               out.at[pl.ds(u * tr, tr)]))
    iw = it = 0
    while iw < len(wide_units) or it < len(tall_units):
        if iw < len(wide_units):
            slot = iw % n_wide
            fn, dst = wide_units[iw]
            free(('w', slot))
            with jax.named_scope(f'wide_{iw}'):
                wide[slot] = fn()
                put(('w', slot), wide.at[slot], dst, s_wide.at[slot])
            iw += 1
        if it < len(tall_units):
            slot = it % n_tall
            fn, dst = tall_units[it]
            free(('t', slot))
            with jax.named_scope(f'tall_{it}'):
                tall[slot] = fn()
                put(('t', slot), tall.at[slot], dst, s_tall.at[slot])
            it += 1
    put(('out', 0), hid, o_hid, s_out.at[0])
    put(('out', 1), gain_a, o_ga, s_out.at[1])
    put(('out', 2), gain_m, o_gm, s_out.at[2])
    qw = local_heads * hd
    with jax.named_scope('qkv'):
        for h in range(local_heads):
            qbuf[pl.ds(h, dim, stride=local_heads), :] = dot(n1[...], gqkv[:, h * hd:(h + 1) * hd], TN)
        put(('q', 0), qbuf, o_wq, s_qkv.at[2])
        for i, out in enumerate((o_wk, o_wv)):
            kvbuf[i] = dot(n1[...], gqkv[:, qw + i * hd:qw + (i + 1) * hd], TN)
            put(('k', i), kvbuf.at[i], out, s_qkv.at[i])

    with jax.named_scope('drain'):
        for key in list(busy):
            free(key)


def solution(mesh):
    n_tp = mesh.shape['tp']
    chips = n_tp // 2
    in_specs = (P('dp', None), P('dp', None), P('tp', None), P(None), P(None),
                P(None, 'tp', None), P(None, 'tp', None), P(None, 'tp', None), P('tp', None, None),
                P(None, 'tp'), P(None, 'tp'), P('tp', None), P('dp', 'tp', None))
    out_specs = (P('dp', 'tp', None), P(('dp', 'tp'), None),
                 P('dp', 'tp', None), P('dp', 'tp', None), P('dp', 'tp', None), P(('dp', 'tp'), None, None),
                 P('dp', 'tp'), P('dp', 'tp'), P(('dp', 'tp'), None), P('dp'), P('dp'))

    def device_fn(tokens, positions, emb, gain_attn, gain_mlp, w_query, w_key, w_value, w_out, w_gate, w_up, w_down, grad_hidden):
        seq = tokens.shape[1]
        rows, dim = emb.shape
        lh, hd = w_query.shape[1], w_query.shape[2]
        ffn = w_down.shape[0]
        blk = grad_hidden.shape[1]
        qkvw = (lh + 2) * hd
        inv_freq = (np.float32(ROPE_THETA) ** (-np.arange(hd // 2, dtype=np.float32) * np.float32(2.0 / hd))).astype(np.float32)
        invf = jnp.asarray(np.concatenate([inv_freq, inv_freq])[None, :])

        def sds(shape, dt=BF):
            return jax.ShapeDtypeStruct(shape, dt)

        hb = pl.BlockSpec(memory_space=pltpu.HBM)
        vm = pl.BlockSpec(memory_space=pltpu.VMEM)
        maxc = max(RS_CHUNKS.values())
        mid = pl.pallas_call(
            functools.partial(layer_kernel, n_tp, lh),
            name='layer',
            out_shape=[sds((n_tp, blk, dim))] * 5 + [sds((seq, ffn)), sds((seq, 2 * ffn)), sds((seq, lh * hd)), sds((seq, qkvw)),
                                                    sds((1, dim), F32), sds((1, dim), F32), sds((blk, dim))],
            in_specs=[hb] * 14,
            out_specs=[vm] * 12,
            scratch_shapes=[
                pltpu.VMEM((1, seq), jnp.int32), pltpu.VMEM((1, seq), jnp.int32), pltpu.VMEM((1, hd), F32),
                pltpu.VMEM((1, dim), F32), pltpu.VMEM((1, dim), F32), pltpu.VMEM((blk, dim), BF),
                pltpu.VMEM((rows, dim), BF), pltpu.VMEM((seq, rows), BF), pltpu.VMEM((dim * lh, hd), BF), pltpu.VMEM((dim * lh, hd), F32),
                pltpu.VMEM((dim, qkvw), BF), pltpu.VMEM((lh * hd, dim), BF), pltpu.VMEM((dim, 2 * ffn), BF), pltpu.VMEM((ffn, dim), BF),
                pltpu.VMEM((5, chips, 2, blk, dim), BF), pltpu.VMEM((5, chips, blk, dim), BF),
                pltpu.VMEM((5, chips, blk, dim), BF), pltpu.VMEM((5, chips - 1, blk, dim), BF),
                pltpu.VMEM((n_tp, blk, dim), BF), pltpu.VMEM((n_tp, blk, dim), BF), pltpu.VMEM((n_tp, blk, dim), BF),
                pltpu.VMEM((n_tp, blk, dim), BF), pltpu.VMEM((2 * ffn, dim), BF), pltpu.VMEM((qkvw, dim), BF), pltpu.VMEM((blk, dim), F32), pltpu.VMEM((blk, dim), F32),
                pltpu.VMEM((2, seq, hd), F32), pltpu.VMEM((seq, ffn), F32), pltpu.VMEM((seq, qkvw), BF),
                pltpu.VMEM((2, seq, hd), F32), pltpu.VMEM((lh, seq, seq), F32),
                pltpu.SemaphoreType.DMA((2, 2)), pltpu.SemaphoreType.DMA(((max(AG_CHUNKS.values()) + 1) * (2 * chips - 1),)),
                pltpu.SemaphoreType.DMA((2, 2)), pltpu.SemaphoreType.DMA((2, maxc, chips)),
                pltpu.SemaphoreType.DMA((18,)),
            ],
            compiler_params=pltpu.CompilerParams(collective_id=0, has_side_effects=True, vmem_limit_bytes=44 * 1024 * 1024),
        )(*(pltpu.with_memory_space_constraint(a, pltpu.HBM) for a in (
            tokens, positions, invf, gain_attn.reshape(1, dim), gain_mlp.reshape(1, dim), grad_hidden.reshape(blk, dim),
            emb, w_query.reshape(dim * lh, hd), w_key.reshape(dim, hd), w_value.reshape(dim, hd), w_out.reshape(lh * hd, dim),
            w_gate, w_up, w_down)))
        n1, n2, gh, gh1, gf, act, gcat, heads, gqkv, gain_m, gain_a, hid = mid
        n1, n2, gh, gh1, gf = (a.reshape(seq, dim) for a in (n1, n2, gh, gh1, gf))
        wide_rows, tall_rows = 256, 512
        res = pl.pallas_call(
            functools.partial(grads_kernel, n_tp, lh),
            name='grads',
            out_shape=[sds((blk, dim)), sds((rows, dim), F32), sds((dim * lh, hd), F32), sds((dim, hd), F32), sds((dim, hd), F32),
                       sds((lh * hd, dim), F32), sds((dim, ffn), F32), sds((dim, ffn), F32), sds((ffn, dim), F32),
                       sds((1, dim), F32), sds((1, dim), F32)],
            in_specs=[vm] * 13,
            out_specs=[hb] * 11,
            scratch_shapes=[
                pltpu.VMEM((3, wide_rows, dim), F32), pltpu.VMEM((3, tall_rows, ffn), F32), pltpu.VMEM((dim * lh, hd), F32),
                pltpu.VMEM((2, dim, hd), F32),
                pltpu.SemaphoreType.DMA((3,)), pltpu.SemaphoreType.DMA((3,)), pltpu.SemaphoreType.DMA((3,)),
                pltpu.SemaphoreType.DMA((3,)),
            ],
            compiler_params=pltpu.CompilerParams(vmem_limit_bytes=24 * 1024 * 1024),
        )(tokens, gain_m, gain_a, hid, gh, act, n2, gcat, gh1, heads, n1, gqkv, gf)
        o_hid, o_emb, o_wq, o_wk, o_wv, o_wo, o_wg, o_wu, o_wd, o_ga, o_gm = res
        return (o_hid.reshape(1, blk, dim), o_emb, o_wq.reshape(dim, lh, hd), o_wk.reshape(dim, 1, hd), o_wv.reshape(dim, 1, hd),
                o_wo.reshape(lh, hd, dim), o_wg, o_wu, o_wd, o_ga.reshape(dim), o_gm.reshape(dim))

    return jax.shard_map(device_fn, mesh=mesh, in_specs=in_specs, out_specs=out_specs, check_vma=False)
```

```python
import functools

import jax
import jax.numpy as jnp
import numpy as np
from jax import lax
from jax.experimental import pallas as pl
from jax.experimental.pallas import tpu as pltpu
from jax.sharding import PartitionSpec as P

ROPE_THETA = 1000000.0
RMS_EPS = 1e-5
MESH = pl.DeviceIdType.MESH
BF = jnp.bfloat16
F32 = jnp.float32
NT = (((1,), (1,)), ((), ()))
TN = (((0,), (0,)), ((), ()))

N1, GH, N2, GH1, GF = range(5)
R_EMB, R_ATT, R_GN2, R_MLP, R_GN1 = range(5)
RS_CHUNKS = {R_EMB: 4, R_ATT: 4, R_GN2: 4, R_MLP: 2, R_GN1: 4}
AG_CHUNKS = {N1: 4, GH: 1, N2: 4, GH1: 4, GF: 4}


def dot(a, b, dims=(((1,), (0,)), ((), ()))):
    return lax.dot_general(a, b, dims, preferred_element_type=F32)


def scoped(name):
    def wrap(fn):
        def run(p, *rest, **kw):
            with jax.named_scope(f'{name}_{p}'):
                return fn(p, *rest, **kw)
        return run
    return wrap


def layer_kernel(n_tp, local_heads,
                 h_tok, h_pos, h_invf, h_ga, h_gm, h_gh, emb, wq4, wk, wv, wo, wg, wu, wd,
                 o_n1, o_n2, o_gh, o_gh1, o_gf, act, gcat, heads, gqkv, gain_m, gain_a, hid,
                 tok, pos, invf, ga, gm, gh_in, embv, onehot, wqr, wqf, wqkv, wov, wguv, wdv, pb, rd, sb, rr,
                 x0g, h1g, gn2g, gn1g, wgut, wqkvt, wovt, x0f, h1f, inv, gact, qkvb, tabs, probs,
                 ag_s, ag_r, rs_s, rs_r, loc):
    chips = n_tp // 2
    seq = h_tok.shape[1]
    rows, dim = emb.shape
    ffn = wd.shape[0]
    blk = gh_in.shape[0]
    hd = wk.shape[1]
    scale = hd ** -0.5
    qw = local_heads * hd

    me = lax.axis_index('tp')
    chip = me // 2
    core = lax.rem(me, 2)
    sib = 2 * chip + 1 - core

    def peer_chip(d):
        return lax.rem(chip + d, chips)

    def peer(d):
        return 2 * peer_chip(d) + core

    order = sorted(range(1, chips), key=lambda d: -min(d, chips - d))

    barrier = pltpu.get_barrier_semaphore()
    for dev in [sib] + [peer(d) for d in range(1, chips)]:
        pl.semaphore_signal(barrier, inc=1, device_id={'tp': dev}, device_id_type=MESH)

    nloc = [1]

    def local(src, dst, slot=None):
        if slot is None:
            slot = nloc[0]
            nloc[0] += 1
        cp = pltpu.make_async_copy(src, dst, loc.at[slot])
        cp.start()
        return cp

    n_emb = RS_CHUNKS[R_EMB]
    ew = dim // n_emb

    def emb_load(j):
        return local(emb.at[:, pl.ds(j * ew, ew)], embv.at[:, pl.ds(j * ew, ew)])

    in_cp = [local(h_tok, tok)]
    emb_cp = [emb_load(j) for j in range(3)]
    in_cp += [local(a, b) for a, b in ((h_pos, pos), (h_invf, invf), (h_ga, ga), (h_gm, gm), (h_gh, gh_in))]
    in_cp[0].wait()

    tok_t = jnp.transpose(jnp.broadcast_to(tok[...].astype(F32), (seq, seq)))
    tok_t = tok_t - (me * rows).astype(F32)
    lane = lax.broadcasted_iota(jnp.int32, (seq, seq), 1).astype(F32)
    for b in range(rows // seq):
        onehot[:, b * seq:(b + 1) * seq] = jnp.where(tok_t == lane + float(b * seq), 1.0, 0.0).astype(BF)

    def remote(src, dst, s, r, dev):
        return pltpu.make_async_remote_copy(src_ref=src, dst_ref=dst, send_sem=s, recv_sem=r,
                                            device_id={'tp': dev}, device_id_type=MESH)

    def send(*args):
        remote(*args).start()

    near = sorted(range(1, chips), key=lambda d: min(d, chips - d))
    incoming = [(d, c) for d in near for c in (1, 0)]

    ag_set = {N1: 0, N2: 0, GH1: 0, GF: 0, GH: 1}
    ag = {N1: x0g, GH: o_gh, N2: h1g, GH1: gn2g, GF: gn1g}
    per = 2 * chips - 1

    def ag_view(p, t, j):
        w = dim // AG_CHUNKS[p]
        return ag[p].at[t, :, pl.ds(j * w, w)]

    def ag_block(p, d, c, j):
        return ag_view(p, 2 * lax.rem(chip + chips - d, chips) + c, j)

    def ag_recv(p, j, i):
        return ag_r.at[(per * j if ag_set[p] == 0 else ag_r.shape[0] - per) + i]

    def ag_wait_sends(p):
        own, passed = ag[p].at[pl.ds(0, chips)], ag[p].at[pl.ds(0, n_tp - 2)]
        remote(own, own, ag_s.at[ag_set[p], 0], ag_recv(p, 0, 0), sib).wait_send()

        @pl.when(core == 1)
        def _():
            remote(passed, passed, ag_s.at[ag_set[p], 1], ag_recv(p, 0, 0), sib).wait_send()

    @scoped('ag_start')
    def ag_start(p, only=None):
        q = ag_set[p]
        for j in range(AG_CHUNKS[p]) if only is None else (only,):
            mine = ag_view(p, me, j)
            for d in order:
                send(mine, mine, ag_s.at[q, 0], ag_recv(p, j, 2 * d - core), 2 * peer_chip(d) + 1)
            send(mine, mine, ag_s.at[q, 0], ag_recv(p, j, 0), sib)

    @scoped('ag_finish')
    def ag_finish(j, *ps, early=None, forward=True, collect=True, between=None):
        if j == 0 and forward:
            @pl.when(core == 1)
            def _():
                for k in range(AG_CHUNKS[ps[0]]):
                    for d, c in incoming:
                        for p in ps:
                            got = ag_block(p, d, c, k)
                            q = ag_set[p]
                            remote(got, got, ag_s.at[q, 1], ag_recv(p, k, 2 * d - c), sib).wait_recv()
                            send(got, got, ag_s.at[q, 1], ag_recv(p, k, 2 * d - c), sib)
                    if early is not None and k == 1:
                        early()
                    if between is not None and k < AG_CHUNKS[ps[0]] - 1:
                        between(k)

        if not collect:
            return
        for p in ps:
            got = ag_view(p, sib, j)
            remote(got, got, ag_s.at[ag_set[p], 0], ag_recv(p, j, 0), sib).wait_recv()

        @pl.when(core == 0)
        def _():
            for i, (d, c) in enumerate(incoming):
                if i == 2 and early is not None:
                    early()
                for p in ps:
                    got = ag_block(p, d, c, j)
                    remote(got, got, ag_s.at[ag_set[p], 1], ag_recv(p, j, 2 * d - c), sib).wait_recv()

    def gathered(p, j=None):
        if j is None:
            return ag[p][...].reshape(seq, dim)
        w = dim // AG_CHUNKS[p]
        return ag[p][:, :, j * w:(j + 1) * w].reshape(seq, w)

    def gathered_dot(p, weight, early):
        w = dim // AG_CHUNKS[p]
        total = None
        for j in range(AG_CHUNKS[p]):
            ag_finish(j, p, early=early if j == 0 else None)
            part = weight(gathered(p, j), slice(j * w, (j + 1) * w))
            total = part if total is None else total + part
        return total

    rs_set = {R_EMB: 0, R_ATT: 0, R_GN2: 0, R_GN1: 0, R_MLP: 1}

    def rs_wait_sends(p):
        q = rs_set[p]
        remote(rd.at[p], rd.at[p], rs_s.at[q, 0], rs_r.at[q, 0, 0], sib).wait_send()
        remote(rr.at[p], rr.at[p], rs_s.at[q, 1], rs_r.at[q, 0, 0], sib).wait_send()

    def rs_cols(p, j):
        w = dim // RS_CHUNKS[p]
        return slice(j * w, (j + 1) * w)

    @scoped('rs_local')
    def rs_local(p, j, val):
        c = rs_cols(p, j)
        w = c.stop - c.start
        pb[p, :, :, :, c] = val.astype(BF).reshape(chips, 2, blk, w)
        send(pb.at[p, :, 1 - core, :, c], rd.at[p, :, :, c], rs_s.at[rs_set[p], 0], rs_r.at[rs_set[p], j, 0], sib)

    @scoped('rs_cross')
    def rs_cross(p, j):
        c = rs_cols(p, j)
        remote(rd.at[p, :, :, c], rd.at[p, :, :, c], rs_s.at[rs_set[p], 0], rs_r.at[rs_set[p], j, 0], sib).wait_recv()
        for d in order:
            to = peer_chip(d)
            both = pb[p, to, core, :, c].astype(F32) + rd[p, to, :, c].astype(F32)
            sb[p, to, :, c] = both.astype(BF)
            send(sb.at[p, to, :, c], rr.at[p, d - 1, :, c], rs_s.at[rs_set[p], 1], rs_r.at[rs_set[p], j, d], peer(d))

    @scoped('rs_finish')
    def rs_finish(p, only=None):
        parts = []
        for j in range(RS_CHUNKS[p]) if only is None else (only,):
            c = rs_cols(p, j)
            total = pb[p, chip, core, :, c].astype(F32) + rd[p, chip, :, c].astype(F32)
            for d in order[::-1]:
                remote(rr.at[p, d - 1, :, c], rr.at[p, d - 1, :, c], rs_s.at[rs_set[p], 1], rs_r.at[rs_set[p], j, d], sib).wait_recv()
                total = total + rr[p, d - 1, :, c].astype(F32)
            parts.append(total)
        return jnp.concatenate(parts, axis=1)

    def rs_start(p, chunk):
        n = RS_CHUNKS[p]
        for j in range(n):
            val = chunk(rs_cols(p, j))
            if p == R_EMB and j == 0:
                with jax.named_scope('barrier'):
                    pl.semaphore_wait(barrier, chips)
            rs_local(p, j, val)
            if j > 0:
                @pl.when(core == 0)
                def _():
                    rs_cross(p, j - 1)

        @pl.when(core == 0)
        def _():
            rs_cross(p, n - 1)

        @pl.when(core == 1)
        def _():
            for j in range(n):
                rs_cross(p, j)

    def on_core(k, fn):
        @pl.when(core == k)
        def _():
            fn()

    def spread(v):
        return jnp.broadcast_to(v, (seq, hd))

    def norm_fwd(p, slot, gain, out, early=None, between=None):
        square = None
        for j in range(AG_CHUNKS[p]):
            ag_finish(j, p, early=early if j == 0 else None, between=between)
            if between is not None and j < AG_CHUNKS[p] - 1:
                on_core(0, lambda: between(j))
            part = gathered(p, j).astype(F32)
            part = jnp.sum(part * part, axis=-1, keepdims=True)
            square = part if square is None else square + part
        r = lax.rsqrt(square * (1.0 / dim) + RMS_EPS)
        inv[slot] = spread(r)
        w = dim // AG_CHUNKS[p]
        for j in range(AG_CHUNKS[p]):
            c = slice(j * w, (j + 1) * w)
            out[:, :, c] = (gathered(p, j).astype(F32) * r * gain[:, c]).astype(BF).reshape(n_tp, blk, w)

    def norm_bwd(p, p_in, slot, gain, around, out, gain_out, early=None, use=None):
        w = dim // AG_CHUNKS[p]
        r = inv[slot][:, :1]
        both = None
        for j in range(AG_CHUNKS[p]):
            c = slice(j * w, (j + 1) * w)
            ag_finish(j, p, early=early if j == 0 else None)
            g = gathered(p, j).astype(F32)
            n = gathered(p_in, j).astype(F32) * r
            gn = g * n
            gain_out[:, c] = jnp.sum(gn, axis=0, keepdims=True)
            part = jnp.sum(gn * gain[:, c], axis=-1, keepdims=True)
            both = part if both is None else both + part
        mean = both * (1.0 / dim)
        for j in range(AG_CHUNKS[p]):
            c = slice(j * w, (j + 1) * w)
            n = gathered(p_in, j).astype(F32) * r
            g_in = r * (gathered(p, j).astype(F32) * gain[:, c] - n * mean)
            total = (around[:, :, c].reshape(seq, w).astype(F32) + g_in).astype(BF)
            out[:, :, c] = total.reshape(n_tp, blk, w)
            if use is not None:
                use(total, c)

    w_cp = {}

    def emb_chunk(c):
        j = c.start // ew
        emb_cp[j].wait()
        if j + 3 < n_emb:
            emb_cp.append(emb_load(j + 3))
        if j == n_emb - 2:
            w_cp['k'] = local(wk, wqkv.at[:, pl.ds(qw, hd)])
            w_cp['v'] = local(wv, wqkv.at[:, pl.ds(qw + hd, hd)])
            w_cp['q'] = local(wq4, wqr)
        if j == n_emb - 1:
            w_cp['o'] = local(wo, wov)
            w_cp['g'] = local(wg, wguv.at[:, pl.ds(0, ffn)])
            w_cp['u'] = local(wu, wguv.at[:, pl.ds(ffn, ffn)])
            w_cp['d'] = local(wd, wdv)
        return dot(onehot[...], embv[:, c])

    rs_start(R_EMB, emb_chunk)

    in_cp[1].wait()
    in_cp[2].wait()
    pos_t = jnp.transpose(jnp.broadcast_to(pos[...].astype(F32), (seq, seq)))
    angle = pos_t * invf[...]
    half = lax.broadcasted_iota(jnp.int32, (seq, hd), 1) < hd // 2
    tabs[0] = jnp.cos(angle)
    sin = jnp.sin(angle)
    tabs[1] = jnp.where(half, -sin, sin)
    for cp in in_cp[3:]:
        cp.wait()
    for j in range(RS_CHUNKS[R_EMB]):
        part = rs_finish(R_EMB, j)
        x0f[:, rs_cols(R_EMB, j)] = part
        x0g[me, :, rs_cols(R_EMB, j)] = part.astype(BF)
        ag_start(N1, j)
    o_gh[me] = gh_in[...]
    w_cp['k'].wait()
    w_cp['v'].wait()
    w_cp['q'].wait()
    wqf[...] = wqr[...].astype(F32)
    for h in range(local_heads):
        wqkv[:, h * hd:(h + 1) * hd] = wqf[pl.ds(h, dim, stride=local_heads), :].astype(BF)


    tw = 256
    eye = (lax.broadcasted_iota(jnp.int32, (tw, tw), 0) == lax.broadcasted_iota(jnp.int32, (tw, tw), 1)).astype(F32).astype(BF)
    with jax.named_scope('wqkvt'):
        for b in range((qw + 2 * hd) // tw):
            wqkvt[b * tw:(b + 1) * tw, :] = dot(eye, wqkv[:, b * tw:(b + 1) * tw], NT).astype(BF)

    def rotate(v, sign):
        return v * tabs[0] + sign * (pltpu.roll(v, hd // 2, 1) * tabs[1])

    w_cp['g'].wait()
    w_cp['u'].wait()

    def transpose_gate_up(k):
        with jax.named_scope('wgut'):
            n = 2 * ffn // tw
            for b in range(n * k // 3, n * (k + 1) // 3):
                wgut[b * tw:(b + 1) * tw, :] = dot(eye, wguv[:, b * tw:(b + 1) * tw], NT).astype(BF)

    norm_fwd(N1, 0, ga, o_n1, early=lambda: ag_start(GH), between=transpose_gate_up)
    qkv = dot(o_n1[...].reshape(seq, dim), wqkv[...])
    for h in range(local_heads + 1):
        qkvb[:, h * hd:(h + 1) * hd] = rotate(qkv[:, h * hd:(h + 1) * hd], 1.0).astype(BF)
    qkvb[:, qw + hd:] = qkv[:, qw + hd:].astype(BF)
    kb = qkvb[:, qw:qw + hd]
    vb = qkvb[:, qw + hd:]
    causal = lax.broadcasted_iota(jnp.int32, (seq, seq), 0) >= lax.broadcasted_iota(jnp.int32, (seq, seq), 1)
    for h in range(local_heads):
        s = dot(qkvb[:, h * hd:(h + 1) * hd], kb, NT) * scale
        s = jnp.where(causal, s, -1e30)
        e = jnp.exp(s - jnp.max(s, axis=-1, keepdims=True))
        pr = e / jnp.sum(e, axis=-1, keepdims=True)
        probs[h] = pr
        heads[:, h * hd:(h + 1) * hd] = dot(pr.astype(BF), vb).astype(BF)
    w_cp['o'].wait()
    rs_wait_sends(R_EMB)
    rs_start(R_ATT, lambda c: dot(heads[...], wov[:, c]))

    with jax.named_scope('wovt'):
        for b in range(dim // tw):
            wovt[b * tw:(b + 1) * tw, :] = dot(eye, wov[:, b * tw:(b + 1) * tw], NT).astype(BF)
    ag_finish(0, GH, collect=False)
    w_cp['d'].wait()

    ag_wait_sends(N1)
    for j in range(RS_CHUNKS[R_ATT]):
        c = rs_cols(R_ATT, j)
        h1 = (x0f[:, c] + rs_finish(R_ATT, j).astype(BF).astype(F32)).astype(BF)
        h1f[:, c] = h1.astype(F32)
        h1g[me, :, c] = h1
        ag_start(N2, j)
    ag_finish(0, GH, forward=False)

    def act_grad(k):
        if k == 0:
            with jax.named_scope('gact'):
                gact[...] = dot(gathered(GH), wdv[...], NT).astype(BF).astype(F32)

    norm_fwd(N2, 1, gm, o_n2, between=act_grad)

    n2 = o_n2[...].reshape(seq, dim)
    fw = 256
    for j in range(ffn // fw):
        c = slice(j * fw, (j + 1) * fw)
        cu = slice(ffn + j * fw, ffn + (j + 1) * fw)
        gate = dot(n2, wguv[:, c])
        up = dot(n2, wguv[:, cu])
        sig = jax.nn.sigmoid(gate)
        ga_act = gate * sig
        act[:, c] = (ga_act * up).astype(BF)
        g = gact[:, c]
        gcat[:, cu] = (g * ga_act).astype(BF)
        gcat[:, c] = (g * up * sig * (1.0 + gate * (1.0 - sig))).astype(BF)
    rs_wait_sends(R_ATT)
    rs_start(R_GN2, lambda c: dot(gcat[...], wgut[:, c]))
    for j in range(RS_CHUNKS[R_MLP]):
        rs_local(R_MLP, j, dot(act[...], wdv[:, rs_cols(R_MLP, j)]))

    ag_wait_sends(N2)
    for j in range(RS_CHUNKS[R_GN2]):
        gn2g[me, :, rs_cols(R_GN2, j)] = rs_finish(R_GN2, j).astype(BF)
        ag_start(GH1, j)

    def mlp_cross():
        for j in range(RS_CHUNKS[R_MLP]):
            rs_cross(R_MLP, j)

    ghd_parts = []
    norm_bwd(GH1, N2, 1, gm, o_gh, o_gh1, gain_m, early=mlp_cross, use=lambda a, c: ghd_parts.append(dot(a, wovt[c, :])))
    ghd = sum(ghd_parts[1:], ghd_parts[0]).astype(BF)

    gv = jnp.zeros((seq, hd), F32)
    gk = jnp.zeros((seq, hd), F32)
    for h in range(local_heads):
        g = ghd[:, h * hd:(h + 1) * hd]
        pr = probs[h]
        gp = dot(g, vb, NT).astype(BF).astype(F32)
        gv = gv + dot(pr.astype(BF), g, TN)
        gs = (pr * (gp - jnp.sum(gp * pr, axis=-1, keepdims=True)) * scale).astype(BF)
        gq = dot(gs, kb).astype(BF).astype(F32)
        gk = gk + dot(gs, qkvb[:, h * hd:(h + 1) * hd], TN)
        gqkv[:, h * hd:(h + 1) * hd] = rotate(gq, -1.0).astype(BF)
    gqkv[:, qw:qw + hd] = rotate(gk.astype(BF).astype(F32), -1.0).astype(BF)
    gqkv[:, qw + hd:] = gv.astype(BF)
    rs_wait_sends(R_GN2)
    rs_start(R_GN1, lambda c: dot(gqkv[...], wqkvt[:, c]))

    ag_wait_sends(GH1)
    for j in range(RS_CHUNKS[R_GN1]):
        gn1g[me, :, rs_cols(R_GN1, j)] = rs_finish(R_GN1, j).astype(BF)
        ag_start(GF, j)
    hid[...] = (h1f[...] + rs_finish(R_MLP).astype(BF).astype(F32)).astype(BF)
    norm_bwd(GF, N1, 0, ga, o_gh1, o_gf, gain_a)
    with jax.named_scope('tail_send'):
        rs_wait_sends(R_GN1)
        rs_wait_sends(R_MLP)
        ag_wait_sends(GH)
        ag_wait_sends(GF)


def grads_kernel(n_tp, local_heads,
                 tok, gain_m, gain_a, hid, gh, act, n2, gcat, gh1, heads, n1, gqkv, gf,
                 o_hid, o_emb, o_wq, o_wk, o_wv, o_wo, o_wg, o_wu, o_wd, o_ga, o_gm,
                 wide, tall, qbuf, kvbuf, s_wide, s_tall, s_qkv, s_out):
    seq, dim = n1.shape
    rows = o_emb.shape[0]
    ffn = act.shape[1]
    hd = gqkv.shape[1] // (local_heads + 2)
    me = lax.axis_index('tp')
    n_wide, wr = wide.shape[0], wide.shape[1]
    n_tall, tr = tall.shape[0], tall.shape[1]
    busy = {}

    def put(key, src, dst, sem):
        cp = pltpu.make_async_copy(src, dst, sem)
        cp.start()
        busy[key] = cp

    def free(key):
        if key in busy:
            busy.pop(key).wait()

    row = lax.broadcasted_iota(jnp.int32, (wr, seq), 0)
    wide_units = []
    for u in range(ffn // wr):
        wide_units.append((lambda u=u: dot(act[:, u * wr:(u + 1) * wr], gh[...], TN), o_wd.at[pl.ds(u * wr, wr)]))
    for u in range(heads.shape[1] // wr):
        wide_units.append((lambda u=u: dot(heads[:, u * wr:(u + 1) * wr], gh1[...], TN), o_wo.at[pl.ds(u * wr, wr)]))
    for u in range(rows // wr):
        wide_units.append((lambda u=u: dot(jnp.where(row + u * wr == tok[...] - me * rows, 1.0, 0.0).astype(BF), gf[...]),
                           o_emb.at[pl.ds(u * wr, wr)]))
    tall_units = []
    for half, out in ((0, o_wg), (1, o_wu)):
        for u in range(dim // tr):
            tall_units.append((lambda u=u, half=half: dot(n2[:, u * tr:(u + 1) * tr], gcat[:, half * ffn:(half + 1) * ffn], TN),
                               out.at[pl.ds(u * tr, tr)]))
    iw = it = 0
    while iw < len(wide_units) or it < len(tall_units):
        if iw < len(wide_units):
            slot = iw % n_wide
            fn, dst = wide_units[iw]
            free(('w', slot))
            with jax.named_scope(f'wide_{iw}'):
                wide[slot] = fn()
                put(('w', slot), wide.at[slot], dst, s_wide.at[slot])
            iw += 1
        if it < len(tall_units):
            slot = it % n_tall
            fn, dst = tall_units[it]
            free(('t', slot))
            with jax.named_scope(f'tall_{it}'):
                tall[slot] = fn()
                put(('t', slot), tall.at[slot], dst, s_tall.at[slot])
            it += 1
    put(('out', 0), hid, o_hid, s_out.at[0])
    put(('out', 1), gain_a, o_ga, s_out.at[1])
    put(('out', 2), gain_m, o_gm, s_out.at[2])
    qw = local_heads * hd
    with jax.named_scope('qkv'):
        for h in range(local_heads):
            qbuf[pl.ds(h, dim, stride=local_heads), :] = dot(n1[...], gqkv[:, h * hd:(h + 1) * hd], TN)
        put(('q', 0), qbuf, o_wq, s_qkv.at[2])
        for i, out in enumerate((o_wk, o_wv)):
            kvbuf[i] = dot(n1[...], gqkv[:, qw + i * hd:qw + (i + 1) * hd], TN)
            put(('k', i), kvbuf.at[i], out, s_qkv.at[i])

    with jax.named_scope('drain'):
        for key in list(busy):
            free(key)


def solution(mesh):
    n_tp = mesh.shape['tp']
    chips = n_tp // 2
    in_specs = (P('dp', None), P('dp', None), P('tp', None), P(None), P(None),
                P(None, 'tp', None), P(None, 'tp', None), P(None, 'tp', None), P('tp', None, None),
                P(None, 'tp'), P(None, 'tp'), P('tp', None), P('dp', 'tp', None))
    out_specs = (P('dp', 'tp', None), P(('dp', 'tp'), None),
                 P('dp', 'tp', None), P('dp', 'tp', None), P('dp', 'tp', None), P(('dp', 'tp'), None, None),
                 P('dp', 'tp'), P('dp', 'tp'), P(('dp', 'tp'), None), P('dp'), P('dp'))

    def device_fn(tokens, positions, emb, gain_attn, gain_mlp, w_query, w_key, w_value, w_out, w_gate, w_up, w_down, grad_hidden):
        seq = tokens.shape[1]
        rows, dim = emb.shape
        lh, hd = w_query.shape[1], w_query.shape[2]
        ffn = w_down.shape[0]
        blk = grad_hidden.shape[1]
        qkvw = (lh + 2) * hd
        inv_freq = (np.float32(ROPE_THETA) ** (-np.arange(hd // 2, dtype=np.float32) * np.float32(2.0 / hd))).astype(np.float32)
        invf = jnp.asarray(np.concatenate([inv_freq, inv_freq])[None, :])

        def sds(shape, dt=BF):
            return jax.ShapeDtypeStruct(shape, dt)

        hb = pl.BlockSpec(memory_space=pltpu.HBM)
        vm = pl.BlockSpec(memory_space=pltpu.VMEM)
        maxc = max(RS_CHUNKS.values())
        mid = pl.pallas_call(
            functools.partial(layer_kernel, n_tp, lh),
            name='layer',
            out_shape=[sds((n_tp, blk, dim))] * 5 + [sds((seq, ffn)), sds((seq, 2 * ffn)), sds((seq, lh * hd)), sds((seq, qkvw)),
                                                    sds((1, dim), F32), sds((1, dim), F32), sds((blk, dim))],
            in_specs=[hb] * 14,
            out_specs=[vm] * 12,
            scratch_shapes=[
                pltpu.VMEM((1, seq), jnp.int32), pltpu.VMEM((1, seq), jnp.int32), pltpu.VMEM((1, hd), F32),
                pltpu.VMEM((1, dim), F32), pltpu.VMEM((1, dim), F32), pltpu.VMEM((blk, dim), BF),
                pltpu.VMEM((rows, dim), BF), pltpu.VMEM((seq, rows), BF), pltpu.VMEM((dim * lh, hd), BF), pltpu.VMEM((dim * lh, hd), F32),
                pltpu.VMEM((dim, qkvw), BF), pltpu.VMEM((lh * hd, dim), BF), pltpu.VMEM((dim, 2 * ffn), BF), pltpu.VMEM((ffn, dim), BF),
                pltpu.VMEM((5, chips, 2, blk, dim), BF), pltpu.VMEM((5, chips, blk, dim), BF),
                pltpu.VMEM((5, chips, blk, dim), BF), pltpu.VMEM((5, chips - 1, blk, dim), BF),
                pltpu.VMEM((n_tp, blk, dim), BF), pltpu.VMEM((n_tp, blk, dim), BF), pltpu.VMEM((n_tp, blk, dim), BF),
                pltpu.VMEM((n_tp, blk, dim), BF), pltpu.VMEM((2 * ffn, dim), BF), pltpu.VMEM((qkvw, dim), BF), pltpu.VMEM((dim, lh * hd), BF), pltpu.VMEM((blk, dim), F32), pltpu.VMEM((blk, dim), F32),
                pltpu.VMEM((2, seq, hd), F32), pltpu.VMEM((seq, ffn), F32), pltpu.VMEM((seq, qkvw), BF),
                pltpu.VMEM((2, seq, hd), F32), pltpu.VMEM((lh, seq, seq), F32),
                pltpu.SemaphoreType.DMA((2, 2)), pltpu.SemaphoreType.DMA(((max(AG_CHUNKS.values()) + 1) * (2 * chips - 1),)),
                pltpu.SemaphoreType.DMA((2, 2)), pltpu.SemaphoreType.DMA((2, maxc, chips)),
                pltpu.SemaphoreType.DMA((18,)),
            ],
            compiler_params=pltpu.CompilerParams(collective_id=0, has_side_effects=True, vmem_limit_bytes=44 * 1024 * 1024),
        )(*(pltpu.with_memory_space_constraint(a, pltpu.HBM) for a in (
            tokens, positions, invf, gain_attn.reshape(1, dim), gain_mlp.reshape(1, dim), grad_hidden.reshape(blk, dim),
            emb, w_query.reshape(dim * lh, hd), w_key.reshape(dim, hd), w_value.reshape(dim, hd), w_out.reshape(lh * hd, dim),
            w_gate, w_up, w_down)))
        n1, n2, gh, gh1, gf, act, gcat, heads, gqkv, gain_m, gain_a, hid = mid
        n1, n2, gh, gh1, gf = (a.reshape(seq, dim) for a in (n1, n2, gh, gh1, gf))
        wide_rows, tall_rows = 256, 512
        res = pl.pallas_call(
            functools.partial(grads_kernel, n_tp, lh),
            name='grads',
            out_shape=[sds((blk, dim)), sds((rows, dim), F32), sds((dim * lh, hd), F32), sds((dim, hd), F32), sds((dim, hd), F32),
                       sds((lh * hd, dim), F32), sds((dim, ffn), F32), sds((dim, ffn), F32), sds((ffn, dim), F32),
                       sds((1, dim), F32), sds((1, dim), F32)],
            in_specs=[vm] * 13,
            out_specs=[hb] * 11,
            scratch_shapes=[
                pltpu.VMEM((3, wide_rows, dim), F32), pltpu.VMEM((3, tall_rows, ffn), F32), pltpu.VMEM((dim * lh, hd), F32),
                pltpu.VMEM((2, dim, hd), F32),
                pltpu.SemaphoreType.DMA((3,)), pltpu.SemaphoreType.DMA((3,)), pltpu.SemaphoreType.DMA((3,)),
                pltpu.SemaphoreType.DMA((3,)),
            ],
            compiler_params=pltpu.CompilerParams(vmem_limit_bytes=24 * 1024 * 1024),
        )(tokens, gain_m, gain_a, hid, gh, act, n2, gcat, gh1, heads, n1, gqkv, gf)
        o_hid, o_emb, o_wq, o_wk, o_wv, o_wo, o_wg, o_wu, o_wd, o_ga, o_gm = res
        return (o_hid.reshape(1, blk, dim), o_emb, o_wq.reshape(dim, lh, hd), o_wk.reshape(dim, 1, hd), o_wv.reshape(dim, 1, hd),
                o_wo.reshape(lh, hd, dim), o_wg, o_wu, o_wd, o_ga.reshape(dim), o_gm.reshape(dim))

    return jax.shard_map(device_fn, mesh=mesh, in_specs=in_specs, out_specs=out_specs, check_vma=False)
```

```python
import functools

import jax
import jax.numpy as jnp
import numpy as np
from jax import lax
from jax.experimental import pallas as pl
from jax.experimental.pallas import tpu as pltpu
from jax.sharding import PartitionSpec as P

ROPE_THETA = 1000000.0
RMS_EPS = 1e-5
MESH = pl.DeviceIdType.MESH
BF = jnp.bfloat16
F32 = jnp.float32
NT = (((1,), (1,)), ((), ()))
TN = (((0,), (0,)), ((), ()))

N1, GH, N2, GH1, GF = range(5)
R_EMB, R_ATT, R_GN2, R_MLP, R_GN1 = range(5)
RS_CHUNKS = {R_EMB: 4, R_ATT: 4, R_GN2: 4, R_MLP: 2, R_GN1: 4}
AG_CHUNKS = {N1: 4, GH: 1, N2: 4, GH1: 4, GF: 4}


def dot(a, b, dims=(((1,), (0,)), ((), ()))):
    return lax.dot_general(a, b, dims, preferred_element_type=F32)


def scoped(name):
    def wrap(fn):
        def run(p, *rest, **kw):
            with jax.named_scope(f'{name}_{p}'):
                return fn(p, *rest, **kw)
        return run
    return wrap


def layer_kernel(n_tp, local_heads,
                 h_tok, h_pos, h_invf, h_ga, h_gm, h_gh, emb, wq4, wk, wv, wo, wg, wu, wd,
                 o_n1, o_n2, o_gh, o_gh1, o_gf, act, gcat, heads, gqkv, gain_m, gain_a, hid,
                 tok, pos, invf, ga, gm, gh_in, embv, onehot, wqr, wqf, wqkv, wov, wguv, wdv, pb, rd, sb, rr,
                 x0g, h1g, gn2g, gn1g, wgut, wqkvt, wovt, x0f, h1f, inv, gact, qkvb, tabs, probs,
                 ag_s, ag_r, rs_s, rs_r, loc):
    chips = n_tp // 2
    seq = h_tok.shape[1]
    rows, dim = emb.shape
    ffn = wd.shape[0]
    blk = gh_in.shape[0]
    hd = wk.shape[1]
    scale = hd ** -0.5
    qw = local_heads * hd

    me = lax.axis_index('tp')
    chip = me // 2
    core = lax.rem(me, 2)
    sib = 2 * chip + 1 - core

    def peer_chip(d):
        return lax.rem(chip + d, chips)

    def peer(d):
        return 2 * peer_chip(d) + core

    order = sorted(range(1, chips), key=lambda d: -min(d, chips - d))

    barrier = pltpu.get_barrier_semaphore()
    for dev in [sib] + [peer(d) for d in range(1, chips)]:
        pl.semaphore_signal(barrier, inc=1, device_id={'tp': dev}, device_id_type=MESH)

    nloc = [1]

    def local(src, dst, slot=None):
        if slot is None:
            slot = nloc[0]
            nloc[0] += 1
        cp = pltpu.make_async_copy(src, dst, loc.at[slot])
        cp.start()
        return cp

    n_emb = RS_CHUNKS[R_EMB]
    ew = dim // n_emb

    def emb_load(j):
        return local(emb.at[:, pl.ds(j * ew, ew)], embv.at[:, pl.ds(j * ew, ew)])

    in_cp = [local(h_tok, tok)]
    emb_cp = [emb_load(j) for j in range(3)]
    in_cp += [local(a, b) for a, b in ((h_pos, pos), (h_invf, invf), (h_ga, ga), (h_gm, gm), (h_gh, gh_in))]
    in_cp[0].wait()

    tok_t = jnp.transpose(jnp.broadcast_to(tok[...].astype(F32), (seq, seq)))
    tok_t = tok_t - (me * rows).astype(F32)
    lane = lax.broadcasted_iota(jnp.int32, (seq, seq), 1).astype(F32)
    for b in range(rows // seq):
        onehot[:, b * seq:(b + 1) * seq] = jnp.where(tok_t == lane + float(b * seq), 1.0, 0.0).astype(BF)

    def remote(src, dst, s, r, dev):
        return pltpu.make_async_remote_copy(src_ref=src, dst_ref=dst, send_sem=s, recv_sem=r,
                                            device_id={'tp': dev}, device_id_type=MESH)

    def send(*args):
        remote(*args).start()

    incoming = [(d, c) for d in order for c in (1, 0)]

    ag_set = {N1: 0, N2: 0, GH1: 0, GF: 0, GH: 1}
    ag = {N1: x0g, GH: o_gh, N2: h1g, GH1: gn2g, GF: gn1g}
    per = 2 * chips - 1

    def ag_view(p, t, j):
        w = dim // AG_CHUNKS[p]
        return ag[p].at[t, :, pl.ds(j * w, w)]

    def ag_block(p, d, c, j):
        return ag_view(p, 2 * lax.rem(chip + chips - d, chips) + c, j)

    def ag_recv(p, j, i):
        return ag_r.at[(per * j if ag_set[p] == 0 else ag_r.shape[0] - per) + i]

    def ag_wait_sends(p):
        own, passed = ag[p].at[pl.ds(0, chips)], ag[p].at[pl.ds(0, n_tp - 2)]
        remote(own, own, ag_s.at[ag_set[p], 0], ag_recv(p, 0, 0), sib).wait_send()

        @pl.when(core == 1)
        def _():
            remote(passed, passed, ag_s.at[ag_set[p], 1], ag_recv(p, 0, 0), sib).wait_send()

    @scoped('ag_start')
    def ag_start(p, only=None):
        q = ag_set[p]
        for j in range(AG_CHUNKS[p]) if only is None else (only,):
            mine = ag_view(p, me, j)
            for d in order:
                send(mine, mine, ag_s.at[q, 0], ag_recv(p, j, 2 * d - core), 2 * peer_chip(d) + 1)
            send(mine, mine, ag_s.at[q, 0], ag_recv(p, j, 0), sib)

    @scoped('ag_finish')
    def ag_finish(j, *ps, early=None, forward=True, collect=True, between=None):
        if j == 0 and forward:
            @pl.when(core == 1)
            def _():
                for k in range(AG_CHUNKS[ps[0]]):
                    for d, c in incoming:
                        for p in ps:
                            got = ag_block(p, d, c, k)
                            q = ag_set[p]
                            remote(got, got, ag_s.at[q, 1], ag_recv(p, k, 2 * d - c), sib).wait_recv()
                            send(got, got, ag_s.at[q, 1], ag_recv(p, k, 2 * d - c), sib)
                    if early is not None and k == 1:
                        early()
                    if between is not None and k < AG_CHUNKS[ps[0]] - 1:
                        between(k)

        if not collect:
            return
        for p in ps:
            got = ag_view(p, sib, j)
            remote(got, got, ag_s.at[ag_set[p], 0], ag_recv(p, j, 0), sib).wait_recv()

        @pl.when(core == 0)
        def _():
            for i, (d, c) in enumerate(incoming):
                if i == 2 and early is not None:
                    early()
                for p in ps:
                    got = ag_block(p, d, c, j)
                    remote(got, got, ag_s.at[ag_set[p], 1], ag_recv(p, j, 2 * d - c), sib).wait_recv()

    def gathered(p, j=None):
        if j is None:
            return ag[p][...].reshape(seq, dim)
        w = dim // AG_CHUNKS[p]
        return ag[p][:, :, j * w:(j + 1) * w].reshape(seq, w)

    def gathered_dot(p, weight, early):
        w = dim // AG_CHUNKS[p]
        total = None
        for j in range(AG_CHUNKS[p]):
            ag_finish(j, p, early=early if j == 0 else None)
            part = weight(gathered(p, j), slice(j * w, (j + 1) * w))
            total = part if total is None else total + part
        return total

    rs_set = {R_EMB: 0, R_ATT: 0, R_GN2: 0, R_GN1: 0, R_MLP: 1}

    def rs_wait_sends(p):
        q = rs_set[p]
        remote(rd.at[p], rd.at[p], rs_s.at[q, 0], rs_r.at[q, 0, 0], sib).wait_send()
        remote(rr.at[p], rr.at[p], rs_s.at[q, 1], rs_r.at[q, 0, 0], sib).wait_send()

    def rs_cols(p, j):
        w = dim // RS_CHUNKS[p]
        return slice(j * w, (j + 1) * w)

    @scoped('rs_local')
    def rs_local(p, j, val):
        c = rs_cols(p, j)
        w = c.stop - c.start
        pb[p, :, :, :, c] = val.astype(BF).reshape(chips, 2, blk, w)
        send(pb.at[p, :, 1 - core, :, c], rd.at[p, :, :, c], rs_s.at[rs_set[p], 0], rs_r.at[rs_set[p], j, 0], sib)

    @scoped('rs_cross')
    def rs_cross(p, j):
        c = rs_cols(p, j)
        remote(rd.at[p, :, :, c], rd.at[p, :, :, c], rs_s.at[rs_set[p], 0], rs_r.at[rs_set[p], j, 0], sib).wait_recv()
        for d in order:
            to = peer_chip(d)
            both = pb[p, to, core, :, c].astype(F32) + rd[p, to, :, c].astype(F32)
            sb[p, to, :, c] = both.astype(BF)
            send(sb.at[p, to, :, c], rr.at[p, d - 1, :, c], rs_s.at[rs_set[p], 1], rs_r.at[rs_set[p], j, d], peer(d))

    @scoped('rs_finish')
    def rs_finish(p, only=None):
        parts = []
        for j in range(RS_CHUNKS[p]) if only is None else (only,):
            c = rs_cols(p, j)
            total = pb[p, chip, core, :, c].astype(F32) + rd[p, chip, :, c].astype(F32)
            for d in order[::-1]:
                remote(rr.at[p, d - 1, :, c], rr.at[p, d - 1, :, c], rs_s.at[rs_set[p], 1], rs_r.at[rs_set[p], j, d], sib).wait_recv()
                total = total + rr[p, d - 1, :, c].astype(F32)
            parts.append(total)
        return jnp.concatenate(parts, axis=1)

    def rs_start(p, chunk):
        n = RS_CHUNKS[p]
        for j in range(n):
            val = chunk(rs_cols(p, j))
            if p == R_EMB and j == 0:
                with jax.named_scope('barrier'):
                    pl.semaphore_wait(barrier, chips)
            rs_local(p, j, val)
            if j > 0:
                @pl.when(core == 0)
                def _():
                    rs_cross(p, j - 1)

        @pl.when(core == 0)
        def _():
            rs_cross(p, n - 1)

        @pl.when(core == 1)
        def _():
            for j in range(n):
                rs_cross(p, j)

    def on_core(k, fn):
        @pl.when(core == k)
        def _():
            fn()

    def spread(v):
        return jnp.broadcast_to(v, (seq, hd))

    def norm_fwd(p, slot, gain, out, early=None, between=None):
        square = None
        for j in range(AG_CHUNKS[p]):
            ag_finish(j, p, early=early if j == 0 else None, between=between)
            if between is not None and j < AG_CHUNKS[p] - 1:
                on_core(0, lambda: between(j))
            part = gathered(p, j).astype(F32)
            part = jnp.sum(part * part, axis=-1, keepdims=True)
            square = part if square is None else square + part
        r = lax.rsqrt(square * (1.0 / dim) + RMS_EPS)
        inv[slot] = spread(r)
        w = dim // AG_CHUNKS[p]
        for j in range(AG_CHUNKS[p]):
            c = slice(j * w, (j + 1) * w)
            out[:, :, c] = (gathered(p, j).astype(F32) * r * gain[:, c]).astype(BF).reshape(n_tp, blk, w)

    def norm_bwd(p, p_in, slot, gain, around, out, gain_out, early=None, use=None):
        w = dim // AG_CHUNKS[p]
        r = inv[slot][:, :1]
        both = None
        for j in range(AG_CHUNKS[p]):
            c = slice(j * w, (j + 1) * w)
            ag_finish(j, p, early=early if j == 0 else None)
            g = gathered(p, j).astype(F32)
            n = gathered(p_in, j).astype(F32) * r
            gn = g * n
            gain_out[:, c] = jnp.sum(gn, axis=0, keepdims=True)
            part = jnp.sum(gn * gain[:, c], axis=-1, keepdims=True)
            both = part if both is None else both + part
        mean = both * (1.0 / dim)
        for j in range(AG_CHUNKS[p]):
            c = slice(j * w, (j + 1) * w)
            n = gathered(p_in, j).astype(F32) * r
            g_in = r * (gathered(p, j).astype(F32) * gain[:, c] - n * mean)
            total = (around[:, :, c].reshape(seq, w).astype(F32) + g_in).astype(BF)
            out[:, :, c] = total.reshape(n_tp, blk, w)
            if use is not None:
                use(total, c)

    w_cp = {}

    def emb_chunk(c):
        j = c.start // ew
        emb_cp[j].wait()
        if j + 3 < n_emb:
            emb_cp.append(emb_load(j + 3))
        if j == n_emb - 2:
            w_cp['k'] = local(wk, wqkv.at[:, pl.ds(qw, hd)])
            w_cp['v'] = local(wv, wqkv.at[:, pl.ds(qw + hd, hd)])
            w_cp['q'] = local(wq4, wqr)
        if j == n_emb - 1:
            w_cp['o'] = local(wo, wov)
            w_cp['g'] = local(wg, wguv.at[:, pl.ds(0, ffn)])
            w_cp['u'] = local(wu, wguv.at[:, pl.ds(ffn, ffn)])
            w_cp['d'] = local(wd, wdv)
        return dot(onehot[...], embv[:, c])

    rs_start(R_EMB, emb_chunk)

    in_cp[1].wait()
    in_cp[2].wait()
    pos_t = jnp.transpose(jnp.broadcast_to(pos[...].astype(F32), (seq, seq)))
    angle = pos_t * invf[...]
    half = lax.broadcasted_iota(jnp.int32, (seq, hd), 1) < hd // 2
    tabs[0] = jnp.cos(angle)
    sin = jnp.sin(angle)
    tabs[1] = jnp.where(half, -sin, sin)
    for cp in in_cp[3:]:
        cp.wait()
    for j in range(RS_CHUNKS[R_EMB]):
        part = rs_finish(R_EMB, j)
        x0f[:, rs_cols(R_EMB, j)] = part
        x0g[me, :, rs_cols(R_EMB, j)] = part.astype(BF)
        ag_start(N1, j)
    o_gh[me] = gh_in[...]
    w_cp['k'].wait()
    w_cp['v'].wait()
    w_cp['q'].wait()
    wqf[...] = wqr[...].astype(F32)
    for h in range(local_heads):
        wqkv[:, h * hd:(h + 1) * hd] = wqf[pl.ds(h, dim, stride=local_heads), :].astype(BF)


    tw = 256
    eye = (lax.broadcasted_iota(jnp.int32, (tw, tw), 0) == lax.broadcasted_iota(jnp.int32, (tw, tw), 1)).astype(F32).astype(BF)
    with jax.named_scope('wqkvt'):
        for b in range((qw + 2 * hd) // tw):
            wqkvt[b * tw:(b + 1) * tw, :] = dot(eye, wqkv[:, b * tw:(b + 1) * tw], NT).astype(BF)

    def rotate(v, sign):
        return v * tabs[0] + sign * (pltpu.roll(v, hd // 2, 1) * tabs[1])

    w_cp['g'].wait()
    w_cp['u'].wait()

    def transpose_gate_up(k):
        with jax.named_scope('wgut'):
            n = 2 * ffn // tw
            for b in range(n * k // 3, n * (k + 1) // 3):
                wgut[b * tw:(b + 1) * tw, :] = dot(eye, wguv[:, b * tw:(b + 1) * tw], NT).astype(BF)

    norm_fwd(N1, 0, ga, o_n1, early=lambda: ag_start(GH), between=transpose_gate_up)
    qkv = dot(o_n1[...].reshape(seq, dim), wqkv[...])
    for h in range(local_heads + 1):
        qkvb[:, h * hd:(h + 1) * hd] = rotate(qkv[:, h * hd:(h + 1) * hd], 1.0).astype(BF)
    qkvb[:, qw + hd:] = qkv[:, qw + hd:].astype(BF)
    kb = qkvb[:, qw:qw + hd]
    vb = qkvb[:, qw + hd:]
    causal = lax.broadcasted_iota(jnp.int32, (seq, seq), 0) >= lax.broadcasted_iota(jnp.int32, (seq, seq), 1)
    for h in range(local_heads):
        s = dot(qkvb[:, h * hd:(h + 1) * hd], kb, NT) * scale
        s = jnp.where(causal, s, -1e30)
        e = jnp.exp(s - jnp.max(s, axis=-1, keepdims=True))
        pr = e / jnp.sum(e, axis=-1, keepdims=True)
        probs[h] = pr
        heads[:, h * hd:(h + 1) * hd] = dot(pr.astype(BF), vb).astype(BF)
    w_cp['o'].wait()
    rs_wait_sends(R_EMB)
    rs_start(R_ATT, lambda c: dot(heads[...], wov[:, c]))

    with jax.named_scope('wovt'):
        for b in range(dim // tw):
            wovt[b * tw:(b + 1) * tw, :] = dot(eye, wov[:, b * tw:(b + 1) * tw], NT).astype(BF)
    ag_finish(0, GH, collect=False)
    w_cp['d'].wait()

    ag_wait_sends(N1)
    for j in range(RS_CHUNKS[R_ATT]):
        c = rs_cols(R_ATT, j)
        h1 = (x0f[:, c] + rs_finish(R_ATT, j).astype(BF).astype(F32)).astype(BF)
        h1f[:, c] = h1.astype(F32)
        h1g[me, :, c] = h1
        ag_start(N2, j)
    ag_finish(0, GH, forward=False)

    def act_grad(k):
        if k == 0:
            with jax.named_scope('gact'):
                gact[...] = dot(gathered(GH), wdv[...], NT).astype(BF).astype(F32)

    norm_fwd(N2, 1, gm, o_n2, between=act_grad)

    n2 = o_n2[...].reshape(seq, dim)
    fw = 256
    for j in range(ffn // fw):
        c = slice(j * fw, (j + 1) * fw)
        cu = slice(ffn + j * fw, ffn + (j + 1) * fw)
        gate = dot(n2, wguv[:, c])
        up = dot(n2, wguv[:, cu])
        sig = jax.nn.sigmoid(gate)
        ga_act = gate * sig
        act[:, c] = (ga_act * up).astype(BF)
        g = gact[:, c]
        gcat[:, cu] = (g * ga_act).astype(BF)
        gcat[:, c] = (g * up * sig * (1.0 + gate * (1.0 - sig))).astype(BF)
    rs_wait_sends(R_ATT)
    rs_start(R_GN2, lambda c: dot(gcat[...], wgut[:, c]))
    for j in range(RS_CHUNKS[R_MLP]):
        rs_local(R_MLP, j, dot(act[...], wdv[:, rs_cols(R_MLP, j)]))

    ag_wait_sends(N2)
    for j in range(RS_CHUNKS[R_GN2]):
        gn2g[me, :, rs_cols(R_GN2, j)] = rs_finish(R_GN2, j).astype(BF)
        ag_start(GH1, j)

    def mlp_cross():
        for j in range(RS_CHUNKS[R_MLP]):
            rs_cross(R_MLP, j)

    ghd_parts = []
    norm_bwd(GH1, N2, 1, gm, o_gh, o_gh1, gain_m, early=mlp_cross, use=lambda a, c: ghd_parts.append(dot(a, wovt[c, :])))
    ghd = sum(ghd_parts[1:], ghd_parts[0]).astype(BF)

    gv = jnp.zeros((seq, hd), F32)
    gk = jnp.zeros((seq, hd), F32)
    for h in range(local_heads):
        g = ghd[:, h * hd:(h + 1) * hd]
        pr = probs[h]
        gp = dot(g, vb, NT).astype(BF).astype(F32)
        gv = gv + dot(pr.astype(BF), g, TN)
        gs = (pr * (gp - jnp.sum(gp * pr, axis=-1, keepdims=True)) * scale).astype(BF)
        gq = dot(gs, kb).astype(BF).astype(F32)
        gk = gk + dot(gs, qkvb[:, h * hd:(h + 1) * hd], TN)
        gqkv[:, h * hd:(h + 1) * hd] = rotate(gq, -1.0).astype(BF)
    gqkv[:, qw:qw + hd] = rotate(gk.astype(BF).astype(F32), -1.0).astype(BF)
    gqkv[:, qw + hd:] = gv.astype(BF)
    rs_wait_sends(R_GN2)
    rs_start(R_GN1, lambda c: dot(gqkv[...], wqkvt[:, c]))

    ag_wait_sends(GH1)
    for j in range(RS_CHUNKS[R_GN1]):
        gn1g[me, :, rs_cols(R_GN1, j)] = rs_finish(R_GN1, j).astype(BF)
        ag_start(GF, j)
    hid[...] = (h1f[...] + rs_finish(R_MLP).astype(BF).astype(F32)).astype(BF)
    norm_bwd(GF, N1, 0, ga, o_gh1, o_gf, gain_a)
    with jax.named_scope('tail_send'):
        rs_wait_sends(R_GN1)
        rs_wait_sends(R_MLP)
        ag_wait_sends(GH)
        ag_wait_sends(GF)


def grads_kernel(n_tp, local_heads,
                 tok, gain_m, gain_a, hid, gh, act, n2, gcat, gh1, heads, n1, gqkv, gf,
                 o_hid, o_emb, o_wq, o_wk, o_wv, o_wo, o_wg, o_wu, o_wd, o_ga, o_gm,
                 wide, tall, qbuf, kvbuf, s_wide, s_tall, s_qkv, s_out, s_first):
    seq, dim = n1.shape
    rows = o_emb.shape[0]
    ffn = act.shape[1]
    hd = gqkv.shape[1] // (local_heads + 2)
    me = lax.axis_index('tp')
    n_wide, wr = wide.shape[0], wide.shape[1]
    n_tall, tr = tall.shape[0], tall.shape[1]
    busy = {}

    def put(key, src, dst, sem):
        cp = pltpu.make_async_copy(src, dst, sem)
        cp.start()
        busy[key] = cp

    def free(key):
        if key in busy:
            busy.pop(key).wait()

    row = lax.broadcasted_iota(jnp.int32, (wr, seq), 0)
    wide_units = []
    for u in range(ffn // wr):
        wide_units.append((lambda u=u: dot(act[:, u * wr:(u + 1) * wr], gh[...], TN), o_wd.at[pl.ds(u * wr, wr)]))
    for u in range(heads.shape[1] // wr):
        wide_units.append((lambda u=u: dot(heads[:, u * wr:(u + 1) * wr], gh1[...], TN), o_wo.at[pl.ds(u * wr, wr)]))
    for u in range(rows // wr):
        wide_units.append((lambda u=u: dot(jnp.where(row + u * wr == tok[...] - me * rows, 1.0, 0.0).astype(BF), gf[...]),
                           o_emb.at[pl.ds(u * wr, wr)]))
    tall_units = []
    for half, out in ((0, o_wg), (1, o_wu)):
        for u in range(dim // tr):
            tall_units.append((lambda u=u, half=half: dot(n2[:, u * tr:(u + 1) * tr], gcat[:, half * ffn:(half + 1) * ffn], TN),
                               out.at[pl.ds(u * tr, tr)]))
    iw = it = 0
    while iw < len(wide_units) or it < len(tall_units):
        if iw < len(wide_units):
            slot = iw % n_wide
            fn, dst = wide_units[iw]
            free(('w', slot))
            if iw == n_wide:
                for k in range(4):
                    free(('f', k))
            with jax.named_scope(f'wide_{iw}'):
                if iw == 0:
                    fr = wr // 4
                    for k in range(4):
                        rows_k = slice(k * fr, (k + 1) * fr)
                        wide[slot, rows_k] = dot(act[:, rows_k], gh[...], TN)
                        put(('f', k), wide.at[slot, pl.ds(k * fr, fr)], o_wd.at[pl.ds(k * fr, fr)], s_first.at[k])
                else:
                    wide[slot] = fn()
                    put(('w', slot), wide.at[slot], dst, s_wide.at[slot])
            iw += 1
        if it < len(tall_units):
            slot = it % n_tall
            fn, dst = tall_units[it]
            free(('t', slot))
            with jax.named_scope(f'tall_{it}'):
                tall[slot] = fn()
                put(('t', slot), tall.at[slot], dst, s_tall.at[slot])
            it += 1
    put(('out', 0), hid, o_hid, s_out.at[0])
    put(('out', 1), gain_a, o_ga, s_out.at[1])
    put(('out', 2), gain_m, o_gm, s_out.at[2])
    qw = local_heads * hd
    with jax.named_scope('qkv'):
        for h in range(local_heads):
            qbuf[pl.ds(h, dim, stride=local_heads), :] = dot(n1[...], gqkv[:, h * hd:(h + 1) * hd], TN)
        put(('q', 0), qbuf, o_wq, s_qkv.at[2])
        for i, out in enumerate((o_wk, o_wv)):
            kvbuf[i] = dot(n1[...], gqkv[:, qw + i * hd:qw + (i + 1) * hd], TN)
            put(('k', i), kvbuf.at[i], out, s_qkv.at[i])

    with jax.named_scope('drain'):
        for key in list(busy):
            free(key)


def solution(mesh):
    n_tp = mesh.shape['tp']
    chips = n_tp // 2
    in_specs = (P('dp', None), P('dp', None), P('tp', None), P(None), P(None),
                P(None, 'tp', None), P(None, 'tp', None), P(None, 'tp', None), P('tp', None, None),
                P(None, 'tp'), P(None, 'tp'), P('tp', None), P('dp', 'tp', None))
    out_specs = (P('dp', 'tp', None), P(('dp', 'tp'), None),
                 P('dp', 'tp', None), P('dp', 'tp', None), P('dp', 'tp', None), P(('dp', 'tp'), None, None),
                 P('dp', 'tp'), P('dp', 'tp'), P(('dp', 'tp'), None), P('dp'), P('dp'))

    def device_fn(tokens, positions, emb, gain_attn, gain_mlp, w_query, w_key, w_value, w_out, w_gate, w_up, w_down, grad_hidden):
        seq = tokens.shape[1]
        rows, dim = emb.shape
        lh, hd = w_query.shape[1], w_query.shape[2]
        ffn = w_down.shape[0]
        blk = grad_hidden.shape[1]
        qkvw = (lh + 2) * hd
        inv_freq = (np.float32(ROPE_THETA) ** (-np.arange(hd // 2, dtype=np.float32) * np.float32(2.0 / hd))).astype(np.float32)
        invf = jnp.asarray(np.concatenate([inv_freq, inv_freq])[None, :])

        def sds(shape, dt=BF):
            return jax.ShapeDtypeStruct(shape, dt)

        hb = pl.BlockSpec(memory_space=pltpu.HBM)
        vm = pl.BlockSpec(memory_space=pltpu.VMEM)
        maxc = max(RS_CHUNKS.values())
        mid = pl.pallas_call(
            functools.partial(layer_kernel, n_tp, lh),
            name='layer',
            out_shape=[sds((n_tp, blk, dim))] * 5 + [sds((seq, ffn)), sds((seq, 2 * ffn)), sds((seq, lh * hd)), sds((seq, qkvw)),
                                                    sds((1, dim), F32), sds((1, dim), F32), sds((blk, dim))],
            in_specs=[hb] * 14,
            out_specs=[vm] * 12,
            scratch_shapes=[
                pltpu.VMEM((1, seq), jnp.int32), pltpu.VMEM((1, seq), jnp.int32), pltpu.VMEM((1, hd), F32),
                pltpu.VMEM((1, dim), F32), pltpu.VMEM((1, dim), F32), pltpu.VMEM((blk, dim), BF),
                pltpu.VMEM((rows, dim), BF), pltpu.VMEM((seq, rows), BF), pltpu.VMEM((dim * lh, hd), BF), pltpu.VMEM((dim * lh, hd), F32),
                pltpu.VMEM((dim, qkvw), BF), pltpu.VMEM((lh * hd, dim), BF), pltpu.VMEM((dim, 2 * ffn), BF), pltpu.VMEM((ffn, dim), BF),
                pltpu.VMEM((5, chips, 2, blk, dim), BF), pltpu.VMEM((5, chips, blk, dim), BF),
                pltpu.VMEM((5, chips, blk, dim), BF), pltpu.VMEM((5, chips - 1, blk, dim), BF),
                pltpu.VMEM((n_tp, blk, dim), BF), pltpu.VMEM((n_tp, blk, dim), BF), pltpu.VMEM((n_tp, blk, dim), BF),
                pltpu.VMEM((n_tp, blk, dim), BF), pltpu.VMEM((2 * ffn, dim), BF), pltpu.VMEM((qkvw, dim), BF), pltpu.VMEM((dim, lh * hd), BF), pltpu.VMEM((blk, dim), F32), pltpu.VMEM((blk, dim), F32),
                pltpu.VMEM((2, seq, hd), F32), pltpu.VMEM((seq, ffn), F32), pltpu.VMEM((seq, qkvw), BF),
                pltpu.VMEM((2, seq, hd), F32), pltpu.VMEM((lh, seq, seq), F32),
                pltpu.SemaphoreType.DMA((2, 2)), pltpu.SemaphoreType.DMA(((max(AG_CHUNKS.values()) + 1) * (2 * chips - 1),)),
                pltpu.SemaphoreType.DMA((2, 2)), pltpu.SemaphoreType.DMA((2, maxc, chips)),
                pltpu.SemaphoreType.DMA((18,)),
            ],
            compiler_params=pltpu.CompilerParams(collective_id=0, has_side_effects=True, vmem_limit_bytes=44 * 1024 * 1024),
        )(*(pltpu.with_memory_space_constraint(a, pltpu.HBM) for a in (
            tokens, positions, invf, gain_attn.reshape(1, dim), gain_mlp.reshape(1, dim), grad_hidden.reshape(blk, dim),
            emb, w_query.reshape(dim * lh, hd), w_key.reshape(dim, hd), w_value.reshape(dim, hd), w_out.reshape(lh * hd, dim),
            w_gate, w_up, w_down)))
        n1, n2, gh, gh1, gf, act, gcat, heads, gqkv, gain_m, gain_a, hid = mid
        n1, n2, gh, gh1, gf = (a.reshape(seq, dim) for a in (n1, n2, gh, gh1, gf))
        wide_rows, tall_rows = 256, 512
        res = pl.pallas_call(
            functools.partial(grads_kernel, n_tp, lh),
            name='grads',
            out_shape=[sds((blk, dim)), sds((rows, dim), F32), sds((dim * lh, hd), F32), sds((dim, hd), F32), sds((dim, hd), F32),
                       sds((lh * hd, dim), F32), sds((dim, ffn), F32), sds((dim, ffn), F32), sds((ffn, dim), F32),
                       sds((1, dim), F32), sds((1, dim), F32)],
            in_specs=[vm] * 13,
            out_specs=[hb] * 11,
            scratch_shapes=[
                pltpu.VMEM((3, wide_rows, dim), F32), pltpu.VMEM((3, tall_rows, ffn), F32), pltpu.VMEM((dim * lh, hd), F32),
                pltpu.VMEM((2, dim, hd), F32),
                pltpu.SemaphoreType.DMA((3,)), pltpu.SemaphoreType.DMA((3,)), pltpu.SemaphoreType.DMA((3,)),
                pltpu.SemaphoreType.DMA((3,)), pltpu.SemaphoreType.DMA((4,)),
            ],
            compiler_params=pltpu.CompilerParams(vmem_limit_bytes=24 * 1024 * 1024),
        )(tokens, gain_m, gain_a, hid, gh, act, n2, gcat, gh1, heads, n1, gqkv, gf)
        o_hid, o_emb, o_wq, o_wk, o_wv, o_wo, o_wg, o_wu, o_wd, o_ga, o_gm = res
        return (o_hid.reshape(1, blk, dim), o_emb, o_wq.reshape(dim, lh, hd), o_wk.reshape(dim, 1, hd), o_wv.reshape(dim, 1, hd),
                o_wo.reshape(lh, hd, dim), o_wg, o_wu, o_wd, o_ga.reshape(dim), o_gm.reshape(dim))

    return jax.shard_map(device_fn, mesh=mesh, in_specs=in_specs, out_specs=out_specs, check_vma=False)
```
